128 devices in a mesh: layer: 4 (over z_hi, core), row: 32 (over x, y, z_lo).
Axes of the slice: x: 4, y: 4, z: 4 (z_hi: 2, z_lo: 2; z = z_hi * 2 + z_lo), core: 2. Of those that a mesh axis runs over, the one named last changes fastest.
Arguments:
- magnet: float32 [3, 4, 2048, 2048], P(None, 'layer', 'row'), may hold values from -6 to 6
- kernel: float32 [7, 6, 2048, 2048], P(None, None, ('layer', 'row')), may hold values from -1.8 to 1.8, as said below
Outputs:
- demag: float32 [3, 4, 2048, 2048], P(None, 'layer', 'row')
The draws below stay inside these ranges and needn't reach their ends.
Inputs may be any that keep to these rules, and one draw needn't show every extreme that they name: With q' = -q mod 2048 and p' = -p mod 2048: parts 0, 1, 2 satisfy kernel[o, j, q', p] = kernel[o, j, q, p'] = kernel[o, j, q, p]; part 3 changes sign under either mirror; part 4 changes sign under p -> p' and keeps it under q -> q'; part 5 keeps its sign under p -> p' and changes it under q -> q'.
All inputs are finite; a program needn't handle non-finite values.
Results may differ from the reference program's by a relative error of at most 0.0001.
Values sent between devices are 32-bit elements; how exact they have to be, the bound alone decides.
No kernel may reach another device: no remote copies, remote signals or barrier semaphores. Data moves between devices by JAX's collectives and lax.ppermute only.
A program may use at most 256 MiB of HBM per device.

```python
import jax
import jax.numpy as jnp

NX = 2048
NY = 2048
PARTS_SIZE = 6
LAYERS = 4
OFFSETS = 7


def mirror_p(values):
    return jnp.roll(jnp.flip(values, -1), 1, -1)


def mirror_q(values):
    return jnp.roll(jnp.flip(values, -2), 1, -2)


def draw_kernel(key, part):
    base = jax.random.normal(jax.random.fold_in(key, 71), (OFFSETS, PARTS_SIZE, NY, NX), jnp.float32) * 0.3
    base = jnp.clip(base, -0.9, 0.9)
    sign_p = jnp.array([1.0, 1.0, 1.0, -1.0, -1.0, 1.0], jnp.float32)[None, :, None, None]
    sign_q = jnp.array([1.0, 1.0, 1.0, -1.0, 1.0, -1.0], jnp.float32)[None, :, None, None]
    flipped_p = mirror_p(base)
    flipped_q = mirror_q(base)
    flipped_both = mirror_q(flipped_p)
    total = base + sign_p * flipped_p + sign_q * flipped_q + sign_p * sign_q * flipped_both
    return (0.5 * total).astype(jnp.float32)


def level_of(own_key, shape, cuts, low, largest):
    loudness, own = 1.0, jax.random.fold_in(own_key, 6)
    for position, parts in cuts:
        heights = jnp.exp(jax.random.uniform(jax.random.fold_in(own, position), (parts,), jnp.float32, low / len(cuts), largest / len(cuts)))
        loudness = loudness * jnp.repeat(heights, shape[position] // parts).reshape([-1 if axis == position else 1 for axis in range(len(shape))])
    return loudness


def bell_draw(own_key, dims, width, bound, pieces=(), kind=jnp.bfloat16):
    values = jax.random.normal(own_key, dims, jnp.float32) * width
    if len(pieces) > 0:
        values = level_of(own_key, dims, pieces, -0.22, 0.18) * values
    return jnp.clip(values, min=-bound, max=bound).astype(kind)


def setup_inputs(seed: int = 0) -> dict:
    key_of = jax.random.split(jax.random.key(seed), 3)
    return {
        "magnet": bell_draw(key_of[0], (3, LAYERS, NX, NY), 1.0, 6.0, ((1, 4), (2, 32)), jnp.float32),
        "kernel": draw_kernel(jax.random.fold_in(key_of[2], 71), 0),
    }


def reference(magnet, kernel):
    layers = magnet.shape[1]
    spectra = jnp.fft.fft2(jnp.swapaxes(magnet, 2, 3))
    results = []
    for target in range(layers):
        field_x = jnp.zeros_like(spectra[0, 0])
        field_y = jnp.zeros_like(spectra[0, 0])
        field_z = jnp.zeros_like(spectra[0, 0])
        for source in range(layers):
            coeffs = kernel[target - source + layers - 1]
            mag_x = spectra[0, source]
            mag_y = spectra[1, source]
            mag_z = spectra[2, source]
            field_x = field_x + coeffs[0] * mag_x + coeffs[3] * mag_y + 1j * coeffs[4] * mag_z
            field_y = field_y + coeffs[3] * mag_x + coeffs[1] * mag_y + 1j * coeffs[5] * mag_z
            field_z = field_z + 1j * coeffs[4] * mag_x + 1j * coeffs[5] * mag_y + coeffs[2] * mag_z
        stacked = jnp.stack([field_x, field_y, field_z])
        results.append(-jnp.real(jnp.fft.ifft2(stacked)))
    demag = jnp.stack(results, axis=1)
    return jnp.swapaxes(demag, 2, 3).astype(jnp.float32)
```

```python
import math

import jax
import jax.numpy as jnp
import numpy as np
from jax import lax
from jax.experimental import pallas as pl
from jax.experimental.pallas import tpu as pltpu
from jax.sharding import PartitionSpec as P

CELLS = 2048
COMPS = 3
LAYERS = 4
ROWS = 32
X_ROWS = 64
DEVICES = 128
PARTS = 6
OFFSETS = 7
OPS = OFFSETS * PARTS
FINE = 256
COARSE = 8
SLOT = COMPS * COARSE
LANES = 128
EXTRA = 16
P1_ROWS = LAYERS * COMPS * COARSE
P1_ALL = P1_ROWS + EXTRA

F32 = jnp.float32
BF16 = jnp.bfloat16


def halves(table):
    high = np.asarray(table, np.float32).astype(jnp.bfloat16)
    low = (np.asarray(table, np.float64) - high.astype(np.float64)).astype(np.float32).astype(jnp.bfloat16)
    return high, low


def second_digit():
    m = np.arange(DEVICES)
    return np.where(m < DEVICES // 2, 2 * m, 2 * DEVICES - 1 - 2 * m)


def fine_table():
    b = np.arange(FINE)
    k2 = second_digit()
    near = 2.0 * np.pi * (np.outer(b, k2) % FINE) / FINE
    far = 2.0 * np.pi * (np.outer(b, FINE - 1 - k2) % FINE) / FINE
    top = np.concatenate([np.cos(near), -np.sin(near), np.cos(far), np.sin(far)], axis=1)
    bottom = np.concatenate([np.sin(near), np.cos(near), np.sin(far), -np.cos(far)], axis=1)
    return np.concatenate([top, bottom], axis=0)


def closing_table():
    b = np.arange(FINE)
    k2 = second_digit()
    angle = 2.0 * np.pi * (np.outer(k2, b) % FINE) / FINE
    real = 2.0 * np.cos(angle)
    imag = -2.0 * np.sin(angle)
    real[0] = 1.0
    imag[0] = np.where(b % 2 == 0, 1.0, -1.0)
    return np.concatenate([real, imag], axis=0)


def y_twiddle(sign, scale):
    k = np.arange(1, 5)[:, None]
    b = np.arange(FINE)[None, :]
    angle = 2.0 * np.pi * k * b / CELLS
    table = scale * np.stack([np.cos(angle), sign * np.sin(angle)], axis=1)
    return table.reshape(8, FINE).astype(np.float32)


def lane_pair(coefficient):
    real = np.concatenate([coefficient.real, coefficient.real], axis=-1)
    imag = np.concatenate([-coefficient.imag, coefficient.imag], axis=-1)
    return real, imag


def x_twiddle(sign, scale):
    p1 = np.arange(ROWS)[:, None]
    t = np.arange(X_ROWS)[None, :]
    base = scale * np.exp(sign * 2.0j * np.pi * (p1 * t) / CELLS)
    side = np.where(p1 <= ROWS // 2, 1.0, -1.0) * (sign * 1.0j)
    kinds = []
    for kind in (1.0, 1.0j):
        first = lane_pair(kind * base)
        second = lane_pair(kind * base * side)
        kinds.append(np.stack(first + second, axis=1))
    return np.stack(kinds).astype(np.float32).reshape(2 * ROWS * 4, LANES)


def x_table(sign):
    index = np.arange(X_ROWS)
    angle = 2.0 * np.pi * (np.outer(index, index) % X_ROWS) / X_ROWS
    real = np.cos(angle)
    imag = sign * np.sin(angle)
    whole = np.block([[real, imag], [-imag, real]])
    high, low = halves(whole)
    line = np.concatenate([high, low], axis=1)
    return np.concatenate([line, line], axis=0)


def real_dft(values):
    n = len(values)
    if n == 1:
        return [values[0]], [None]
    if n == 2:
        return [values[0] + values[1], values[0] - values[1]], [None, None]
    even_c, even_s = real_dft(values[0::2])
    odd_c, odd_s = real_dft(values[1::2])
    half = n // 2
    quarter = n // 4
    cos_out = [None] * (half + 1)
    sin_out = [None] * (half + 1)
    for k in range(quarter + 1):
        if k == 0:
            cos_out[0] = even_c[0] + odd_c[0]
            cos_out[half] = even_c[0] - odd_c[0]
        elif k == quarter:
            cos_out[k] = even_c[k]
            sin_out[k] = odd_c[k]
        else:
            theta = 2.0 * math.pi * k / n
            cosine, sine = math.cos(theta), math.sin(theta)
            if 8 * k == n:
                real = cosine * (odd_c[k] - odd_s[k])
                imag = cosine * (odd_s[k] + odd_c[k])
            else:
                real = cosine * odd_c[k] - sine * odd_s[k]
                imag = cosine * odd_s[k] + sine * odd_c[k]
            cos_out[k] = even_c[k] + real
            sin_out[k] = even_s[k] + imag
            cos_out[half - k] = even_c[k] - real
            sin_out[half - k] = imag - even_s[k]
    return cos_out, sin_out


def real_sum(cos_in, sin_in, n):
    if n == 1:
        return [cos_in[0]]
    half = n // 2
    if n == 2:
        return [cos_in[0] + cos_in[1], cos_in[0] - cos_in[1]]
    quarter = n // 4
    even_c = [None] * (quarter + 1)
    even_s = [None] * (quarter + 1)
    odd_c = [None] * (quarter + 1)
    odd_s = [None] * (quarter + 1)
    even_c[0] = cos_in[0] + cos_in[half]
    odd_c[0] = cos_in[0] - cos_in[half]
    even_c[quarter] = cos_in[quarter]
    odd_c[quarter] = sin_in[quarter]
    for k in range(1, quarter):
        theta = 2.0 * math.pi * k / n
        cosine, sine = math.cos(theta), math.sin(theta)
        even_c[k] = cos_in[k] + cos_in[half - k]
        even_s[k] = sin_in[k] - sin_in[half - k]
        gap = cos_in[k] - cos_in[half - k]
        both = sin_in[k] + sin_in[half - k]
        if 8 * k == n:
            odd_c[k] = cosine * (gap + both)
            odd_s[k] = cosine * (both - gap)
        else:
            odd_c[k] = cosine * gap + sine * both
            odd_s[k] = cosine * both - sine * gap
    evens = real_sum(even_c, even_s, half)
    odds = real_sum(odd_c, odd_s, half)
    out = [None] * n
    out[0::2] = evens
    out[1::2] = odds
    return out


def split_pair(value):
    high = value.astype(BF16)
    low = (value - high.astype(F32)).astype(BF16)
    return high, low


def dot(left, right):
    return jnp.dot(left, right, preferred_element_type=F32)


def triple_dot(left, high, low):
    left_high, left_low = split_pair(left)
    return dot(left_high, high) + (dot(left_low, high) + dot(left_high, low))


def forward_y_kernel(x_ref, high_ref, low_ref, twiddle_ref, out_ref):
    root = math.sqrt(0.5)
    part = [x_ref[:, FINE * a : FINE * (a + 1)] for a in range(COARSE)]
    s04, d04 = part[0] + part[4], part[0] - part[4]
    s26, d26 = part[2] + part[6], part[2] - part[6]
    s15, d15 = part[1] + part[5], part[1] - part[5]
    s37, d37 = part[3] + part[7], part[3] - part[7]
    even, odd = s04 + s26, s15 + s37
    minus, plus = root * (d15 - d37), root * (d15 + d37)
    sums = [
        (even + odd, None),
        (d04 + minus, -(d26 + plus)),
        (s04 - s26, s37 - s15),
        (d04 - minus, d26 - plus),
        (even - odd, None),
    ]
    flat = out_ref.reshape(DEVICES * COARSE, LANES)
    lane = lax.broadcasted_iota(jnp.int32, (X_ROWS, LANES), 1)
    half = DEVICES // 2

    def emit(real, imag, k1):
        block = jnp.concatenate([real, imag], axis=0).T
        flat[pl.ds(k1, half, stride=COARSE), :] = block[:half]
        flat[pl.ds(half * COARSE + COARSE - 1 - k1, half, stride=COARSE), :] = block[half:]

    for k in range(5):
        real, imag = sums[k]
        if k > 0:
            cosine = twiddle_ref[2 * k - 2 : 2 * k - 1, :]
            sine = twiddle_ref[2 * k - 1 : 2 * k, :]
            if imag is None:
                real, imag = real * cosine, real * sine
            else:
                real, imag = real * cosine - imag * sine, real * sine + imag * cosine
        if k == 0:
            out = triple_dot(real, high_ref[:FINE, : 2 * LANES], low_ref[:FINE, : 2 * LANES])
            sign = 1.0 - 2.0 * (lax.broadcasted_iota(jnp.int32, (X_ROWS, FINE), 1) % 2).astype(F32)
            nyquist = jnp.sum(real * sign, axis=1, keepdims=True)
            emit(out[:, :LANES], jnp.where(lane == 0, nyquist, out[:, LANES:]), 0)
        elif k == 4:
            out = triple_dot(
                jnp.concatenate([real, imag], axis=1), high_ref[:, : 2 * LANES], low_ref[:, : 2 * LANES]
            )
            emit(out[:, :LANES], out[:, LANES:], 4)
        else:
            out = triple_dot(jnp.concatenate([real, imag], axis=1), high_ref[...], low_ref[...])
            emit(out[:, :LANES], out[:, LANES : 2 * LANES], k)
            emit(out[:, 2 * LANES : 3 * LANES], out[:, 3 * LANES :], COARSE - k)


def relayout_kernel(flag_ref, kernel_ref, out_ref, rows_ref, columns_ref):
    mirrored = flag_ref[0] > 0
    n_ops = kernel_ref.shape[0] // 16
    first = pl.program_id(0) * n_ops
    sub = lax.broadcasted_iota(jnp.int32, (COARSE, CELLS), 0)
    for op in range(n_ops):
        low = kernel_ref[16 * op : 16 * op + 8, :]
        high = kernel_ref[16 * op + 8 : 16 * op + 16, :]
        moved = jnp.where(sub < 7, pltpu.roll(low, 7, 0), pltpu.roll(high, 7, 0))
        part = (first + op) % PARTS
        odd = jnp.logical_or(part == 3, part == 5)
        sign = jnp.where(odd, -1.0, 1.0).astype(F32)
        rows_ref[8 * op : 8 * op + 8, :] = jnp.where(mirrored, moved * sign, low)
    for tile in range(CELLS // LANES):
        block = rows_ref[:, LANES * tile : LANES * (tile + 1)].T
        columns_ref[LANES * tile : LANES * (tile + 1), : 8 * n_ops] = block

    def step(p1, carry):
        column = columns_ref[pl.ds(p1, X_ROWS, stride=ROWS), :]
        both = jnp.concatenate([column, column], axis=0).T
        out_ref[p1] = both[: 8 * n_ops]
        return carry

    lax.fori_loop(0, ROWS, step, 0, unroll=4)


def spectral_kernel(
    x_ref,
    kernel_hbm,
    delta_ref,
    twiddle_ref,
    back_twiddle_ref,
    table_ref,
    back_table_ref,
    out_ref,
    kernel_ref,
    extra_ref,
    sums_ref,
    pair_ref,
    spec_ref,
    fix_ref,
    kernel_sem,
):
    fetch = pltpu.make_async_copy(kernel_hbm, kernel_ref, kernel_sem)
    fetch.start()
    half = ROWS // 2
    lane = lax.broadcasted_iota(jnp.int32, (ROWS, LANES), 1)

    extra_ref[...] = jnp.zeros_like(extra_ref)
    for layer in range(LAYERS):
        for comp in range(COMPS):
            line = x_ref[pl.ds(layer * ROWS * SLOT + comp * COARSE, ROWS, stride=SLOT), :]
            extra_ref[pl.ds(comp * LAYERS + layer, ROWS, stride=EXTRA), :] = jnp.where(lane < X_ROWS, 0.0, line)
    fix_ref[...] = jnp.zeros_like(fix_ref)

    def store_sums(values, place):
        cos_out, sin_out = real_dft(values)
        for k in range(half + 1):
            sums_ref[pl.ds(k * P1_ALL + place, COARSE), :] = cos_out[k]
        for k in range(1, half):
            sums_ref[pl.ds((half + k) * P1_ALL + place, COARSE), :] = sin_out[k]

    def over_rows(index, carry):
        layer = index // COMPS
        comp = index % COMPS
        base = layer * (ROWS * SLOT) + comp * COARSE
        base = pl.multiple_of(base, COARSE)
        values = [x_ref[pl.ds(base + r * SLOT, COARSE), :] for r in range(ROWS)]
        store_sums(values, pl.multiple_of(index * COARSE, COARSE))
        return carry

    lax.fori_loop(0, LAYERS * COMPS, over_rows, 0)
    for group in range(2):
        values = [extra_ref[r * EXTRA + group * 8 : r * EXTRA + group * 8 + 8, :] for r in range(ROWS)]
        store_sums(values, P1_ROWS + group * 8)

    def factors(ref, p1, kind):
        base = kind * (ROWS * 4) + p1 * 4
        return [ref[pl.ds(base + j, 1), :] for j in range(4)]

    def save_pair(row, value):
        high, low = split_pair(value)
        pair_ref[pl.ds(row, value.shape[0]), :LANES] = high
        pair_ref[pl.ds(row, value.shape[0]), LANES:] = low

    kinds = [1 if j % COMPS == 2 else 0 for j in range(LAYERS * COMPS)] + [0, 1]

    def blocks(ref, row, count):
        return [ref[pl.ds(row + COARSE * j, COARSE), :] for j in range(count)]

    def twist(k, p1_list, with_sin):
        cos_rows = blocks(sums_ref, pl.multiple_of(k * P1_ALL, COARSE), len(kinds))
        cos_swap = [pltpu.roll(v, X_ROWS, 1) for v in cos_rows]
        if with_sin:
            sin_rows = blocks(sums_ref, pl.multiple_of((half + k) * P1_ALL, COARSE), len(kinds))
            sin_swap = [pltpu.roll(v, X_ROWS, 1) for v in sin_rows]
        for p1 in p1_list:
            table = [factors(twiddle_ref, p1, kind) for kind in range(2)]
            out = []
            for j, kind in enumerate(kinds):
                f = table[kind]
                value = cos_rows[j] * f[0] + cos_swap[j] * f[1]
                if with_sin:
                    value = value + (sin_rows[j] * f[2] + sin_swap[j] * f[3])
                out.append(value)
            for j in range(0, len(kinds), 2):
                row = p1 * P1_ALL + COARSE * j
                save_pair(pl.multiple_of(row, 2 * COARSE), jnp.concatenate(out[j : j + 2], axis=0))

    twist(0, [0], False)
    twist(half, [half], False)

    def twist_step(k, carry):
        twist(k, [k, ROWS - k], True)
        return carry

    lax.fori_loop(1, half, twist_step, 0)

    def forward_dot(step, carry):
        rows = 4 * P1_ALL
        base = pl.multiple_of(step * rows, 2 * COARSE)
        both = dot(pair_ref[pl.ds(base, rows), :], table_ref[...])
        spec_ref[pl.ds(base, rows), :] = both[:, :LANES] + both[:, LANES:]
        return carry

    lax.fori_loop(0, ROWS // 4, forward_dot, 0)
    fetch.wait()

    def mix(spectra, coefficient):
        fields = []
        for target in range(LAYERS):
            total = [None, None, None]

            def add(comp, term):
                total[comp] = term if total[comp] is None else total[comp] + term

            for source in range(LAYERS):
                offset = target - source + LAYERS - 1
                k = [coefficient(offset * PARTS + j) for j in range(PARTS)]
                mx, my, mz = spectra[source]
                add(0, k[0] * mx + k[3] * my + k[4] * mz)
                add(1, k[3] * mx + k[1] * my + k[5] * mz)
                add(2, k[4] * mx + k[5] * my - k[2] * mz)
            fields.append(total)
        return fields

    def fix_step(group, carry):
        base = group * COARSE
        spectra = [
            [
                spec_ref[pl.ds(base * P1_ALL + P1_ROWS + comp * LAYERS + source, COARSE, stride=P1_ALL), :]
                for comp in range(COMPS)
            ]
            for source in range(LAYERS)
        ]

        def coefficient(op):
            return delta_ref[pl.ds(pl.multiple_of(op * ROWS + base, COARSE), COARSE), :]

        fields = mix(spectra, coefficient)
        for target in range(LAYERS):
            for comp in range(COMPS):
                row = base * P1_ROWS + (target * COMPS + comp) * COARSE
                fix_ref[pl.ds(row, COARSE, stride=P1_ROWS), :] = fields[target][comp]
        return carry

    lax.fori_loop(0, ROWS // COARSE, fix_step, 0)

    def mix_step(p1, carry):
        base = pl.multiple_of(p1 * P1_ALL, COARSE)
        lines = blocks(spec_ref, base, LAYERS * COMPS)
        spectra = [lines[COMPS * s : COMPS * s + COMPS] for s in range(LAYERS)]
        kernel_base = pl.multiple_of(p1 * (OPS * COARSE), COARSE)

        def coefficient(op):
            return kernel_ref[pl.ds(kernel_base + op * COARSE, COARSE), :]

        fields = mix(spectra, coefficient)
        flat = [fields[j // COMPS][j % COMPS] for j in range(LAYERS * COMPS)]
        row = pl.multiple_of(p1 * P1_ROWS, 2 * COARSE)
        fixes = blocks(fix_ref, row, LAYERS * COMPS)
        flat = [a + b for a, b in zip(flat, fixes)]
        for j in range(0, LAYERS * COMPS, 2):
            save_pair(row + COARSE * j, jnp.concatenate(flat[j : j + 2], axis=0))
        return carry

    lax.fori_loop(0, ROWS, mix_step, 0)

    def backward_dot(step, carry):
        rows = 4 * P1_ROWS
        base = pl.multiple_of(step * rows, 2 * COARSE)
        both = dot(pair_ref[pl.ds(base, rows), :], back_table_ref[...])
        spec_ref[pl.ds(base, rows), :] = both[:, :LANES] + both[:, LANES:]
        return carry

    lax.fori_loop(0, ROWS // 4, backward_dot, 0)

    count = LAYERS * COMPS

    def untwist_edge(p1, slot):
        table = [factors(back_twiddle_ref, p1, kind) for kind in range(2)]
        for j, value in enumerate(blocks(spec_ref, p1 * P1_ROWS, count)):
            f = table[kinds[j]]
            sums_ref[pl.ds(slot * P1_ROWS + COARSE * j, COARSE), :] = value * f[0] + pltpu.roll(value, X_ROWS, 1) * f[1]

    untwist_edge(0, 0)
    untwist_edge(half, half)

    def untwist_step(k, carry):
        near = [factors(back_twiddle_ref, k, kind) for kind in range(2)]
        far = [factors(back_twiddle_ref, ROWS - k, kind) for kind in range(2)]
        near_rows = blocks(spec_ref, pl.multiple_of(k * P1_ROWS, COARSE), count)
        far_rows = blocks(spec_ref, pl.multiple_of((ROWS - k) * P1_ROWS, COARSE), count)
        cos_base = pl.multiple_of(k * P1_ROWS, COARSE)
        sin_base = pl.multiple_of((half + k) * P1_ROWS, COARSE)
        for j in range(count):
            n, f = near[kinds[j]], far[kinds[j]]
            a, b = near_rows[j], far_rows[j]
            a_swap, b_swap = pltpu.roll(a, X_ROWS, 1), pltpu.roll(b, X_ROWS, 1)
            sums_ref[pl.ds(cos_base + COARSE * j, COARSE), :] = (a * n[0] + a_swap * n[1]) + (b * f[0] + b_swap * f[1])
            sums_ref[pl.ds(sin_base + COARSE * j, COARSE), :] = (a * n[2] + a_swap * n[3]) + (b * f[2] + b_swap * f[3])
        return carry

    lax.fori_loop(1, half, untwist_step, 0)

    def back_rows(index, carry):
        place = pl.multiple_of(index * COARSE, COARSE)
        cos_in = [sums_ref[pl.ds(k * P1_ROWS + place, COARSE), :] for k in range(half + 1)]
        sin_in = [None] + [sums_ref[pl.ds((half + k) * P1_ROWS + place, COARSE), :] for k in range(1, half)] + [None]
        values = real_sum(cos_in, sin_in, ROWS)
        layer = index // COMPS
        comp = index % COMPS
        base = pl.multiple_of(layer * (ROWS * SLOT) + comp * COARSE, COARSE)
        for r in range(ROWS):
            out_ref[pl.ds(base + r * SLOT, COARSE), :] = values[r]
        return carry

    lax.fori_loop(0, LAYERS * COMPS, back_rows, 0)


def inverse_y_kernel(x_ref, high_ref, low_ref, first_high_ref, first_low_ref, twiddle_ref, out_ref):
    flat = x_ref.reshape(DEVICES * COARSE, LANES)
    half = DEVICES // 2

    def take(k1):
        near = flat[pl.ds(k1, half, stride=COARSE), :]
        far = flat[pl.ds(half * COARSE + COARSE - 1 - k1, half, stride=COARSE), :]
        block = jnp.concatenate([near, far], axis=0).T
        return [block[:X_ROWS], block[X_ROWS:]]

    cos_in = [None] * 5
    sin_in = [None] * 5
    for k in range(5):
        if k == 0:
            left = jnp.concatenate(take(0), axis=1)
            cos_in[0] = triple_dot(left, first_high_ref[...], first_low_ref[...])
            continue
        cosine = twiddle_ref[2 * k - 2 : 2 * k - 1, :]
        sine = twiddle_ref[2 * k - 1 : 2 * k, :]
        if k == 4:
            left = jnp.concatenate(take(4), axis=1)
            both = triple_dot(left, high_ref[: 2 * LANES, :], low_ref[: 2 * LANES, :])
            cos_in[4] = both[:, :FINE] * cosine - both[:, FINE:] * sine
            continue
        left = jnp.concatenate(take(k) + take(COARSE - k), axis=1)
        both = triple_dot(left, high_ref[...], low_ref[...])
        cos_in[k] = both[:, :FINE] * cosine - both[:, FINE:] * sine
        sin_in[k] = -(both[:, :FINE] * sine + both[:, FINE:] * cosine)
    values = real_sum(cos_in, sin_in, COARSE)
    for a in range(COARSE):
        out_ref[:, FINE * a : FINE * (a + 1)] = values[a]


def whole(shape):
    rank = len(shape)
    return pl.BlockSpec(shape, lambda *_: (0,) * rank)


def params():
    return pltpu.CompilerParams(vmem_limit_bytes=48 * 1024 * 1024)


def forward_y(field):
    high, low = halves(fine_table())
    twiddle = y_twiddle(-1.0, 1.0)
    return pl.pallas_call(
        forward_y_kernel,
        grid=(COMPS,),
        in_specs=[
            pl.BlockSpec((X_ROWS, CELLS), lambda c: (c, 0)),
            whole(high.shape),
            whole(low.shape),
            whole(twiddle.shape),
        ],
        out_specs=pl.BlockSpec((DEVICES, COARSE, LANES), lambda c: (0, c, 0)),
        out_shape=jax.ShapeDtypeStruct((DEVICES, SLOT, LANES), F32),
        compiler_params=params(),
        name="forward_y",
    )(field, jnp.asarray(high), jnp.asarray(low), jnp.asarray(twiddle))


def relayout(kernel, flag):
    groups = 3
    rows = OPS // groups * 16
    out_rows = OPS // groups * COARSE
    return pl.pallas_call(
        relayout_kernel,
        grid=(groups,),
        in_specs=[
            pl.BlockSpec(memory_space=pltpu.SMEM),
            pl.BlockSpec((rows, CELLS), lambda g: (g, 0)),
        ],
        out_specs=pl.BlockSpec((ROWS, out_rows, LANES), lambda g: (0, g, 0)),
        out_shape=jax.ShapeDtypeStruct((ROWS, OPS * COARSE, LANES), F32),
        scratch_shapes=[pltpu.VMEM((out_rows, CELLS), F32), pltpu.VMEM((CELLS, LANES), F32)],
        compiler_params=params(),
        name="relayout",
    )(flag, kernel)


def spectral(lines, kernel, delta):
    twiddle = x_twiddle(-1.0, 1.0)
    back_twiddle = x_twiddle(1.0, -1.0 / (CELLS * CELLS))
    table = x_table(-1.0)
    back_table = x_table(1.0)
    total = DEVICES * SLOT
    return pl.pallas_call(
        spectral_kernel,
        in_specs=[
            whole((total, LANES)),
            pl.BlockSpec(memory_space=pl.ANY),
            whole(delta.shape),
            whole(twiddle.shape),
            whole(back_twiddle.shape),
            whole(table.shape),
            whole(back_table.shape),
        ],
        out_specs=whole((total, LANES)),
        grid=(1,),
        out_shape=jax.ShapeDtypeStruct((total, LANES), F32),
        scratch_shapes=[
            pltpu.VMEM((ROWS * OPS * COARSE, LANES), F32),
            pltpu.VMEM((ROWS * EXTRA, LANES), F32),
            pltpu.VMEM((ROWS * P1_ALL, LANES), F32),
            pltpu.VMEM((ROWS * P1_ALL, 2 * LANES), BF16),
            pltpu.VMEM((ROWS * P1_ALL, LANES), F32),
            pltpu.VMEM((ROWS * P1_ROWS, LANES), F32),
            pltpu.SemaphoreType.DMA,
        ],
        compiler_params=params(),
        name="spectral",
    )(
        lines,
        kernel,
        delta,
        jnp.asarray(twiddle),
        jnp.asarray(back_twiddle),
        jnp.asarray(table),
        jnp.asarray(back_table),
    )


def inverse_y(spectra):
    high, low = halves(fine_table().T)
    first_high, first_low = halves(closing_table())
    twiddle = y_twiddle(1.0, 2.0)
    return pl.pallas_call(
        inverse_y_kernel,
        grid=(COMPS,),
        in_specs=[
            pl.BlockSpec((DEVICES, COARSE, LANES), lambda c: (0, c, 0)),
            whole(high.shape),
            whole(low.shape),
            whole(first_high.shape),
            whole(first_low.shape),
            whole(twiddle.shape),
        ],
        out_specs=pl.BlockSpec((X_ROWS, CELLS), lambda c: (c, 0)),
        out_shape=jax.ShapeDtypeStruct((COMPS * X_ROWS, CELLS), F32),
        compiler_params=params(),
        name="inverse_y",
    )(
        spectra,
        jnp.asarray(high),
        jnp.asarray(low),
        jnp.asarray(first_high),
        jnp.asarray(first_low),
        jnp.asarray(twiddle),
    )


def local(magnet, kernel):
    axes = ("layer", "row")
    device = lax.axis_index(axes)
    field = magnet.reshape(COMPS * X_ROWS, CELLS)
    flag = (device >= DEVICES // 2).astype(jnp.int32).reshape(1)
    edge = kernel[:, :, 0, :].reshape(OPS, CELLS)
    middle = lax.ppermute(edge, axes, [(DEVICES // 2, 0)])
    sent = forward_y(field)
    got = lax.all_to_all(sent, axes, 0, 0, tiled=True)
    coefficient = relayout(kernel.reshape(OPS * 16, CELLS), flag)
    delta = jnp.where(device == 0, middle - edge, 0.0)
    delta = jnp.swapaxes(delta.reshape(OPS, X_ROWS, ROWS), 1, 2)
    delta = jnp.concatenate([delta, delta], axis=2).reshape(OPS * ROWS, LANES)
    fields = spectral(
        got.reshape(DEVICES * SLOT, LANES), coefficient.reshape(ROWS * OPS * COARSE, LANES), delta
    )
    back = lax.all_to_all(fields.reshape(DEVICES, SLOT, LANES), axes, 0, 0, tiled=True)
    result = inverse_y(back)
    return result.reshape(COMPS, 1, X_ROWS, CELLS)


def solution(mesh):
    in_specs = (P(None, "layer", "row", None), P(None, None, ("layer", "row"), None))
    out_specs = P(None, "layer", "row", None)
    return jax.shard_map(local, mesh=mesh, in_specs=in_specs, out_specs=out_specs, check_vma=False)
```

```python
import math

import jax
import jax.numpy as jnp
import numpy as np
from jax import lax
from jax.experimental import pallas as pl
from jax.experimental.pallas import tpu as pltpu
from jax.sharding import PartitionSpec as P

CELLS = 2048
COMPS = 3
LAYERS = 4
ROWS = 32
X_ROWS = 64
DEVICES = 128
PARTS = 6
OFFSETS = 7
OPS = OFFSETS * PARTS
FINE = 128
COARSE = 16
OWNED = 8
SLOT = COMPS * OWNED
LANES = 128
EXTRA = 16
P1_ROWS = LAYERS * COMPS * OWNED
P1_ALL = P1_ROWS + EXTRA

F32 = jnp.float32
BF16 = jnp.bfloat16


def halves(table):
    high = np.asarray(table, np.float32).astype(jnp.bfloat16)
    low = (np.asarray(table, np.float64) - high.astype(np.float64)).astype(np.float32).astype(jnp.bfloat16)
    return high, low


def fine_table():
    index = np.arange(FINE)
    angle = 2.0 * np.pi * (np.outer(index, index) % FINE) / FINE
    return np.block([[np.cos(angle), -np.sin(angle)], [np.sin(angle), np.cos(angle)]])


def stacked(table):
    return np.concatenate(halves(table), axis=0)


def y_twiddle(sign, scale):
    k = np.arange(1, COARSE // 2 + 1)[:, None]
    b = np.arange(FINE)[None, :]
    angle = 2.0 * np.pi * k * b / CELLS
    table = scale * np.stack([np.cos(angle), sign * np.sin(angle)], axis=1)
    return table.reshape(COARSE, FINE).astype(np.float32)


def lane_pair(coefficient):
    real = np.concatenate([coefficient.real, coefficient.real], axis=-1)
    imag = np.concatenate([-coefficient.imag, coefficient.imag], axis=-1)
    return real, imag


def x_twiddle(sign, scale):
    p1 = np.arange(ROWS)[:, None]
    t = np.arange(X_ROWS)[None, :]
    base = scale * np.exp(sign * 2.0j * np.pi * (p1 * t) / CELLS)
    side = np.where(p1 <= ROWS // 2, 1.0, -1.0) * (sign * 1.0j)
    kinds = []
    for kind in (1.0, 1.0j):
        first = lane_pair(kind * base)
        second = lane_pair(kind * base * side)
        kinds.append(np.stack(first + second, axis=1))
    return np.stack(kinds).astype(np.float32).reshape(2 * ROWS * 4, LANES)


def x_table(sign):
    index = np.arange(X_ROWS)
    angle = 2.0 * np.pi * (np.outer(index, index) % X_ROWS) / X_ROWS
    real = np.cos(angle)
    imag = sign * np.sin(angle)
    whole = np.block([[real, imag], [-imag, real]])
    high, low = halves(whole)
    line = np.concatenate([high, low], axis=1)
    return np.concatenate([line, line], axis=0)


def real_dft(values):
    n = len(values)
    if n == 1:
        return [values[0]], [None]
    if n == 2:
        return [values[0] + values[1], values[0] - values[1]], [None, None]
    even_c, even_s = real_dft(values[0::2])
    odd_c, odd_s = real_dft(values[1::2])
    half = n // 2
    quarter = n // 4
    cos_out = [None] * (half + 1)
    sin_out = [None] * (half + 1)
    for k in range(quarter + 1):
        if k == 0:
            cos_out[0] = even_c[0] + odd_c[0]
            cos_out[half] = even_c[0] - odd_c[0]
        elif k == quarter:
            cos_out[k] = even_c[k]
            sin_out[k] = odd_c[k]
        else:
            theta = 2.0 * math.pi * k / n
            cosine, sine = math.cos(theta), math.sin(theta)
            if 8 * k == n:
                real = cosine * (odd_c[k] - odd_s[k])
                imag = cosine * (odd_s[k] + odd_c[k])
            else:
                real = cosine * odd_c[k] - sine * odd_s[k]
                imag = cosine * odd_s[k] + sine * odd_c[k]
            cos_out[k] = even_c[k] + real
            sin_out[k] = even_s[k] + imag
            cos_out[half - k] = even_c[k] - real
            sin_out[half - k] = imag - even_s[k]
    return cos_out, sin_out


def real_sum(cos_in, sin_in, n):
    if n == 1:
        return [cos_in[0]]
    half = n // 2
    if n == 2:
        return [cos_in[0] + cos_in[1], cos_in[0] - cos_in[1]]
    quarter = n // 4
    even_c = [None] * (quarter + 1)
    even_s = [None] * (quarter + 1)
    odd_c = [None] * (quarter + 1)
    odd_s = [None] * (quarter + 1)
    even_c[0] = cos_in[0] + cos_in[half]
    odd_c[0] = cos_in[0] - cos_in[half]
    even_c[quarter] = cos_in[quarter]
    odd_c[quarter] = sin_in[quarter]
    for k in range(1, quarter):
        theta = 2.0 * math.pi * k / n
        cosine, sine = math.cos(theta), math.sin(theta)
        even_c[k] = cos_in[k] + cos_in[half - k]
        even_s[k] = sin_in[k] - sin_in[half - k]
        gap = cos_in[k] - cos_in[half - k]
        both = sin_in[k] + sin_in[half - k]
        if 8 * k == n:
            odd_c[k] = cosine * (gap + both)
            odd_s[k] = cosine * (both - gap)
        else:
            odd_c[k] = cosine * gap + sine * both
            odd_s[k] = cosine * both - sine * gap
    evens = real_sum(even_c, even_s, half)
    odds = real_sum(odd_c, odd_s, half)
    out = [None] * n
    out[0::2] = evens
    out[1::2] = odds
    return out


def split_pair(value):
    high = value.astype(BF16)
    low = (value - high.astype(F32)).astype(BF16)
    return high, low


def dot(left, right):
    return jnp.dot(left, right, preferred_element_type=F32)


def triple_dot(high, low, table_ref):
    size = table_ref.shape[0] // 2
    table_high, table_low = table_ref[:size, :], table_ref[size:, :]
    left = jnp.concatenate([high, low, high], axis=1)
    return dot(left, jnp.concatenate([table_high, table_high, table_low], axis=0))


def slot_rows(comp, k1):
    half = DEVICES // 2
    near = pl.ds(comp * OWNED + k1, half, stride=SLOT)
    far = pl.ds(half * SLOT + comp * OWNED + k1 - 1, half, stride=SLOT)
    return near, far


def forward_y_kernel(x_ref, table_ref, twiddle_ref, out_ref, high_ref, low_ref):
    half = DEVICES // 2
    middle = COARSE // 2
    group = 16
    lane = lax.broadcasted_iota(jnp.int32, (X_ROWS, LANES), 1)
    alternate = 1.0 - 2.0 * (lax.broadcasted_iota(jnp.int32, (X_ROWS, FINE), 1) % 2).astype(F32)
    for comp in range(COMPS):
        base = comp * (middle + 1) * X_ROWS
        nyquist = []
        for g in range(X_ROWS // group):
            top = comp * X_ROWS + g * group
            parts = [x_ref[top : top + group, FINE * a : FINE * (a + 1)] for a in range(COARSE)]
            cos_out, sin_out = real_dft(parts)
            nyquist.append(jnp.sum(cos_out[0] * alternate[:group], axis=1, keepdims=True))
            for k in range(middle + 1):
                rows = slice(base + k * X_ROWS + g * group, base + k * X_ROWS + (g + 1) * group)
                real = cos_out[k]
                imag = None
                if k > 0:
                    cosine = twiddle_ref[2 * k - 2 : 2 * k - 1, :]
                    sine = twiddle_ref[2 * k - 1 : 2 * k, :]
                    if k == middle:
                        real, imag = real * cosine, real * sine
                    else:
                        real, imag = real * cosine + sin_out[k] * sine, real * sine - sin_out[k] * cosine
                high_ref[rows, :LANES], low_ref[rows, :LANES] = split_pair(real)
                if imag is None:
                    zero = jnp.zeros((group, LANES), BF16)
                    high_ref[rows, LANES:], low_ref[rows, LANES:] = zero, zero
                else:
                    high_ref[rows, LANES:], low_ref[rows, LANES:] = split_pair(imag)
        size = (middle + 1) * X_ROWS
        out = triple_dot(high_ref[base : base + size, :], low_ref[base : base + size, :], table_ref)

        def pick(k):
            rows = out[k * X_ROWS : (k + 1) * X_ROWS]
            return rows[:, :LANES], rows[:, LANES:]

        for k in range(middle):
            real, imag = pick(k)
            if k == 0:
                last_real, last_imag = pick(middle)
                imag = jnp.where(lane == 0, jnp.concatenate(nyquist, axis=0), imag)
                real = jnp.where(lane < half, real, last_real)
                imag = jnp.where(lane < half, imag, last_imag)
            block = jnp.concatenate([real, imag], axis=0).T
            near, far = slot_rows(comp, k)
            if k == 0:
                far = slot_rows(comp, middle)[1]
            out_ref[near, :] = block[:half]
            out_ref[far, :] = block[half:]


def relayout_kernel(flag_ref, kernel_ref, out_ref, rows_ref, columns_ref):
    shifted = flag_ref[0] > 0
    n_ops = kernel_ref.shape[0] // 16
    sub = lax.broadcasted_iota(jnp.int32, (OWNED, CELLS), 0)
    for op in range(n_ops):
        low = kernel_ref[16 * op : 16 * op + 8, :]
        high = kernel_ref[16 * op + 8 : 16 * op + 16, :]
        moved = jnp.where(sub < 7, pltpu.roll(low, 7, 0), pltpu.roll(high, 7, 0))
        rows_ref[8 * op : 8 * op + 8, :] = jnp.where(shifted, moved, low)
    for tile in range(CELLS // LANES):
        block = rows_ref[:, LANES * tile : LANES * (tile + 1)].T
        columns_ref[LANES * tile : LANES * (tile + 1), : 8 * n_ops] = block

    def step(p1, carry):
        column = columns_ref[pl.ds(p1, X_ROWS, stride=ROWS), :]
        both = jnp.concatenate([column, column], axis=0).T
        out_ref[p1] = both[: 8 * n_ops]
        return carry

    lax.fori_loop(0, ROWS, step, 0, unroll=4)


def spectral_kernel(
    x_ref,
    kernel_hbm,
    delta_ref,
    twiddle_ref,
    back_twiddle_ref,
    table_ref,
    back_table_ref,
    out_ref,
    kernel_ref,
    extra_ref,
    sums_ref,
    pair_ref,
    spec_ref,
    fix_ref,
    back_ref,
    kernel_sem,
):
    fetch = pltpu.make_async_copy(kernel_hbm, kernel_ref, kernel_sem)
    fetch.start()
    half = ROWS // 2
    lane = lax.broadcasted_iota(jnp.int32, (ROWS, LANES), 1)

    extra_ref[...] = jnp.zeros_like(extra_ref)
    for layer in range(LAYERS):
        for comp in range(COMPS):
            line = x_ref[pl.ds(layer * ROWS * SLOT + comp * OWNED, ROWS, stride=SLOT), :]
            extra_ref[pl.ds(comp * LAYERS + layer, ROWS, stride=EXTRA), :] = jnp.where(lane < X_ROWS, 0.0, line)
    fix_ref[...] = jnp.zeros_like(fix_ref)

    def store_sums(values, place):
        cos_out, sin_out = real_dft(values)
        for k in range(half + 1):
            sums_ref[pl.ds(k * P1_ALL + place, OWNED), :] = cos_out[k]
        for k in range(1, half):
            sums_ref[pl.ds((half + k) * P1_ALL + place, OWNED), :] = sin_out[k]

    def over_rows(index, carry):
        layer = index // COMPS
        comp = index % COMPS
        base = layer * (ROWS * SLOT) + comp * OWNED
        base = pl.multiple_of(base, OWNED)
        values = [x_ref[pl.ds(base + r * SLOT, OWNED), :] for r in range(ROWS)]
        store_sums(values, pl.multiple_of(index * OWNED, OWNED))
        return carry

    lax.fori_loop(0, LAYERS * COMPS, over_rows, 0)
    for group in range(2):
        values = [extra_ref[r * EXTRA + group * 8 : r * EXTRA + group * 8 + 8, :] for r in range(ROWS)]
        store_sums(values, P1_ROWS + group * 8)

    def factors(ref, p1, kind):
        base = kind * (ROWS * 4) + p1 * 4
        return [ref[pl.ds(base + j, 1), :] for j in range(4)]

    def save_pair(row, value):
        high, low = split_pair(value)
        pair_ref[pl.ds(row, value.shape[0]), :LANES] = high
        pair_ref[pl.ds(row, value.shape[0]), LANES:] = low

    kinds = [1 if j % COMPS == 2 else 0 for j in range(LAYERS * COMPS)] + [0, 1]

    def blocks(ref, row, count):
        return [ref[pl.ds(row + OWNED * j, OWNED), :] for j in range(count)]

    def twist(k, p1_list, with_sin):
        cos_rows = blocks(sums_ref, pl.multiple_of(k * P1_ALL, OWNED), len(kinds))
        cos_swap = [pltpu.roll(v, X_ROWS, 1) for v in cos_rows]
        if with_sin:
            sin_rows = blocks(sums_ref, pl.multiple_of((half + k) * P1_ALL, OWNED), len(kinds))
            sin_swap = [pltpu.roll(v, X_ROWS, 1) for v in sin_rows]
        for place, p1 in enumerate(p1_list):
            table = [factors(twiddle_ref, p1, kind) for kind in range(2)]
            out = []
            for j, kind in enumerate(kinds):
                f = table[kind]
                value = cos_rows[j] * f[0] + cos_swap[j] * f[1]
                if with_sin:
                    value = value + (sin_rows[j] * f[2] + sin_swap[j] * f[3])
                out.append(value)
            for j in range(0, len(kinds), 2):
                row = 2 * k * P1_ALL + place * P1_ALL + OWNED * j
                save_pair(pl.multiple_of(row, 2 * OWNED), jnp.concatenate(out[j : j + 2], axis=0))

    def forward_dot(k, first, second):
        rows = 2 * P1_ALL
        base = k * rows if isinstance(k, int) else pl.multiple_of(k * rows, 2 * OWNED)
        both = dot(pair_ref[pl.ds(base, rows), :], table_ref[...])
        whole_line = both[:, :LANES] + both[:, LANES:]
        spec_ref[pl.ds(first * P1_ALL, P1_ALL), :] = whole_line[:P1_ALL]
        spec_ref[pl.ds(second * P1_ALL, P1_ALL), :] = whole_line[P1_ALL:]

    twist(0, [0], False)
    cos_edge = blocks(sums_ref, half * P1_ALL, len(kinds))
    table = [factors(twiddle_ref, half, kind) for kind in range(2)]
    edge = [v * table[kind][0] + pltpu.roll(v, X_ROWS, 1) * table[kind][1] for v, kind in zip(cos_edge, kinds)]
    for j in range(0, len(kinds), 2):
        save_pair(P1_ALL + OWNED * j, jnp.concatenate(edge[j : j + 2], axis=0))
    forward_dot(0, 0, half)
    twist(1, [1, ROWS - 1], True)

    def twist_step(k, carry):
        forward_dot(k - 1, k - 1, ROWS + 1 - k)
        twist(k, [k, ROWS - k], True)
        return carry

    lax.fori_loop(2, half, twist_step, 0)
    forward_dot(half - 1, half - 1, half + 1)
    fetch.wait()

    def mix(spectra, coefficient):
        fields = []
        for target in range(LAYERS):
            total = [None, None, None]

            def add(comp, term):
                total[comp] = term if total[comp] is None else total[comp] + term

            for source in range(LAYERS):
                offset = target - source + LAYERS - 1
                k = [coefficient(offset * PARTS + j) for j in range(PARTS)]
                mx, my, mz = spectra[source]
                add(0, k[0] * mx + k[3] * my + k[4] * mz)
                add(1, k[3] * mx + k[1] * my + k[5] * mz)
                add(2, k[4] * mx + k[5] * my - k[2] * mz)
            fields.append(total)
        return fields

    def fix_step(group, carry):
        base = group * OWNED
        spectra = [
            [
                spec_ref[pl.ds(base * P1_ALL + P1_ROWS + comp * LAYERS + source, OWNED, stride=P1_ALL), :]
                for comp in range(COMPS)
            ]
            for source in range(LAYERS)
        ]

        def coefficient(op):
            return delta_ref[pl.ds(pl.multiple_of(op * ROWS + base, OWNED), OWNED), :]

        fields = mix(spectra, coefficient)
        for target in range(LAYERS):
            for comp in range(COMPS):
                row = base * P1_ROWS + (target * COMPS + comp) * OWNED
                fix_ref[pl.ds(row, OWNED, stride=P1_ROWS), :] = fields[target][comp]
        return carry

    lax.fori_loop(0, ROWS // OWNED, fix_step, 0)

    def mix_line(p1):
        lines = blocks(spec_ref, p1 * P1_ALL, LAYERS * COMPS)
        spectra = [lines[COMPS * s : COMPS * s + COMPS] for s in range(LAYERS)]
        kernel_base = p1 * (OPS * OWNED)

        def coefficient(op):
            return kernel_ref[pl.ds(kernel_base + op * OWNED, OWNED), :]

        fields = mix(spectra, coefficient)
        flat = [fields[j // COMPS][j % COMPS] for j in range(LAYERS * COMPS)]
        row = p1 * P1_ROWS
        fixes = blocks(fix_ref, row, LAYERS * COMPS)
        flat = [a + b for a, b in zip(flat, fixes)]
        for j in range(0, LAYERS * COMPS, 2):
            save_pair(row + OWNED * j, jnp.concatenate(flat[j : j + 2], axis=0))

    def backward_dot(p1, rows):
        both = dot(pair_ref[pl.ds(p1 * P1_ROWS, rows), :], back_table_ref[...])
        back_ref[pl.ds(p1 * P1_ROWS, rows), :] = both[:, :LANES] + both[:, LANES:]

    mix_line(0)
    mix_line(1)

    def mix_step(step, carry):
        p1 = pl.multiple_of(2 * step, 2)
        backward_dot(p1 - 2, 2 * P1_ROWS)
        mix_line(p1)
        mix_line(p1 + 1)
        return carry

    lax.fori_loop(1, half, mix_step, 0)
    backward_dot(ROWS - 2, 2 * P1_ROWS)

    count = LAYERS * COMPS

    def untwist_edge(p1, slot):
        table = [factors(back_twiddle_ref, p1, kind) for kind in range(2)]
        for j, value in enumerate(blocks(back_ref, p1 * P1_ROWS, count)):
            f = table[kinds[j]]
            sums_ref[pl.ds(slot * P1_ROWS + OWNED * j, OWNED), :] = value * f[0] + pltpu.roll(value, X_ROWS, 1) * f[1]

    untwist_edge(0, 0)
    untwist_edge(half, half)

    def untwist_step(k, carry):
        near = [factors(back_twiddle_ref, k, kind) for kind in range(2)]
        far = [factors(back_twiddle_ref, ROWS - k, kind) for kind in range(2)]
        near_rows = blocks(back_ref, pl.multiple_of(k * P1_ROWS, OWNED), count)
        far_rows = blocks(back_ref, pl.multiple_of((ROWS - k) * P1_ROWS, OWNED), count)
        cos_base = pl.multiple_of(k * P1_ROWS, OWNED)
        sin_base = pl.multiple_of((half + k) * P1_ROWS, OWNED)
        for j in range(count):
            n, f = near[kinds[j]], far[kinds[j]]
            a, b = near_rows[j], far_rows[j]
            a_swap, b_swap = pltpu.roll(a, X_ROWS, 1), pltpu.roll(b, X_ROWS, 1)
            sums_ref[pl.ds(cos_base + OWNED * j, OWNED), :] = (a * n[0] + a_swap * n[1]) + (b * f[0] + b_swap * f[1])
            sums_ref[pl.ds(sin_base + OWNED * j, OWNED), :] = (a * n[2] + a_swap * n[3]) + (b * f[2] + b_swap * f[3])
        return carry

    lax.fori_loop(1, half, untwist_step, 0)

    def back_rows(index, carry):
        place = pl.multiple_of(index * OWNED, OWNED)
        cos_in = [sums_ref[pl.ds(k * P1_ROWS + place, OWNED), :] for k in range(half + 1)]
        sin_in = [None] + [sums_ref[pl.ds((half + k) * P1_ROWS + place, OWNED), :] for k in range(1, half)] + [None]
        values = real_sum(cos_in, sin_in, ROWS)
        layer = index // COMPS
        comp = index % COMPS
        base = pl.multiple_of(layer * (ROWS * SLOT) + comp * OWNED, OWNED)
        for r in range(ROWS):
            out_ref[pl.ds(base + r * SLOT, OWNED), :] = values[r]
        return carry

    lax.fori_loop(0, LAYERS * COMPS, back_rows, 0)


def inverse_y_kernel(x_ref, table_ref, twiddle_ref, out_hbm, high_ref, low_ref, lines_ref, result_ref, sem):
    half = DEVICES // 2
    middle = COARSE // 2
    group = 8
    lane = lax.broadcasted_iota(jnp.int32, (X_ROWS, LANES), 1)
    alternate = 1.0 - 2.0 * (lax.broadcasted_iota(jnp.int32, (group, FINE), 1) % 2).astype(F32)
    copies = []
    for comp in range(COMPS):
        size = (middle + 1) * X_ROWS
        base = comp * size

        def put(k, real, imag):
            rows = slice(base + k * X_ROWS, base + (k + 1) * X_ROWS)
            high_ref[rows, :LANES], low_ref[rows, :LANES] = split_pair(real)
            high_ref[rows, LANES:], low_ref[rows, LANES:] = split_pair(imag)

        for k in range(middle):
            near, far = slot_rows(comp, k)
            if k == 0:
                far = slot_rows(comp, middle)[1]
            block = jnp.concatenate([x_ref[near, :], x_ref[far, :]], axis=0).T
            real, imag = block[:X_ROWS], block[X_ROWS:]
            if k == 0:
                nyquist = imag[:, :1]
                put(middle, jnp.where(lane < half, 0.0, real), jnp.where(lane < half, 0.0, imag))
                scale = jnp.where(lane < half, jnp.where(lane == 0, 0.5, 1.0), 0.0)
                real, imag = real * scale, imag * scale
            put(k, real, imag)
        lines_ref[base : base + size, :] = triple_dot(
            high_ref[base : base + size, :], low_ref[base : base + size, :], table_ref
        )
        for g in range(X_ROWS // group):
            cos_in = [None] * (middle + 1)
            sin_in = [None] * (middle + 1)
            for k in range(middle + 1):
                rows = slice(base + k * X_ROWS + g * group, base + k * X_ROWS + (g + 1) * group)
                real = lines_ref[rows, :LANES]
                if k == 0:
                    cos_in[0] = 2.0 * real + nyquist[g * group : (g + 1) * group] * alternate
                    continue
                imag = lines_ref[rows, LANES:]
                cosine = twiddle_ref[2 * k - 2 : 2 * k - 1, :]
                sine = twiddle_ref[2 * k - 1 : 2 * k, :]
                cos_in[k] = real * cosine - imag * sine
                if k < middle:
                    sin_in[k] = -(real * sine + imag * cosine)
            values = real_sum(cos_in, sin_in, COARSE)
            top = comp * X_ROWS + g * group
            for a in range(COARSE):
                result_ref[top : top + group, FINE * a : FINE * (a + 1)] = values[a]
        span = pl.ds(comp * X_ROWS, X_ROWS)
        copy = pltpu.make_async_copy(result_ref.at[span], out_hbm.at[span], sem.at[comp])
        copy.start()
        copies.append(copy)
    for copy in copies:
        copy.wait()


VMEM = pl.BlockSpec(memory_space=pltpu.VMEM)
HBM = pl.BlockSpec(memory_space=pl.ANY)
FINE_ROWS = COMPS * (COARSE // 2 + 1) * X_ROWS


def params():
    return pltpu.CompilerParams(vmem_limit_bytes=48 * 1024 * 1024)


def forward_y(field):
    return pl.pallas_call(
        forward_y_kernel,
        in_specs=[VMEM] * 3,
        out_specs=VMEM,
        out_shape=jax.ShapeDtypeStruct((DEVICES * SLOT, LANES), F32),
        scratch_shapes=[pltpu.VMEM((FINE_ROWS, 2 * LANES), BF16)] * 2,
        compiler_params=params(),
        name="forward_y",
    )(field, jnp.asarray(stacked(fine_table())), jnp.asarray(y_twiddle(-1.0, 1.0)))


def relayout(kernel, flag):
    groups = 3
    rows = OPS // groups * 16
    out_rows = OPS // groups * OWNED
    return pl.pallas_call(
        relayout_kernel,
        grid=(groups,),
        in_specs=[
            pl.BlockSpec(memory_space=pltpu.SMEM),
            pl.BlockSpec((rows, CELLS), lambda g: (g, 0)),
        ],
        out_specs=pl.BlockSpec((ROWS, out_rows, LANES), lambda g: (0, g, 0)),
        out_shape=jax.ShapeDtypeStruct((ROWS, OPS * OWNED, LANES), F32),
        scratch_shapes=[pltpu.VMEM((out_rows, CELLS), F32), pltpu.VMEM((CELLS, LANES), F32)],
        compiler_params=params(),
        name="relayout",
    )(flag, kernel)


def spectral(lines, kernel, delta):
    twiddle = x_twiddle(-1.0, 1.0)
    back_twiddle = x_twiddle(1.0, -1.0 / (CELLS * CELLS))
    return pl.pallas_call(
        spectral_kernel,
        in_specs=[VMEM, HBM] + [VMEM] * 5,
        out_specs=VMEM,
        out_shape=jax.ShapeDtypeStruct((DEVICES * SLOT, LANES), F32),
        scratch_shapes=[
            pltpu.VMEM((ROWS * OPS * OWNED, LANES), F32),
            pltpu.VMEM((ROWS * EXTRA, LANES), F32),
            pltpu.VMEM((ROWS * P1_ALL, LANES), F32),
            pltpu.VMEM((ROWS * P1_ALL, 2 * LANES), BF16),
            pltpu.VMEM((ROWS * P1_ALL, LANES), F32),
            pltpu.VMEM((ROWS * P1_ROWS, LANES), F32),
            pltpu.VMEM((ROWS * P1_ROWS, LANES), F32),
            pltpu.SemaphoreType.DMA,
        ],
        compiler_params=params(),
        name="spectral",
    )(
        lines,
        kernel,
        delta,
        jnp.asarray(twiddle),
        jnp.asarray(back_twiddle),
        jnp.asarray(x_table(-1.0)),
        jnp.asarray(x_table(1.0)),
    )


def inverse_y(spectra):
    rows = COMPS * X_ROWS
    return pl.pallas_call(
        inverse_y_kernel,
        in_specs=[VMEM] * 3,
        out_specs=HBM,
        out_shape=jax.ShapeDtypeStruct((rows, CELLS), F32),
        scratch_shapes=[
            pltpu.VMEM((FINE_ROWS, 2 * LANES), BF16),
            pltpu.VMEM((FINE_ROWS, 2 * LANES), BF16),
            pltpu.VMEM((FINE_ROWS, 2 * LANES), F32),
            pltpu.VMEM((rows, CELLS), F32),
            pltpu.SemaphoreType.DMA((COMPS,)),
        ],
        compiler_params=params(),
        name="inverse_y",
    )(spectra, jnp.asarray(stacked(fine_table().T)), jnp.asarray(y_twiddle(1.0, 2.0)))


def exchange(lines):
    moved = lax.all_to_all(lines.reshape(DEVICES, SLOT, LANES), ("layer", "row"), 0, 0, tiled=True)
    return moved.reshape(DEVICES * SLOT, LANES)


def local(magnet, kernel):
    axes = ("layer", "row")
    device = lax.axis_index(axes)
    field = magnet.reshape(COMPS * X_ROWS, CELLS)
    flag = (device >= DEVICES // 2).astype(jnp.int32).reshape(1)
    edge = kernel[:, :, 0, :].reshape(OPS, CELLS)
    middle = lax.ppermute(edge, axes, [(DEVICES // 2, 0)])
    sent, middle = lax.optimization_barrier((forward_y(field), middle))
    got = exchange(sent)
    coefficient = relayout(kernel.reshape(OPS * 16, CELLS), flag)
    delta = jnp.where(device == 0, middle - edge, 0.0)
    delta = jnp.swapaxes(delta.reshape(OPS, X_ROWS, ROWS), 1, 2)
    delta = jnp.concatenate([delta, delta], axis=2).reshape(OPS * ROWS, LANES)
    fields = spectral(got, coefficient.reshape(ROWS * OPS * OWNED, LANES), delta)
    result = inverse_y(exchange(fields))
    return result.reshape(COMPS, 1, X_ROWS, CELLS)


def solution(mesh):
    in_specs = (P(None, "layer", "row", None), P(None, None, ("layer", "row"), None))
    out_specs = P(None, "layer", "row", None)
    return jax.shard_map(local, mesh=mesh, in_specs=in_specs, out_specs=out_specs, check_vma=False)
```

```python
import math

import jax
import jax.numpy as jnp
import numpy as np
from jax import lax
from jax.experimental import pallas as pl
from jax.experimental.pallas import tpu as pltpu
from jax.sharding import PartitionSpec as P


CELLS = 2048
COMPS = 3
LAYERS = 4
ROWS = 32
X_ROWS = 64
DEVICES = 128
PARTS = 6
OFFSETS = 7
OPS = OFFSETS * PARTS
FINE = 128
COARSE = 16
OWNED = 8
SLOT = COMPS * OWNED
LANES = 128
EXTRA = 16
P1_ROWS = LAYERS * COMPS * OWNED
P1_ALL = P1_ROWS + EXTRA

F32 = jnp.float32
BF16 = jnp.bfloat16


def halves(table):
    high = np.asarray(table, np.float32).astype(jnp.bfloat16)
    low = (np.asarray(table, np.float64) - high.astype(np.float64)).astype(np.float32).astype(jnp.bfloat16)
    return high, low


def fine_table():
    index = np.arange(FINE)
    angle = 2.0 * np.pi * (np.outer(index, index) % FINE) / FINE
    return np.block([[np.cos(angle), -np.sin(angle)], [np.sin(angle), np.cos(angle)]])


def stacked(table):
    return np.concatenate(halves(table), axis=0)


def y_twiddle(sign, scale):
    k = np.arange(1, COARSE // 2 + 1)[:, None]
    b = np.arange(FINE)[None, :]
    angle = 2.0 * np.pi * k * b / CELLS
    table = scale * np.stack([np.cos(angle), sign * np.sin(angle)], axis=1)
    return table.reshape(COARSE, FINE).astype(np.float32)


def lane_pair(coefficient):
    real = np.concatenate([coefficient.real, coefficient.real], axis=-1)
    imag = np.concatenate([-coefficient.imag, coefficient.imag], axis=-1)
    return real, imag


def x_twiddle(sign, scale):
    p1 = np.arange(ROWS)[:, None]
    t = np.arange(X_ROWS)[None, :]
    base = scale * np.exp(sign * 2.0j * np.pi * (p1 * t) / CELLS)
    side = np.where(p1 <= ROWS // 2, 1.0, -1.0) * (sign * 1.0j)
    kinds = []
    for kind in (1.0, 1.0j):
        first = lane_pair(kind * base)
        second = lane_pair(kind * base * side)
        kinds.append(np.stack(first + second, axis=1))
    return np.stack(kinds).astype(np.float32).reshape(2 * ROWS * 4, LANES)


def x_table(sign):
    index = np.arange(X_ROWS)
    angle = 2.0 * np.pi * (np.outer(index, index) % X_ROWS) / X_ROWS
    real = np.cos(angle)
    imag = sign * np.sin(angle)
    whole = np.block([[real, imag], [-imag, real]])
    high, low = halves(whole)
    line = np.concatenate([high, low], axis=1)
    return np.concatenate([line, line], axis=0)


def real_dft(values):
    n = len(values)
    if n == 1:
        return [values[0]], [None]
    if n == 2:
        return [values[0] + values[1], values[0] - values[1]], [None, None]
    even_c, even_s = real_dft(values[0::2])
    odd_c, odd_s = real_dft(values[1::2])
    half = n // 2
    quarter = n // 4
    cos_out = [None] * (half + 1)
    sin_out = [None] * (half + 1)
    for k in range(quarter + 1):
        if k == 0:
            cos_out[0] = even_c[0] + odd_c[0]
            cos_out[half] = even_c[0] - odd_c[0]
        elif k == quarter:
            cos_out[k] = even_c[k]
            sin_out[k] = odd_c[k]
        else:
            theta = 2.0 * math.pi * k / n
            cosine, sine = math.cos(theta), math.sin(theta)
            if 8 * k == n:
                real = cosine * (odd_c[k] - odd_s[k])
                imag = cosine * (odd_s[k] + odd_c[k])
            else:
                real = cosine * odd_c[k] - sine * odd_s[k]
                imag = cosine * odd_s[k] + sine * odd_c[k]
            cos_out[k] = even_c[k] + real
            sin_out[k] = even_s[k] + imag
            cos_out[half - k] = even_c[k] - real
            sin_out[half - k] = imag - even_s[k]
    return cos_out, sin_out


def real_sum(cos_in, sin_in, n):
    if n == 1:
        return [cos_in[0]]
    half = n // 2
    if n == 2:
        return [cos_in[0] + cos_in[1], cos_in[0] - cos_in[1]]
    quarter = n // 4
    even_c = [None] * (quarter + 1)
    even_s = [None] * (quarter + 1)
    odd_c = [None] * (quarter + 1)
    odd_s = [None] * (quarter + 1)
    even_c[0] = cos_in[0] + cos_in[half]
    odd_c[0] = cos_in[0] - cos_in[half]
    even_c[quarter] = cos_in[quarter]
    odd_c[quarter] = sin_in[quarter]
    for k in range(1, quarter):
        theta = 2.0 * math.pi * k / n
        cosine, sine = math.cos(theta), math.sin(theta)
        even_c[k] = cos_in[k] + cos_in[half - k]
        even_s[k] = sin_in[k] - sin_in[half - k]
        gap = cos_in[k] - cos_in[half - k]
        both = sin_in[k] + sin_in[half - k]
        if 8 * k == n:
            odd_c[k] = cosine * (gap + both)
            odd_s[k] = cosine * (both - gap)
        else:
            odd_c[k] = cosine * gap + sine * both
            odd_s[k] = cosine * both - sine * gap
    evens = real_sum(even_c, even_s, half)
    odds = real_sum(odd_c, odd_s, half)
    out = [None] * n
    out[0::2] = evens
    out[1::2] = odds
    return out


def split_pair(value):
    high = value.astype(BF16)
    low = (value - high.astype(F32)).astype(BF16)
    return high, low


def dot(left, right):
    return jnp.dot(left, right, preferred_element_type=F32)


def triple_dot(high, low, table_ref):
    size = table_ref.shape[0] // 2
    table_high, table_low = table_ref[:size, :], table_ref[size:, :]
    left = jnp.concatenate([high, low, high], axis=1)
    return dot(left, jnp.concatenate([table_high, table_high, table_low], axis=0))


def slot_rows(comp, k1):
    half = DEVICES // 2
    near = pl.ds(comp * OWNED + k1, half, stride=SLOT)
    far = pl.ds(half * SLOT + comp * OWNED + k1 - 1, half, stride=SLOT)
    return near, far


def forward_y_kernel(
    x_hbm,
    table_hbm,
    twiddle_hbm,
    kernel_hbm,
    out_hbm,
    edge_hbm,
    high_ref,
    low_ref,
    x_ref,
    table_ref,
    twiddle_ref,
    tiles_ref,
    out_ref,
    edge_ref,
    sem,
    tiles_sem,
):
    blocks = [pl.ds(comp * X_ROWS, X_ROWS) for comp in range(COMPS)]
    copies = [pltpu.make_async_copy(x_hbm.at[b], x_ref.at[b], sem.at[c]) for c, b in enumerate(blocks)]
    tables = [
        pltpu.make_async_copy(table_hbm, table_ref, sem.at[COMPS]),
        pltpu.make_async_copy(twiddle_hbm, twiddle_ref, sem.at[COMPS + 1]),
    ]
    n_tiles = CELLS // LANES
    edges = [
        pltpu.make_async_copy(
            kernel_hbm.at[:, pl.ds(0, OWNED), pl.ds(LANES * j, LANES)], tiles_ref.at[j], tiles_sem.at[j]
        )
        for j in range(n_tiles)
    ]
    copies[0].start()
    for copy in tables + copies[1:] + edges:
        copy.start()
    for copy in tables:
        copy.wait()
    slots = out_ref.reshape(DEVICES, SLOT, LANES)
    saves = []
    half = DEVICES // 2
    middle = COARSE // 2
    group = 16
    lane = lax.broadcasted_iota(jnp.int32, (X_ROWS, LANES), 1)
    alternate = 1.0 - 2.0 * (lax.broadcasted_iota(jnp.int32, (X_ROWS, FINE), 1) % 2).astype(F32)
    for comp in range(COMPS):
        base = comp * (middle + 1) * X_ROWS
        nyquist = []
        copies[comp].wait()
        for g in range(X_ROWS // group):
            top = comp * X_ROWS + g * group
            parts = [x_ref[top : top + group, FINE * a : FINE * (a + 1)] for a in range(COARSE)]
            cos_out, sin_out = real_dft(parts)
            nyquist.append(jnp.sum(cos_out[0] * alternate[:group], axis=1, keepdims=True))
            for k in range(middle + 1):
                rows = slice(base + k * X_ROWS + g * group, base + k * X_ROWS + (g + 1) * group)
                real = cos_out[k]
                imag = None
                if k > 0:
                    cosine = twiddle_ref[2 * k - 2 : 2 * k - 1, :]
                    sine = twiddle_ref[2 * k - 1 : 2 * k, :]
                    if k == middle:
                        real, imag = real * cosine, real * sine
                    else:
                        real, imag = real * cosine + sin_out[k] * sine, real * sine - sin_out[k] * cosine
                high_ref[rows, :LANES], low_ref[rows, :LANES] = split_pair(real)
                if imag is None:
                    zero = jnp.zeros((group, LANES), BF16)
                    high_ref[rows, LANES:], low_ref[rows, LANES:] = zero, zero
                else:
                    high_ref[rows, LANES:], low_ref[rows, LANES:] = split_pair(imag)
        size = (middle + 1) * X_ROWS
        out = triple_dot(high_ref[base : base + size, :], low_ref[base : base + size, :], table_ref)

        def pick(k):
            rows = out[k * X_ROWS : (k + 1) * X_ROWS]
            return rows[:, :LANES], rows[:, LANES:]

        for k in range(middle):
            real, imag = pick(k)
            if k == 0:
                last_real, last_imag = pick(middle)
                imag = jnp.where(lane == 0, jnp.concatenate(nyquist, axis=0), imag)
                real = jnp.where(lane < half, real, last_real)
                imag = jnp.where(lane < half, imag, last_imag)
            block = jnp.concatenate([real, imag], axis=0).T
            near, far = slot_rows(comp, k)
            if k == 0:
                far = slot_rows(comp, middle)[1]
            out_ref[near, :] = block[:half]
            out_ref[far, :] = block[half:]
        lines = (slice(None), pl.ds(comp * OWNED, OWNED))
        save = pltpu.make_async_copy(slots.at[lines], out_hbm.at[lines], sem.at[COMPS + 2 + comp])
        save.start()
        saves.append(save)
        if comp == COMPS - 2:
            flat = tiles_ref.reshape(n_tiles * OPS * OWNED, LANES)
            for j in range(n_tiles):
                edges[j].wait()
                edge_ref[:, LANES * j : LANES * (j + 1)] = flat[pl.ds(j * OPS * OWNED, OPS, stride=OWNED), :]
            save = pltpu.make_async_copy(edge_ref, edge_hbm, sem.at[2 * COMPS + 2])
            save.start()
            saves.append(save)
    for save in saves:
        save.wait()


def relayout_kernel(flag_ref, kernel_ref, out_ref, rows_ref, columns_ref):
    shifted = flag_ref[0] > 0
    n_ops = kernel_ref.shape[0] // 16
    sub = lax.broadcasted_iota(jnp.int32, (OWNED, CELLS), 0)
    for op in range(n_ops):
        low = kernel_ref[16 * op : 16 * op + 8, :]
        high = kernel_ref[16 * op + 8 : 16 * op + 16, :]
        moved = jnp.where(sub < 7, pltpu.roll(low, 7, 0), pltpu.roll(high, 7, 0))
        rows_ref[8 * op : 8 * op + 8, :] = jnp.where(shifted, moved, low)
    for tile in range(CELLS // LANES):
        block = rows_ref[:, LANES * tile : LANES * (tile + 1)].T
        columns_ref[LANES * tile : LANES * (tile + 1), : 8 * n_ops] = block

    def step(p1, carry):
        column = columns_ref[pl.ds(p1, X_ROWS, stride=ROWS), :]
        both = jnp.concatenate([column, column], axis=0).T
        out_ref[p1] = both[: 8 * n_ops]
        return carry

    lax.fori_loop(0, ROWS, step, 0, unroll=4)


def spectral_kernel(
    x_ref,
    kernel_hbm,
    delta_ref,
    twiddle_ref,
    back_twiddle_ref,
    table_ref,
    back_table_ref,
    out_ref,
    kernel_ref,
    extra_ref,
    sums_ref,
    pair_ref,
    spec_ref,
    fix_ref,
    back_ref,
    kernel_sem,
):
    fetch = pltpu.make_async_copy(kernel_hbm, kernel_ref, kernel_sem)
    fetch.start()
    half = ROWS // 2
    lane = lax.broadcasted_iota(jnp.int32, (ROWS, LANES), 1)

    extra_ref[...] = jnp.zeros_like(extra_ref)
    for layer in range(LAYERS):
        for comp in range(COMPS):
            line = x_ref[pl.ds(layer * ROWS * SLOT + comp * OWNED, ROWS, stride=SLOT), :]
            extra_ref[pl.ds(comp * LAYERS + layer, ROWS, stride=EXTRA), :] = jnp.where(lane < X_ROWS, 0.0, line)
    fix_ref[...] = jnp.zeros_like(fix_ref)

    def store_sums(values, place):
        cos_out, sin_out = real_dft(values)
        for k in range(half + 1):
            sums_ref[pl.ds(k * P1_ALL + place, OWNED), :] = cos_out[k]
        for k in range(1, half):
            sums_ref[pl.ds((half + k) * P1_ALL + place, OWNED), :] = sin_out[k]

    def over_rows(index, carry):
        layer = index // COMPS
        comp = index % COMPS
        base = layer * (ROWS * SLOT) + comp * OWNED
        base = pl.multiple_of(base, OWNED)
        values = [x_ref[pl.ds(base + r * SLOT, OWNED), :] for r in range(ROWS)]
        store_sums(values, pl.multiple_of(index * OWNED, OWNED))
        return carry

    lax.fori_loop(0, LAYERS * COMPS, over_rows, 0)
    for group in range(2):
        values = [extra_ref[r * EXTRA + group * 8 : r * EXTRA + group * 8 + 8, :] for r in range(ROWS)]
        store_sums(values, P1_ROWS + group * 8)

    def factors(ref, p1, kind):
        base = kind * (ROWS * 4) + p1 * 4
        return [ref[pl.ds(base + j, 1), :] for j in range(4)]

    def save_pair(row, value):
        high, low = split_pair(value)
        pair_ref[pl.ds(row, value.shape[0]), :LANES] = high
        pair_ref[pl.ds(row, value.shape[0]), LANES:] = low

    kinds = [1 if j % COMPS == 2 else 0 for j in range(LAYERS * COMPS)] + [0, 1]

    def blocks(ref, row, count):
        return [ref[pl.ds(row + OWNED * j, OWNED), :] for j in range(count)]

    def twist(k, p1_list, with_sin):
        cos_rows = blocks(sums_ref, pl.multiple_of(k * P1_ALL, OWNED), len(kinds))
        cos_swap = [pltpu.roll(v, X_ROWS, 1) for v in cos_rows]
        if with_sin:
            sin_rows = blocks(sums_ref, pl.multiple_of((half + k) * P1_ALL, OWNED), len(kinds))
            sin_swap = [pltpu.roll(v, X_ROWS, 1) for v in sin_rows]
        for place, p1 in enumerate(p1_list):
            table = [factors(twiddle_ref, p1, kind) for kind in range(2)]
            out = []
            for j, kind in enumerate(kinds):
                f = table[kind]
                value = cos_rows[j] * f[0] + cos_swap[j] * f[1]
                if with_sin:
                    value = value + (sin_rows[j] * f[2] + sin_swap[j] * f[3])
                out.append(value)
            for j in range(0, len(kinds), 2):
                row = 2 * k * P1_ALL + place * P1_ALL + OWNED * j
                save_pair(pl.multiple_of(row, 2 * OWNED), jnp.concatenate(out[j : j + 2], axis=0))

    def forward_dot(k, first, second):
        rows = 2 * P1_ALL
        base = k * rows if isinstance(k, int) else pl.multiple_of(k * rows, 2 * OWNED)
        both = dot(pair_ref[pl.ds(base, rows), :], table_ref[...])
        whole_line = both[:, :LANES] + both[:, LANES:]
        spec_ref[pl.ds(first * P1_ALL, P1_ALL), :] = whole_line[:P1_ALL]
        spec_ref[pl.ds(second * P1_ALL, P1_ALL), :] = whole_line[P1_ALL:]

    twist(0, [0], False)
    cos_edge = blocks(sums_ref, half * P1_ALL, len(kinds))
    table = [factors(twiddle_ref, half, kind) for kind in range(2)]
    edge = [v * table[kind][0] + pltpu.roll(v, X_ROWS, 1) * table[kind][1] for v, kind in zip(cos_edge, kinds)]
    for j in range(0, len(kinds), 2):
        save_pair(P1_ALL + OWNED * j, jnp.concatenate(edge[j : j + 2], axis=0))
    forward_dot(0, 0, half)
    twist(1, [1, ROWS - 1], True)

    def twist_step(k, carry):
        forward_dot(k - 1, k - 1, ROWS + 1 - k)
        twist(k, [k, ROWS - k], True)
        return carry

    lax.fori_loop(2, half, twist_step, 0)
    forward_dot(half - 1, half - 1, half + 1)
    fetch.wait()

    def mix(spectra, coefficient):
        fields = []
        for target in range(LAYERS):
            total = [None, None, None]

            def add(comp, term):
                total[comp] = term if total[comp] is None else total[comp] + term

            for source in range(LAYERS):
                offset = target - source + LAYERS - 1
                k = [coefficient(offset * PARTS + j) for j in range(PARTS)]
                mx, my, mz = spectra[source]
                add(0, k[0] * mx + k[3] * my + k[4] * mz)
                add(1, k[3] * mx + k[1] * my + k[5] * mz)
                add(2, k[4] * mx + k[5] * my - k[2] * mz)
            fields.append(total)
        return fields

    def fix_step(group, carry):
        base = group * OWNED
        spectra = [
            [
                spec_ref[pl.ds(base * P1_ALL + P1_ROWS + comp * LAYERS + source, OWNED, stride=P1_ALL), :]
                for comp in range(COMPS)
            ]
            for source in range(LAYERS)
        ]

        def coefficient(op):
            return delta_ref[pl.ds(pl.multiple_of(op * ROWS + base, OWNED), OWNED), :]

        fields = mix(spectra, coefficient)
        for target in range(LAYERS):
            for comp in range(COMPS):
                row = base * P1_ROWS + (target * COMPS + comp) * OWNED
                fix_ref[pl.ds(row, OWNED, stride=P1_ROWS), :] = fields[target][comp]
        return carry

    lax.fori_loop(0, ROWS // OWNED, fix_step, 0)

    def mix_line(p1):
        lines = blocks(spec_ref, p1 * P1_ALL, LAYERS * COMPS)
        spectra = [lines[COMPS * s : COMPS * s + COMPS] for s in range(LAYERS)]
        kernel_base = p1 * (OPS * OWNED)

        def coefficient(op):
            return kernel_ref[pl.ds(kernel_base + op * OWNED, OWNED), :]

        fields = mix(spectra, coefficient)
        flat = [fields[j // COMPS][j % COMPS] for j in range(LAYERS * COMPS)]
        row = p1 * P1_ROWS
        fixes = blocks(fix_ref, row, LAYERS * COMPS)
        flat = [a + b for a, b in zip(flat, fixes)]
        for j in range(0, LAYERS * COMPS, 2):
            save_pair(row + OWNED * j, jnp.concatenate(flat[j : j + 2], axis=0))

    def backward_dot(p1, rows):
        both = dot(pair_ref[pl.ds(p1 * P1_ROWS, rows), :], back_table_ref[...])
        back_ref[pl.ds(p1 * P1_ROWS, rows), :] = both[:, :LANES] + both[:, LANES:]

    mix_line(0)
    mix_line(1)

    def mix_step(step, carry):
        p1 = pl.multiple_of(2 * step, 2)
        backward_dot(p1 - 2, 2 * P1_ROWS)
        mix_line(p1)
        mix_line(p1 + 1)
        return carry

    lax.fori_loop(1, half, mix_step, 0)
    backward_dot(ROWS - 2, 2 * P1_ROWS)

    count = LAYERS * COMPS

    def untwist_edge(p1, slot):
        table = [factors(back_twiddle_ref, p1, kind) for kind in range(2)]
        for j, value in enumerate(blocks(back_ref, p1 * P1_ROWS, count)):
            f = table[kinds[j]]
            sums_ref[pl.ds(slot * P1_ROWS + OWNED * j, OWNED), :] = value * f[0] + pltpu.roll(value, X_ROWS, 1) * f[1]

    untwist_edge(0, 0)
    untwist_edge(half, half)

    def untwist_step(k, carry):
        near = [factors(back_twiddle_ref, k, kind) for kind in range(2)]
        far = [factors(back_twiddle_ref, ROWS - k, kind) for kind in range(2)]
        near_rows = blocks(back_ref, pl.multiple_of(k * P1_ROWS, OWNED), count)
        far_rows = blocks(back_ref, pl.multiple_of((ROWS - k) * P1_ROWS, OWNED), count)
        cos_base = pl.multiple_of(k * P1_ROWS, OWNED)
        sin_base = pl.multiple_of((half + k) * P1_ROWS, OWNED)
        for j in range(count):
            n, f = near[kinds[j]], far[kinds[j]]
            a, b = near_rows[j], far_rows[j]
            a_swap, b_swap = pltpu.roll(a, X_ROWS, 1), pltpu.roll(b, X_ROWS, 1)
            sums_ref[pl.ds(cos_base + OWNED * j, OWNED), :] = (a * n[0] + a_swap * n[1]) + (b * f[0] + b_swap * f[1])
            sums_ref[pl.ds(sin_base + OWNED * j, OWNED), :] = (a * n[2] + a_swap * n[3]) + (b * f[2] + b_swap * f[3])
        return carry

    lax.fori_loop(1, half, untwist_step, 0)

    def back_rows(index, carry):
        place = pl.multiple_of(index * OWNED, OWNED)
        cos_in = [sums_ref[pl.ds(k * P1_ROWS + place, OWNED), :] for k in range(half + 1)]
        sin_in = [None] + [sums_ref[pl.ds((half + k) * P1_ROWS + place, OWNED), :] for k in range(1, half)] + [None]
        values = real_sum(cos_in, sin_in, ROWS)
        layer = index // COMPS
        comp = index % COMPS
        base = pl.multiple_of(layer * (ROWS * SLOT) + comp * OWNED, OWNED)
        for r in range(ROWS):
            out_ref[pl.ds(base + r * SLOT, OWNED), :] = values[r]
        return carry

    lax.fori_loop(0, LAYERS * COMPS, back_rows, 0)


def inverse_y_kernel(x_ref, table_ref, twiddle_ref, out_hbm, high_ref, low_ref, lines_ref, result_ref, sem):
    half = DEVICES // 2
    middle = COARSE // 2
    group = 8
    lane = lax.broadcasted_iota(jnp.int32, (X_ROWS, LANES), 1)
    alternate = 1.0 - 2.0 * (lax.broadcasted_iota(jnp.int32, (group, FINE), 1) % 2).astype(F32)
    copies = []
    for comp in range(COMPS):
        size = (middle + 1) * X_ROWS
        base = comp * size

        def put(k, real, imag):
            rows = slice(base + k * X_ROWS, base + (k + 1) * X_ROWS)
            high_ref[rows, :LANES], low_ref[rows, :LANES] = split_pair(real)
            high_ref[rows, LANES:], low_ref[rows, LANES:] = split_pair(imag)

        for k in range(middle):
            near, far = slot_rows(comp, k)
            if k == 0:
                far = slot_rows(comp, middle)[1]
            block = jnp.concatenate([x_ref[near, :], x_ref[far, :]], axis=0).T
            real, imag = block[:X_ROWS], block[X_ROWS:]
            if k == 0:
                nyquist = imag[:, :1]
                put(middle, jnp.where(lane < half, 0.0, real), jnp.where(lane < half, 0.0, imag))
                scale = jnp.where(lane < half, jnp.where(lane == 0, 0.5, 1.0), 0.0)
                real, imag = real * scale, imag * scale
            put(k, real, imag)
        lines_ref[base : base + size, :] = triple_dot(
            high_ref[base : base + size, :], low_ref[base : base + size, :], table_ref
        )
        for g in range(X_ROWS // group):
            cos_in = [None] * (middle + 1)
            sin_in = [None] * (middle + 1)
            for k in range(middle + 1):
                rows = slice(base + k * X_ROWS + g * group, base + k * X_ROWS + (g + 1) * group)
                real = lines_ref[rows, :LANES]
                if k == 0:
                    cos_in[0] = 2.0 * real + nyquist[g * group : (g + 1) * group] * alternate
                    continue
                imag = lines_ref[rows, LANES:]
                cosine = twiddle_ref[2 * k - 2 : 2 * k - 1, :]
                sine = twiddle_ref[2 * k - 1 : 2 * k, :]
                cos_in[k] = real * cosine - imag * sine
                if k < middle:
                    sin_in[k] = -(real * sine + imag * cosine)
            values = real_sum(cos_in, sin_in, COARSE)
            top = comp * X_ROWS + g * group
            for a in range(COARSE):
                result_ref[top : top + group, FINE * a : FINE * (a + 1)] = values[a]
        span = pl.ds(comp * X_ROWS, X_ROWS)
        copy = pltpu.make_async_copy(result_ref.at[span], out_hbm.at[span], sem.at[comp])
        copy.start()
        copies.append(copy)
    for copy in copies:
        copy.wait()


VMEM = pl.BlockSpec(memory_space=pltpu.VMEM)
HBM = pl.BlockSpec(memory_space=pltpu.HBM)
FINE_ROWS = COMPS * (COARSE // 2 + 1) * X_ROWS


def params(mebibytes):
    return pltpu.CompilerParams(vmem_limit_bytes=mebibytes * 1024 * 1024)


def forward_y(field, kernel):
    table = stacked(fine_table())
    twiddle = y_twiddle(-1.0, 1.0)
    return pl.pallas_call(
        forward_y_kernel,
        in_specs=[HBM] * 4,
        out_specs=[HBM, HBM],
        out_shape=[
            jax.ShapeDtypeStruct((DEVICES, SLOT, LANES), F32),
            jax.ShapeDtypeStruct((OPS, CELLS), F32),
        ],
        scratch_shapes=[
            pltpu.VMEM((FINE_ROWS, 2 * LANES), BF16),
            pltpu.VMEM((FINE_ROWS, 2 * LANES), BF16),
            pltpu.VMEM((COMPS * X_ROWS, CELLS), F32),
            pltpu.VMEM(table.shape, BF16),
            pltpu.VMEM(twiddle.shape, F32),
            pltpu.VMEM((CELLS // LANES, OPS, OWNED, LANES), F32),
            pltpu.VMEM((DEVICES * SLOT, LANES), F32),
            pltpu.VMEM((OPS, CELLS), F32),
            pltpu.SemaphoreType.DMA((2 * COMPS + 3,)),
            pltpu.SemaphoreType.DMA((CELLS // LANES,)),
        ],
        compiler_params=params(63),
        name="forward_y",
    )(field, jnp.asarray(table), jnp.asarray(twiddle), kernel)


def relayout(kernel, flag):
    groups = 3
    rows = OPS // groups * 16
    out_rows = OPS // groups * OWNED
    return pl.pallas_call(
        relayout_kernel,
        grid=(groups,),
        in_specs=[
            pl.BlockSpec(memory_space=pltpu.SMEM),
            pl.BlockSpec((rows, CELLS), lambda g: (g, 0)),
        ],
        out_specs=pl.BlockSpec((ROWS, out_rows, LANES), lambda g: (0, g, 0)),
        out_shape=jax.ShapeDtypeStruct((ROWS, OPS * OWNED, LANES), F32),
        scratch_shapes=[pltpu.VMEM((out_rows, CELLS), F32), pltpu.VMEM((CELLS, LANES), F32)],
        compiler_params=params(48),
        name="relayout",
    )(flag, kernel)


def spectral(lines, kernel, delta):
    twiddle = x_twiddle(-1.0, 1.0)
    back_twiddle = x_twiddle(1.0, -1.0 / (CELLS * CELLS))
    return pl.pallas_call(
        spectral_kernel,
        in_specs=[VMEM, HBM] + [VMEM] * 5,
        out_specs=VMEM,
        out_shape=jax.ShapeDtypeStruct((DEVICES * SLOT, LANES), F32),
        scratch_shapes=[
            pltpu.VMEM((ROWS * OPS * OWNED, LANES), F32),
            pltpu.VMEM((ROWS * EXTRA, LANES), F32),
            pltpu.VMEM((ROWS * P1_ALL, LANES), F32),
            pltpu.VMEM((ROWS * P1_ALL, 2 * LANES), BF16),
            pltpu.VMEM((ROWS * P1_ALL, LANES), F32),
            pltpu.VMEM((ROWS * P1_ROWS, LANES), F32),
            pltpu.VMEM((ROWS * P1_ROWS, LANES), F32),
            pltpu.SemaphoreType.DMA,
        ],
        compiler_params=params(48),
        name="spectral",
    )(
        lines,
        kernel,
        delta,
        jnp.asarray(twiddle),
        jnp.asarray(back_twiddle),
        jnp.asarray(x_table(-1.0)),
        jnp.asarray(x_table(1.0)),
    )


def inverse_y(spectra):
    rows = COMPS * X_ROWS
    return pl.pallas_call(
        inverse_y_kernel,
        in_specs=[VMEM] * 3,
        out_specs=HBM,
        out_shape=jax.ShapeDtypeStruct((rows, CELLS), F32),
        scratch_shapes=[
            pltpu.VMEM((FINE_ROWS, 2 * LANES), BF16),
            pltpu.VMEM((FINE_ROWS, 2 * LANES), BF16),
            pltpu.VMEM((FINE_ROWS, 2 * LANES), F32),
            pltpu.VMEM((rows, CELLS), F32),
            pltpu.SemaphoreType.DMA((COMPS,)),
        ],
        compiler_params=params(20),
        name="inverse_y",
    )(spectra, jnp.asarray(stacked(fine_table().T)), jnp.asarray(y_twiddle(1.0, 2.0)))


def exchange(lines):
    moved = lax.all_to_all(lines.reshape(DEVICES, SLOT, LANES), ("layer", "row"), 0, 0, tiled=True)
    return moved.reshape(DEVICES * SLOT, LANES)


def local(magnet, kernel):
    axes = ("layer", "row")
    device = lax.axis_index(axes)
    field = magnet.reshape(COMPS * X_ROWS, CELLS)
    flag = (device >= DEVICES // 2).astype(jnp.int32).reshape(1)
    sent, edge = forward_y(field, kernel.reshape(OPS, 16, CELLS))
    middle = lax.ppermute(edge, axes, [(DEVICES // 2, 0)])
    got = exchange(sent)
    coefficient = relayout(kernel.reshape(OPS * 16, CELLS), flag)
    delta = jnp.where(device == 0, middle - edge, 0.0)
    delta = jnp.swapaxes(delta.reshape(OPS, X_ROWS, ROWS), 1, 2)
    delta = jnp.concatenate([delta, delta], axis=2).reshape(OPS * ROWS, LANES)
    fields = spectral(got, coefficient.reshape(ROWS * OPS * OWNED, LANES), delta)
    result = inverse_y(exchange(fields))
    return result.reshape(COMPS, 1, X_ROWS, CELLS)


def solution(mesh):
    in_specs = (P(None, "layer", "row", None), P(None, None, ("layer", "row"), None))
    out_specs = P(None, "layer", "row", None)
    return jax.shard_map(local, mesh=mesh, in_specs=in_specs, out_specs=out_specs, check_vma=False)
```

```python
import math

import jax
import jax.numpy as jnp
import numpy as np
from jax import lax
from jax.experimental import pallas as pl
from jax.experimental.pallas import tpu as pltpu
from jax.sharding import PartitionSpec as P


CELLS = 2048
COMPS = 3
LAYERS = 4
ROWS = 32
X_ROWS = 64
DEVICES = 128
PARTS = 6
OFFSETS = 7
OPS = OFFSETS * PARTS
FINE = 128
COARSE = 16
OWNED = 8
SLOT = COMPS * OWNED
LANES = 128
EXTRA = 16
P1_ROWS = LAYERS * COMPS * OWNED
P1_ALL = P1_ROWS + EXTRA

F32 = jnp.float32
BF16 = jnp.bfloat16


def halves(table):
    high = np.asarray(table, np.float32).astype(jnp.bfloat16)
    low = (np.asarray(table, np.float64) - high.astype(np.float64)).astype(np.float32).astype(jnp.bfloat16)
    return high, low


def fine_table():
    index = np.arange(FINE)
    angle = 2.0 * np.pi * (np.outer(index, index) % FINE) / FINE
    return np.block([[np.cos(angle), -np.sin(angle)], [np.sin(angle), np.cos(angle)]])


def stacked(table):
    return np.concatenate(halves(table), axis=0)


def y_twiddle(sign, scale):
    k = np.arange(1, COARSE // 2 + 1)[:, None]
    b = np.arange(FINE)[None, :]
    angle = 2.0 * np.pi * k * b / CELLS
    table = scale * np.stack([np.cos(angle), sign * np.sin(angle)], axis=1)
    return table.reshape(COARSE, FINE).astype(np.float32)


def lane_pair(coefficient):
    real = np.concatenate([coefficient.real, coefficient.real], axis=-1)
    imag = np.concatenate([-coefficient.imag, coefficient.imag], axis=-1)
    return real, imag


def x_twiddle(sign, scale):
    p1 = np.arange(ROWS)[:, None]
    t = np.arange(X_ROWS)[None, :]
    base = scale * np.exp(sign * 2.0j * np.pi * (p1 * t) / CELLS)
    side = np.where(p1 <= ROWS // 2, 1.0, -1.0) * (sign * 1.0j)
    kinds = []
    for kind in (1.0, 1.0j):
        first = lane_pair(kind * base)
        second = lane_pair(kind * base * side)
        kinds.append(np.stack(first + second, axis=1))
    return np.stack(kinds).astype(np.float32).reshape(2 * ROWS * 4, LANES)


def x_table(sign):
    index = np.arange(X_ROWS)
    angle = 2.0 * np.pi * (np.outer(index, index) % X_ROWS) / X_ROWS
    real = np.cos(angle)
    imag = sign * np.sin(angle)
    whole = np.block([[real, imag], [-imag, real]])
    high, low = halves(whole)
    line = np.concatenate([high, low], axis=1)
    return np.concatenate([line, line], axis=0)


def real_dft(values):
    n = len(values)
    if n == 1:
        return [values[0]], [None]
    if n == 2:
        return [values[0] + values[1], values[0] - values[1]], [None, None]
    even_c, even_s = real_dft(values[0::2])
    odd_c, odd_s = real_dft(values[1::2])
    half = n // 2
    quarter = n // 4
    cos_out = [None] * (half + 1)
    sin_out = [None] * (half + 1)
    for k in range(quarter + 1):
        if k == 0:
            cos_out[0] = even_c[0] + odd_c[0]
            cos_out[half] = even_c[0] - odd_c[0]
        elif k == quarter:
            cos_out[k] = even_c[k]
            sin_out[k] = odd_c[k]
        else:
            theta = 2.0 * math.pi * k / n
            cosine, sine = math.cos(theta), math.sin(theta)
            if 8 * k == n:
                real = cosine * (odd_c[k] - odd_s[k])
                imag = cosine * (odd_s[k] + odd_c[k])
            else:
                real = cosine * odd_c[k] - sine * odd_s[k]
                imag = cosine * odd_s[k] + sine * odd_c[k]
            cos_out[k] = even_c[k] + real
            sin_out[k] = even_s[k] + imag
            cos_out[half - k] = even_c[k] - real
            sin_out[half - k] = imag - even_s[k]
    return cos_out, sin_out


def real_sum(cos_in, sin_in, n):
    if n == 1:
        return [cos_in[0]]
    half = n // 2
    if n == 2:
        return [cos_in[0] + cos_in[1], cos_in[0] - cos_in[1]]
    quarter = n // 4
    even_c = [None] * (quarter + 1)
    even_s = [None] * (quarter + 1)
    odd_c = [None] * (quarter + 1)
    odd_s = [None] * (quarter + 1)
    even_c[0] = cos_in[0] + cos_in[half]
    odd_c[0] = cos_in[0] - cos_in[half]
    even_c[quarter] = cos_in[quarter]
    odd_c[quarter] = sin_in[quarter]
    for k in range(1, quarter):
        theta = 2.0 * math.pi * k / n
        cosine, sine = math.cos(theta), math.sin(theta)
        even_c[k] = cos_in[k] + cos_in[half - k]
        even_s[k] = sin_in[k] - sin_in[half - k]
        gap = cos_in[k] - cos_in[half - k]
        both = sin_in[k] + sin_in[half - k]
        if 8 * k == n:
            odd_c[k] = cosine * (gap + both)
            odd_s[k] = cosine * (both - gap)
        else:
            odd_c[k] = cosine * gap + sine * both
            odd_s[k] = cosine * both - sine * gap
    evens = real_sum(even_c, even_s, half)
    odds = real_sum(odd_c, odd_s, half)
    out = [None] * n
    out[0::2] = evens
    out[1::2] = odds
    return out


def split_pair(value):
    high = value.astype(BF16)
    low = (value - high.astype(F32)).astype(BF16)
    return high, low


def dot(left, right):
    return jnp.dot(left, right, preferred_element_type=F32)


def triple_dot(high, low, table_ref):
    size = table_ref.shape[0] // 2
    table_high, table_low = table_ref[:size, :], table_ref[size:, :]
    left = jnp.concatenate([high, low, high], axis=1)
    return dot(left, jnp.concatenate([table_high, table_high, table_low], axis=0))


def slot_rows(comp, k1):
    half = DEVICES // 2
    near = pl.ds(comp * OWNED + k1, half, stride=SLOT)
    far = pl.ds(half * SLOT + comp * OWNED + k1 - 1, half, stride=SLOT)
    return near, far


EDGE_PARTS = 4
EDGES = OFFSETS * EDGE_PARTS


def edge_kernel(kernel_hbm, out_ref, tiles_ref, sem):
    n_tiles = CELLS // LANES
    copies = []
    for j in range(n_tiles):
        lanes = pl.ds(LANES * j, LANES)
        for i, (source, target) in enumerate([((0, 3), (0, 3)), ((4, 1), (3, 1))]):
            copy = pltpu.make_async_copy(
                kernel_hbm.at[:, pl.ds(*source), pl.ds(0, OWNED), lanes],
                tiles_ref.at[j, :, pl.ds(*target)],
                sem.at[j, i],
            )
            copy.start()
            copies.append(copy)
    flat = tiles_ref.reshape(n_tiles * EDGES * OWNED, LANES)
    for j in range(n_tiles):
        copies[2 * j].wait()
        copies[2 * j + 1].wait()
        out_ref[:, LANES * j : LANES * (j + 1)] = flat[pl.ds(j * EDGES * OWNED, EDGES, stride=OWNED), :]


def forward_y_kernel(x_ref, table_ref, twiddle_ref, out_hbm, high_ref, low_ref, out_ref, sem):
    slots = out_ref.reshape(DEVICES, SLOT, LANES)
    saves = []
    half = DEVICES // 2
    middle = COARSE // 2
    group = 16
    lane = lax.broadcasted_iota(jnp.int32, (X_ROWS, LANES), 1)
    alternate = 1.0 - 2.0 * (lax.broadcasted_iota(jnp.int32, (X_ROWS, FINE), 1) % 2).astype(F32)
    for comp in range(COMPS):
        base = comp * (middle + 1) * X_ROWS
        nyquist = []
        for g in range(X_ROWS // group):
            top = comp * X_ROWS + g * group
            parts = [x_ref[top : top + group, FINE * a : FINE * (a + 1)] for a in range(COARSE)]
            cos_out, sin_out = real_dft(parts)
            nyquist.append(jnp.sum(cos_out[0] * alternate[:group], axis=1, keepdims=True))
            for k in range(middle + 1):
                rows = slice(base + k * X_ROWS + g * group, base + k * X_ROWS + (g + 1) * group)
                real = cos_out[k]
                imag = None
                if k > 0:
                    cosine = twiddle_ref[2 * k - 2 : 2 * k - 1, :]
                    sine = twiddle_ref[2 * k - 1 : 2 * k, :]
                    if k == middle:
                        real, imag = real * cosine, real * sine
                    else:
                        real, imag = real * cosine + sin_out[k] * sine, real * sine - sin_out[k] * cosine
                high_ref[rows, :LANES], low_ref[rows, :LANES] = split_pair(real)
                if imag is None:
                    zero = jnp.zeros((group, LANES), BF16)
                    high_ref[rows, LANES:], low_ref[rows, LANES:] = zero, zero
                else:
                    high_ref[rows, LANES:], low_ref[rows, LANES:] = split_pair(imag)
        size = (middle + 1) * X_ROWS
        out = triple_dot(high_ref[base : base + size, :], low_ref[base : base + size, :], table_ref)

        def pick(k):
            rows = out[k * X_ROWS : (k + 1) * X_ROWS]
            return rows[:, :LANES], rows[:, LANES:]

        for k in range(middle):
            real, imag = pick(k)
            if k == 0:
                last_real, last_imag = pick(middle)
                imag = jnp.where(lane == 0, jnp.concatenate(nyquist, axis=0), imag)
                real = jnp.where(lane < half, real, last_real)
                imag = jnp.where(lane < half, imag, last_imag)
            block = jnp.concatenate([real, imag], axis=0).T
            near, far = slot_rows(comp, k)
            if k == 0:
                far = slot_rows(comp, middle)[1]
            out_ref[near, :] = block[:half]
            out_ref[far, :] = block[half:]
        lines = (slice(None), pl.ds(comp * OWNED, OWNED))
        save = pltpu.make_async_copy(slots.at[lines], out_hbm.at[lines], sem.at[comp])
        save.start()
        saves.append(save)
    for save in saves:
        save.wait()


def relayout_kernel(flag_ref, kernel_ref, out_ref, rows_ref, columns_ref):
    shifted = flag_ref[0] > 0
    n_ops = kernel_ref.shape[0] // 16
    sub = lax.broadcasted_iota(jnp.int32, (OWNED, CELLS), 0)
    for op in range(n_ops):
        low = kernel_ref[16 * op : 16 * op + 8, :]
        high = kernel_ref[16 * op + 8 : 16 * op + 16, :]
        moved = jnp.where(sub < 7, pltpu.roll(low, 7, 0), pltpu.roll(high, 7, 0))
        rows_ref[8 * op : 8 * op + 8, :] = jnp.where(shifted, moved, low)
    for tile in range(CELLS // LANES):
        block = rows_ref[:, LANES * tile : LANES * (tile + 1)].T
        columns_ref[LANES * tile : LANES * (tile + 1), : 8 * n_ops] = block

    def step(p1, carry):
        column = columns_ref[pl.ds(p1, X_ROWS, stride=ROWS), :]
        both = jnp.concatenate([column, column], axis=0).T
        out_ref[p1] = both[: 8 * n_ops]
        return carry

    lax.fori_loop(0, ROWS, step, 0, unroll=4)


def spectral_kernel(
    x_ref,
    kernel_hbm,
    delta_ref,
    twiddle_ref,
    back_twiddle_ref,
    table_ref,
    back_table_ref,
    out_ref,
    kernel_ref,
    extra_ref,
    sums_ref,
    pair_ref,
    spec_ref,
    fix_ref,
    back_ref,
    kernel_sem,
):
    fetch = pltpu.make_async_copy(kernel_hbm, kernel_ref, kernel_sem)
    fetch.start()
    half = ROWS // 2
    lane = lax.broadcasted_iota(jnp.int32, (ROWS, LANES), 1)

    extra_ref[...] = jnp.zeros_like(extra_ref)
    for layer in range(LAYERS):
        for comp in range(COMPS):
            line = x_ref[pl.ds(layer * ROWS * SLOT + comp * OWNED, ROWS, stride=SLOT), :]
            extra_ref[pl.ds(comp * LAYERS + layer, ROWS, stride=EXTRA), :] = jnp.where(lane < X_ROWS, 0.0, line)
    fix_ref[...] = jnp.zeros_like(fix_ref)

    def store_sums(values, place):
        cos_out, sin_out = real_dft(values)
        for k in range(half + 1):
            sums_ref[pl.ds(k * P1_ALL + place, OWNED), :] = cos_out[k]
        for k in range(1, half):
            sums_ref[pl.ds((half + k) * P1_ALL + place, OWNED), :] = sin_out[k]

    def over_rows(index, carry):
        layer = index // COMPS
        comp = index % COMPS
        base = layer * (ROWS * SLOT) + comp * OWNED
        base = pl.multiple_of(base, OWNED)
        values = [x_ref[pl.ds(base + r * SLOT, OWNED), :] for r in range(ROWS)]
        store_sums(values, pl.multiple_of(index * OWNED, OWNED))
        return carry

    lax.fori_loop(0, LAYERS * COMPS, over_rows, 0)
    for group in range(2):
        values = [extra_ref[r * EXTRA + group * 8 : r * EXTRA + group * 8 + 8, :] for r in range(ROWS)]
        store_sums(values, P1_ROWS + group * 8)

    def factors(ref, p1, kind):
        base = kind * (ROWS * 4) + p1 * 4
        return [ref[pl.ds(base + j, 1), :] for j in range(4)]

    def save_pair(row, value):
        high, low = split_pair(value)
        pair_ref[pl.ds(row, value.shape[0]), :LANES] = high
        pair_ref[pl.ds(row, value.shape[0]), LANES:] = low

    kinds = [1 if j % COMPS == 2 else 0 for j in range(LAYERS * COMPS)] + [0, 1]

    def blocks(ref, row, count):
        return [ref[pl.ds(row + OWNED * j, OWNED), :] for j in range(count)]

    def twist(k, p1_list, with_sin):
        cos_rows = blocks(sums_ref, pl.multiple_of(k * P1_ALL, OWNED), len(kinds))
        cos_swap = [pltpu.roll(v, X_ROWS, 1) for v in cos_rows]
        if with_sin:
            sin_rows = blocks(sums_ref, pl.multiple_of((half + k) * P1_ALL, OWNED), len(kinds))
            sin_swap = [pltpu.roll(v, X_ROWS, 1) for v in sin_rows]
        for place, p1 in enumerate(p1_list):
            table = [factors(twiddle_ref, p1, kind) for kind in range(2)]
            out = []
            for j, kind in enumerate(kinds):
                f = table[kind]
                value = cos_rows[j] * f[0] + cos_swap[j] * f[1]
                if with_sin:
                    value = value + (sin_rows[j] * f[2] + sin_swap[j] * f[3])
                out.append(value)
            for j in range(0, len(kinds), 2):
                row = 2 * k * P1_ALL + place * P1_ALL + OWNED * j
                save_pair(pl.multiple_of(row, 2 * OWNED), jnp.concatenate(out[j : j + 2], axis=0))

    def forward_dot(k, first, second):
        rows = 2 * P1_ALL
        base = k * rows if isinstance(k, int) else pl.multiple_of(k * rows, 2 * OWNED)
        both = dot(pair_ref[pl.ds(base, rows), :], table_ref[...])
        whole_line = both[:, :LANES] + both[:, LANES:]
        spec_ref[pl.ds(first * P1_ALL, P1_ALL), :] = whole_line[:P1_ALL]
        spec_ref[pl.ds(second * P1_ALL, P1_ALL), :] = whole_line[P1_ALL:]

    twist(0, [0], False)
    cos_edge = blocks(sums_ref, half * P1_ALL, len(kinds))
    table = [factors(twiddle_ref, half, kind) for kind in range(2)]
    edge = [v * table[kind][0] + pltpu.roll(v, X_ROWS, 1) * table[kind][1] for v, kind in zip(cos_edge, kinds)]
    for j in range(0, len(kinds), 2):
        save_pair(P1_ALL + OWNED * j, jnp.concatenate(edge[j : j + 2], axis=0))
    forward_dot(0, 0, half)
    twist(1, [1, ROWS - 1], True)

    def twist_step(k, carry):
        forward_dot(k - 1, k - 1, ROWS + 1 - k)
        twist(k, [k, ROWS - k], True)
        return carry

    lax.fori_loop(2, half, twist_step, 0)
    forward_dot(half - 1, half - 1, half + 1)
    fetch.wait()

    def mix(spectra, coefficient, edge=False):
        fields = []
        for target in range(LAYERS):
            total = [None, None, None]

            def add(comp, term):
                total[comp] = term if total[comp] is None else total[comp] + term

            for source in range(LAYERS):
                offset = target - source + LAYERS - 1
                mx, my, mz = spectra[source]
                if edge:
                    k = [coefficient(offset * EDGE_PARTS + j) for j in range(EDGE_PARTS)]
                    add(0, k[0] * mx + k[3] * mz)
                    add(1, k[1] * my)
                    add(2, k[3] * mx - k[2] * mz)
                    continue
                k = [coefficient(offset * PARTS + j) for j in range(PARTS)]
                add(0, k[0] * mx + k[3] * my + k[4] * mz)
                add(1, k[3] * mx + k[1] * my + k[5] * mz)
                add(2, k[4] * mx + k[5] * my - k[2] * mz)
            fields.append(total)
        return fields

    def fix_step(group, carry):
        base = group * OWNED
        spectra = [
            [
                spec_ref[pl.ds(base * P1_ALL + P1_ROWS + comp * LAYERS + source, OWNED, stride=P1_ALL), :]
                for comp in range(COMPS)
            ]
            for source in range(LAYERS)
        ]

        def coefficient(op):
            return delta_ref[pl.ds(pl.multiple_of(op * ROWS + base, OWNED), OWNED), :]

        fields = mix(spectra, coefficient, edge=True)
        for target in range(LAYERS):
            for comp in range(COMPS):
                row = base * P1_ROWS + (target * COMPS + comp) * OWNED
                fix_ref[pl.ds(row, OWNED, stride=P1_ROWS), :] = fields[target][comp]
        return carry

    lax.fori_loop(0, ROWS // OWNED, fix_step, 0)

    def mix_line(p1):
        lines = blocks(spec_ref, p1 * P1_ALL, LAYERS * COMPS)
        spectra = [lines[COMPS * s : COMPS * s + COMPS] for s in range(LAYERS)]
        kernel_base = p1 * (OPS * OWNED)

        def coefficient(op):
            return kernel_ref[pl.ds(kernel_base + op * OWNED, OWNED), :]

        fields = mix(spectra, coefficient)
        flat = [fields[j // COMPS][j % COMPS] for j in range(LAYERS * COMPS)]
        row = p1 * P1_ROWS
        fixes = blocks(fix_ref, row, LAYERS * COMPS)
        flat = [a + b for a, b in zip(flat, fixes)]
        for j in range(0, LAYERS * COMPS, 2):
            save_pair(row + OWNED * j, jnp.concatenate(flat[j : j + 2], axis=0))

    def backward_dot(p1, rows):
        both = dot(pair_ref[pl.ds(p1 * P1_ROWS, rows), :], back_table_ref[...])
        back_ref[pl.ds(p1 * P1_ROWS, rows), :] = both[:, :LANES] + both[:, LANES:]

    mix_line(0)
    mix_line(1)

    def mix_step(step, carry):
        p1 = pl.multiple_of(2 * step, 2)
        backward_dot(p1 - 2, 2 * P1_ROWS)
        mix_line(p1)
        mix_line(p1 + 1)
        return carry

    lax.fori_loop(1, half, mix_step, 0)
    backward_dot(ROWS - 2, 2 * P1_ROWS)

    count = LAYERS * COMPS

    def untwist_edge(p1, slot):
        table = [factors(back_twiddle_ref, p1, kind) for kind in range(2)]
        for j, value in enumerate(blocks(back_ref, p1 * P1_ROWS, count)):
            f = table[kinds[j]]
            sums_ref[pl.ds(slot * P1_ROWS + OWNED * j, OWNED), :] = value * f[0] + pltpu.roll(value, X_ROWS, 1) * f[1]

    untwist_edge(0, 0)
    untwist_edge(half, half)

    def untwist_step(k, carry):
        near = [factors(back_twiddle_ref, k, kind) for kind in range(2)]
        far = [factors(back_twiddle_ref, ROWS - k, kind) for kind in range(2)]
        near_rows = blocks(back_ref, pl.multiple_of(k * P1_ROWS, OWNED), count)
        far_rows = blocks(back_ref, pl.multiple_of((ROWS - k) * P1_ROWS, OWNED), count)
        cos_base = pl.multiple_of(k * P1_ROWS, OWNED)
        sin_base = pl.multiple_of((half + k) * P1_ROWS, OWNED)
        for j in range(count):
            n, f = near[kinds[j]], far[kinds[j]]
            a, b = near_rows[j], far_rows[j]
            a_swap, b_swap = pltpu.roll(a, X_ROWS, 1), pltpu.roll(b, X_ROWS, 1)
            sums_ref[pl.ds(cos_base + OWNED * j, OWNED), :] = (a * n[0] + a_swap * n[1]) + (b * f[0] + b_swap * f[1])
            sums_ref[pl.ds(sin_base + OWNED * j, OWNED), :] = (a * n[2] + a_swap * n[3]) + (b * f[2] + b_swap * f[3])
        return carry

    lax.fori_loop(1, half, untwist_step, 0)

    def back_rows(index, carry):
        place = pl.multiple_of(index * OWNED, OWNED)
        cos_in = [sums_ref[pl.ds(k * P1_ROWS + place, OWNED), :] for k in range(half + 1)]
        sin_in = [None] + [sums_ref[pl.ds((half + k) * P1_ROWS + place, OWNED), :] for k in range(1, half)] + [None]
        values = real_sum(cos_in, sin_in, ROWS)
        layer = index // COMPS
        comp = index % COMPS
        base = pl.multiple_of(layer * (ROWS * SLOT) + comp * OWNED, OWNED)
        for r in range(ROWS):
            out_ref[pl.ds(base + r * SLOT, OWNED), :] = values[r]
        return carry

    lax.fori_loop(0, LAYERS * COMPS, back_rows, 0)


def inverse_y_kernel(x_ref, table_ref, twiddle_ref, out_hbm, high_ref, low_ref, lines_ref, result_ref, sem):
    half = DEVICES // 2
    middle = COARSE // 2
    group = 8
    lane = lax.broadcasted_iota(jnp.int32, (X_ROWS, LANES), 1)
    alternate = 1.0 - 2.0 * (lax.broadcasted_iota(jnp.int32, (group, FINE), 1) % 2).astype(F32)
    copies = []
    for comp in range(COMPS):
        size = (middle + 1) * X_ROWS
        base = comp * size

        def put(k, real, imag):
            rows = slice(base + k * X_ROWS, base + (k + 1) * X_ROWS)
            high_ref[rows, :LANES], low_ref[rows, :LANES] = split_pair(real)
            high_ref[rows, LANES:], low_ref[rows, LANES:] = split_pair(imag)

        for k in range(middle):
            near, far = slot_rows(comp, k)
            if k == 0:
                far = slot_rows(comp, middle)[1]
            block = jnp.concatenate([x_ref[near, :], x_ref[far, :]], axis=0).T
            real, imag = block[:X_ROWS], block[X_ROWS:]
            if k == 0:
                nyquist = imag[:, :1]
                put(middle, jnp.where(lane < half, 0.0, real), jnp.where(lane < half, 0.0, imag))
                scale = jnp.where(lane < half, jnp.where(lane == 0, 0.5, 1.0), 0.0)
                real, imag = real * scale, imag * scale
            put(k, real, imag)
        lines_ref[base : base + size, :] = triple_dot(
            high_ref[base : base + size, :], low_ref[base : base + size, :], table_ref
        )
        for g in range(X_ROWS // group):
            cos_in = [None] * (middle + 1)
            sin_in = [None] * (middle + 1)
            for k in range(middle + 1):
                rows = slice(base + k * X_ROWS + g * group, base + k * X_ROWS + (g + 1) * group)
                real = lines_ref[rows, :LANES]
                if k == 0:
                    cos_in[0] = 2.0 * real + nyquist[g * group : (g + 1) * group] * alternate
                    continue
                imag = lines_ref[rows, LANES:]
                cosine = twiddle_ref[2 * k - 2 : 2 * k - 1, :]
                sine = twiddle_ref[2 * k - 1 : 2 * k, :]
                cos_in[k] = real * cosine - imag * sine
                if k < middle:
                    sin_in[k] = -(real * sine + imag * cosine)
            values = real_sum(cos_in, sin_in, COARSE)
            top = comp * X_ROWS + g * group
            for a in range(COARSE):
                result_ref[top : top + group, FINE * a : FINE * (a + 1)] = values[a]
        span = pl.ds(comp * X_ROWS, X_ROWS)
        copy = pltpu.make_async_copy(result_ref.at[span], out_hbm.at[span], sem.at[comp])
        copy.start()
        copies.append(copy)
    for copy in copies:
        copy.wait()


VMEM = pl.BlockSpec(memory_space=pltpu.VMEM)
HBM = pl.BlockSpec(memory_space=pltpu.HBM)
FINE_ROWS = COMPS * (COARSE // 2 + 1) * X_ROWS


def params(mebibytes):
    return pltpu.CompilerParams(vmem_limit_bytes=mebibytes * 1024 * 1024)


def edge_lines(kernel):
    return pl.pallas_call(
        edge_kernel,
        in_specs=[HBM],
        out_specs=VMEM,
        out_shape=jax.ShapeDtypeStruct((EDGES, CELLS), F32),
        scratch_shapes=[
            pltpu.VMEM((CELLS // LANES, OFFSETS, EDGE_PARTS, OWNED, LANES), F32),
            pltpu.SemaphoreType.DMA((CELLS // LANES, 2)),
        ],
        compiler_params=params(58),
        name="edge_lines",
    )(kernel)


def forward_y(field):
    table = stacked(fine_table())
    twiddle = y_twiddle(-1.0, 1.0)
    return pl.pallas_call(
        forward_y_kernel,
        in_specs=[VMEM] * 3,
        out_specs=HBM,
        out_shape=jax.ShapeDtypeStruct((DEVICES, SLOT, LANES), F32),
        scratch_shapes=[
            pltpu.VMEM((FINE_ROWS, 2 * LANES), BF16),
            pltpu.VMEM((FINE_ROWS, 2 * LANES), BF16),
            pltpu.VMEM((DEVICES * SLOT, LANES), F32),
            pltpu.SemaphoreType.DMA((COMPS,)),
        ],
        compiler_params=params(48),
        name="forward_y",
    )(field, jnp.asarray(table), jnp.asarray(twiddle))


def relayout(kernel, flag):
    groups = 3
    rows = OPS // groups * 16
    out_rows = OPS // groups * OWNED
    return pl.pallas_call(
        relayout_kernel,
        grid=(groups,),
        in_specs=[
            pl.BlockSpec(memory_space=pltpu.SMEM),
            pl.BlockSpec((rows, CELLS), lambda g: (g, 0)),
        ],
        out_specs=pl.BlockSpec((ROWS, out_rows, LANES), lambda g: (0, g, 0)),
        out_shape=jax.ShapeDtypeStruct((ROWS, OPS * OWNED, LANES), F32),
        scratch_shapes=[pltpu.VMEM((out_rows, CELLS), F32), pltpu.VMEM((CELLS, LANES), F32)],
        compiler_params=params(48),
        name="relayout",
    )(flag, kernel)


def spectral(lines, kernel, delta):
    twiddle = x_twiddle(-1.0, 1.0)
    back_twiddle = x_twiddle(1.0, -1.0 / (CELLS * CELLS))
    return pl.pallas_call(
        spectral_kernel,
        in_specs=[VMEM, HBM] + [VMEM] * 5,
        out_specs=VMEM,
        out_shape=jax.ShapeDtypeStruct((DEVICES * SLOT, LANES), F32),
        scratch_shapes=[
            pltpu.VMEM((ROWS * OPS * OWNED, LANES), F32),
            pltpu.VMEM((ROWS * EXTRA, LANES), F32),
            pltpu.VMEM((ROWS * P1_ALL, LANES), F32),
            pltpu.VMEM((ROWS * P1_ALL, 2 * LANES), BF16),
            pltpu.VMEM((ROWS * P1_ALL, LANES), F32),
            pltpu.VMEM((ROWS * P1_ROWS, LANES), F32),
            pltpu.VMEM((ROWS * P1_ROWS, LANES), F32),
            pltpu.SemaphoreType.DMA,
        ],
        compiler_params=params(48),
        name="spectral",
    )(
        lines,
        kernel,
        delta,
        jnp.asarray(twiddle),
        jnp.asarray(back_twiddle),
        jnp.asarray(x_table(-1.0)),
        jnp.asarray(x_table(1.0)),
    )


def inverse_y(spectra):
    rows = COMPS * X_ROWS
    return pl.pallas_call(
        inverse_y_kernel,
        in_specs=[VMEM] * 3,
        out_specs=HBM,
        out_shape=jax.ShapeDtypeStruct((rows, CELLS), F32),
        scratch_shapes=[
            pltpu.VMEM((FINE_ROWS, 2 * LANES), BF16),
            pltpu.VMEM((FINE_ROWS, 2 * LANES), BF16),
            pltpu.VMEM((FINE_ROWS, 2 * LANES), F32),
            pltpu.VMEM((rows, CELLS), F32),
            pltpu.SemaphoreType.DMA((COMPS,)),
        ],
        compiler_params=params(20),
        name="inverse_y",
    )(spectra, jnp.asarray(stacked(fine_table().T)), jnp.asarray(y_twiddle(1.0, 2.0)))


def exchange(lines):
    moved = lax.all_to_all(lines.reshape(DEVICES, SLOT, LANES), ("layer", "row"), 0, 0, tiled=True)
    return moved.reshape(DEVICES * SLOT, LANES)


def local(magnet, kernel):
    axes = ("layer", "row")
    device = lax.axis_index(axes)
    field = magnet.reshape(COMPS * X_ROWS, CELLS)
    flag = (device >= DEVICES // 2).astype(jnp.int32).reshape(1)
    edge = edge_lines(kernel)
    middle = lax.ppermute(edge, axes, [(DEVICES // 2, 0)])
    sent = forward_y(field)
    got = exchange(sent)
    coefficient = relayout(kernel.reshape(OPS * 16, CELLS), flag)
    delta = jnp.where(device == 0, middle - edge, 0.0)
    delta = jnp.swapaxes(delta.reshape(EDGES, X_ROWS, ROWS), 1, 2)
    delta = jnp.concatenate([delta, delta], axis=2).reshape(EDGES * ROWS, LANES)
    fields = spectral(got, coefficient.reshape(ROWS * OPS * OWNED, LANES), delta)
    result = inverse_y(exchange(fields))
    return result.reshape(COMPS, 1, X_ROWS, CELLS)


def solution(mesh):
    in_specs = (P(None, "layer", "row", None), P(None, None, ("layer", "row"), None))
    out_specs = P(None, "layer", "row", None)
    return jax.shard_map(local, mesh=mesh, in_specs=in_specs, out_specs=out_specs, check_vma=False)
```

```python
import math

import jax
import jax.numpy as jnp
import numpy as np
from jax import lax
from jax.experimental import pallas as pl
from jax.experimental.pallas import tpu as pltpu
from jax.sharding import PartitionSpec as P


CELLS = 2048
COMPS = 3
LAYERS = 4
ROWS = 32
X_ROWS = 64
DEVICES = 128
PARTS = 6
OFFSETS = 7
OPS = OFFSETS * PARTS
FINE = 128
COARSE = 16
OWNED = 8
SLOT = COMPS * OWNED
LANES = 128
EXTRA = 16
P1_ROWS = LAYERS * COMPS * OWNED
P1_ALL = P1_ROWS + EXTRA

F32 = jnp.float32
BF16 = jnp.bfloat16


def halves(table):
    high = np.asarray(table, np.float32).astype(jnp.bfloat16)
    low = (np.asarray(table, np.float64) - high.astype(np.float64)).astype(np.float32).astype(jnp.bfloat16)
    return high, low


def fine_table():
    index = np.arange(FINE)
    angle = 2.0 * np.pi * (np.outer(index, index) % FINE) / FINE
    return np.block([[np.cos(angle), -np.sin(angle)], [np.sin(angle), np.cos(angle)]])


def stacked(table):
    return np.concatenate(halves(table), axis=0)


def y_twiddle(sign, scale):
    k = np.arange(1, COARSE // 2 + 1)[:, None]
    b = np.arange(FINE)[None, :]
    angle = 2.0 * np.pi * k * b / CELLS
    table = scale * np.stack([np.cos(angle), sign * np.sin(angle)], axis=1)
    return table.reshape(COARSE, FINE).astype(np.float32)


def lane_pair(coefficient):
    real = np.concatenate([coefficient.real, coefficient.real], axis=-1)
    imag = np.concatenate([-coefficient.imag, coefficient.imag], axis=-1)
    return real, imag


def x_twiddle(sign, scale):
    p1 = np.arange(ROWS)[:, None]
    t = np.arange(X_ROWS)[None, :]
    base = scale * np.exp(sign * 2.0j * np.pi * (p1 * t) / CELLS)
    side = np.where(p1 <= ROWS // 2, 1.0, -1.0) * (sign * 1.0j)
    kinds = []
    for kind in (1.0, 1.0j):
        first = lane_pair(kind * base)
        second = lane_pair(kind * base * side)
        kinds.append(np.stack(first + second, axis=1))
    return np.stack(kinds).astype(np.float32).reshape(2 * ROWS * 4, LANES)


def x_table(sign):
    index = np.arange(X_ROWS)
    angle = 2.0 * np.pi * (np.outer(index, index) % X_ROWS) / X_ROWS
    real = np.cos(angle)
    imag = sign * np.sin(angle)
    whole = np.block([[real, imag], [-imag, real]])
    high, low = halves(whole)
    line = np.concatenate([high, low], axis=1)
    return np.concatenate([line, line], axis=0)


def real_dft(values):
    n = len(values)
    if n == 1:
        return [values[0]], [None]
    if n == 2:
        return [values[0] + values[1], values[0] - values[1]], [None, None]
    even_c, even_s = real_dft(values[0::2])
    odd_c, odd_s = real_dft(values[1::2])
    half = n // 2
    quarter = n // 4
    cos_out = [None] * (half + 1)
    sin_out = [None] * (half + 1)
    for k in range(quarter + 1):
        if k == 0:
            cos_out[0] = even_c[0] + odd_c[0]
            cos_out[half] = even_c[0] - odd_c[0]
        elif k == quarter:
            cos_out[k] = even_c[k]
            sin_out[k] = odd_c[k]
        else:
            theta = 2.0 * math.pi * k / n
            cosine, sine = math.cos(theta), math.sin(theta)
            if 8 * k == n:
                real = cosine * (odd_c[k] - odd_s[k])
                imag = cosine * (odd_s[k] + odd_c[k])
            else:
                real = cosine * odd_c[k] - sine * odd_s[k]
                imag = cosine * odd_s[k] + sine * odd_c[k]
            cos_out[k] = even_c[k] + real
            sin_out[k] = even_s[k] + imag
            cos_out[half - k] = even_c[k] - real
            sin_out[half - k] = imag - even_s[k]
    return cos_out, sin_out


def real_sum(cos_in, sin_in, n):
    if n == 1:
        return [cos_in[0]]
    half = n // 2
    if n == 2:
        return [cos_in[0] + cos_in[1], cos_in[0] - cos_in[1]]
    quarter = n // 4
    even_c = [None] * (quarter + 1)
    even_s = [None] * (quarter + 1)
    odd_c = [None] * (quarter + 1)
    odd_s = [None] * (quarter + 1)
    even_c[0] = cos_in[0] + cos_in[half]
    odd_c[0] = cos_in[0] - cos_in[half]
    even_c[quarter] = cos_in[quarter]
    odd_c[quarter] = sin_in[quarter]
    for k in range(1, quarter):
        theta = 2.0 * math.pi * k / n
        cosine, sine = math.cos(theta), math.sin(theta)
        even_c[k] = cos_in[k] + cos_in[half - k]
        even_s[k] = sin_in[k] - sin_in[half - k]
        gap = cos_in[k] - cos_in[half - k]
        both = sin_in[k] + sin_in[half - k]
        if 8 * k == n:
            odd_c[k] = cosine * (gap + both)
            odd_s[k] = cosine * (both - gap)
        else:
            odd_c[k] = cosine * gap + sine * both
            odd_s[k] = cosine * both - sine * gap
    evens = real_sum(even_c, even_s, half)
    odds = real_sum(odd_c, odd_s, half)
    out = [None] * n
    out[0::2] = evens
    out[1::2] = odds
    return out


def split_pair(value):
    high = value.astype(BF16)
    low = (value - high.astype(F32)).astype(BF16)
    return high, low


def dot(left, right):
    return jnp.dot(left, right, preferred_element_type=F32)


def triple_dot(high, low, table_ref):
    size = table_ref.shape[0] // 2
    table_high, table_low = table_ref[:size, :], table_ref[size:, :]
    left = jnp.concatenate([high, low, high], axis=1)
    return dot(left, jnp.concatenate([table_high, table_high, table_low], axis=0))


def slot_rows(comp, k1):
    half = DEVICES // 2
    near = pl.ds(comp * OWNED + k1, half, stride=SLOT)
    far = pl.ds(half * SLOT + comp * OWNED + k1 - 1, half, stride=SLOT)
    return near, far


EDGE_PARTS = 4
EDGES = OFFSETS * EDGE_PARTS


def edge_kernel(kernel_hbm, out_ref, tiles_ref, sem):
    n_tiles = CELLS // LANES
    copies = []
    for j in range(n_tiles):
        lanes = pl.ds(LANES * j, LANES)
        for i, (source, target) in enumerate([((0, 3), (0, 3)), ((4, 1), (3, 1))]):
            copy = pltpu.make_async_copy(
                kernel_hbm.at[:, pl.ds(*source), pl.ds(0, OWNED), lanes],
                tiles_ref.at[j, :, pl.ds(*target)],
                sem.at[j, i],
            )
            copy.start()
            copies.append(copy)
    flat = tiles_ref.reshape(n_tiles * EDGES * OWNED, LANES)
    for j in range(n_tiles):
        copies[2 * j].wait()
        copies[2 * j + 1].wait()
        out_ref[:, LANES * j : LANES * (j + 1)] = flat[pl.ds(j * EDGES * OWNED, EDGES, stride=OWNED), :]


def forward_y_kernel(x_ref, table_ref, twiddle_ref, out_hbm, high_ref, low_ref, out_ref, sem):
    slots = out_ref.reshape(DEVICES, SLOT, LANES)
    saves = []
    half = DEVICES // 2
    middle = COARSE // 2
    group = 16
    lane = lax.broadcasted_iota(jnp.int32, (X_ROWS, LANES), 1)
    alternate = 1.0 - 2.0 * (lax.broadcasted_iota(jnp.int32, (X_ROWS, FINE), 1) % 2).astype(F32)
    for comp in range(COMPS):
        base = comp * (middle + 1) * X_ROWS
        nyquist = []
        for g in range(X_ROWS // group):
            top = comp * X_ROWS + g * group
            parts = [x_ref[top : top + group, FINE * a : FINE * (a + 1)] for a in range(COARSE)]
            cos_out, sin_out = real_dft(parts)
            nyquist.append(jnp.sum(cos_out[0] * alternate[:group], axis=1, keepdims=True))
            for k in range(middle + 1):
                rows = slice(base + k * X_ROWS + g * group, base + k * X_ROWS + (g + 1) * group)
                real = cos_out[k]
                imag = None
                if k > 0:
                    cosine = twiddle_ref[2 * k - 2 : 2 * k - 1, :]
                    sine = twiddle_ref[2 * k - 1 : 2 * k, :]
                    if k == middle:
                        real, imag = real * cosine, real * sine
                    else:
                        real, imag = real * cosine + sin_out[k] * sine, real * sine - sin_out[k] * cosine
                high_ref[rows, :LANES], low_ref[rows, :LANES] = split_pair(real)
                if imag is None:
                    zero = jnp.zeros((group, LANES), BF16)
                    high_ref[rows, LANES:], low_ref[rows, LANES:] = zero, zero
                else:
                    high_ref[rows, LANES:], low_ref[rows, LANES:] = split_pair(imag)
        size = (middle + 1) * X_ROWS
        out = triple_dot(high_ref[base : base + size, :], low_ref[base : base + size, :], table_ref)

        def pick(k):
            rows = out[k * X_ROWS : (k + 1) * X_ROWS]
            return rows[:, :LANES], rows[:, LANES:]

        for k in range(middle):
            real, imag = pick(k)
            if k == 0:
                last_real, last_imag = pick(middle)
                imag = jnp.where(lane == 0, jnp.concatenate(nyquist, axis=0), imag)
                real = jnp.where(lane < half, real, last_real)
                imag = jnp.where(lane < half, imag, last_imag)
            block = jnp.concatenate([real, imag], axis=0).T
            near, far = slot_rows(comp, k)
            if k == 0:
                far = slot_rows(comp, middle)[1]
            out_ref[near, :] = block[:half]
            out_ref[far, :] = block[half:]
        lines = (slice(None), pl.ds(comp * OWNED, OWNED))
        save = pltpu.make_async_copy(slots.at[lines], out_hbm.at[lines], sem.at[comp])
        save.start()
        saves.append(save)
    for save in saves:
        save.wait()


def relayout_kernel(flag_ref, kernel_ref, out_ref, rows_ref, columns_ref):
    shifted = flag_ref[0] > 0
    n_ops = kernel_ref.shape[0] // 16
    sub = lax.broadcasted_iota(jnp.int32, (OWNED, CELLS), 0)
    for op in range(n_ops):
        low = kernel_ref[16 * op : 16 * op + 8, :]
        high = kernel_ref[16 * op + 8 : 16 * op + 16, :]
        moved = jnp.where(sub < 7, pltpu.roll(low, 7, 0), pltpu.roll(high, 7, 0))
        rows_ref[8 * op : 8 * op + 8, :] = jnp.where(shifted, moved, low)
    for tile in range(CELLS // LANES):
        block = rows_ref[:, LANES * tile : LANES * (tile + 1)].T
        columns_ref[LANES * tile : LANES * (tile + 1), : 8 * n_ops] = block

    def step(p1, carry):
        column = columns_ref[pl.ds(p1, X_ROWS, stride=ROWS), :]
        both = jnp.concatenate([column, column], axis=0).T
        out_ref[p1] = both[: 8 * n_ops]
        return carry

    lax.fori_loop(0, ROWS, step, 0, unroll=4)


def spectral_kernel(
    x_ref,
    kernel_hbm,
    delta_ref,
    twiddle_ref,
    back_twiddle_ref,
    table_ref,
    back_table_ref,
    out_ref,
    kernel_ref,
    extra_ref,
    sums_ref,
    pair_ref,
    spec_ref,
    fix_ref,
    back_ref,
    kernel_sem,
):
    fetch = pltpu.make_async_copy(kernel_hbm, kernel_ref, kernel_sem)
    fetch.start()
    half = ROWS // 2
    lane = lax.broadcasted_iota(jnp.int32, (ROWS, LANES), 1)

    extra_ref[...] = jnp.zeros_like(extra_ref)
    for layer in range(LAYERS):
        for comp in range(COMPS):
            line = x_ref[pl.ds(layer * ROWS * SLOT + comp * OWNED, ROWS, stride=SLOT), :]
            extra_ref[pl.ds(comp * LAYERS + layer, ROWS, stride=EXTRA), :] = jnp.where(lane < X_ROWS, 0.0, line)
    fix_ref[...] = jnp.zeros_like(fix_ref)

    def store_sums(values, place):
        cos_out, sin_out = real_dft(values)
        for k in range(half + 1):
            sums_ref[pl.ds(k * P1_ALL + place, OWNED), :] = cos_out[k]
        for k in range(1, half):
            sums_ref[pl.ds((half + k) * P1_ALL + place, OWNED), :] = sin_out[k]

    def over_rows(index, carry):
        layer = index // COMPS
        comp = index % COMPS
        base = layer * (ROWS * SLOT) + comp * OWNED
        base = pl.multiple_of(base, OWNED)
        values = [x_ref[pl.ds(base + r * SLOT, OWNED), :] for r in range(ROWS)]
        store_sums(values, pl.multiple_of(index * OWNED, OWNED))
        return carry

    lax.fori_loop(0, LAYERS * COMPS, over_rows, 0)
    for group in range(2):
        values = [extra_ref[r * EXTRA + group * 8 : r * EXTRA + group * 8 + 8, :] for r in range(ROWS)]
        store_sums(values, P1_ROWS + group * 8)

    def factors(ref, p1, kind):
        base = kind * (ROWS * 4) + p1 * 4
        return [ref[pl.ds(base + j, 1), :] for j in range(4)]

    def save_pair(row, value):
        high, low = split_pair(value)
        pair_ref[pl.ds(row, value.shape[0]), :LANES] = high
        pair_ref[pl.ds(row, value.shape[0]), LANES:] = low

    kinds = [1 if j % COMPS == 2 else 0 for j in range(LAYERS * COMPS)] + [0, 1]

    def blocks(ref, row, count):
        return [ref[pl.ds(row + OWNED * j, OWNED), :] for j in range(count)]

    def twist(k, p1_list, with_sin):
        cos_rows = blocks(sums_ref, pl.multiple_of(k * P1_ALL, OWNED), len(kinds))
        cos_swap = [pltpu.roll(v, X_ROWS, 1) for v in cos_rows]
        if with_sin:
            sin_rows = blocks(sums_ref, pl.multiple_of((half + k) * P1_ALL, OWNED), len(kinds))
            sin_swap = [pltpu.roll(v, X_ROWS, 1) for v in sin_rows]
        for place, p1 in enumerate(p1_list):
            table = [factors(twiddle_ref, p1, kind) for kind in range(2)]
            out = []
            for j, kind in enumerate(kinds):
                f = table[kind]
                value = cos_rows[j] * f[0] + cos_swap[j] * f[1]
                if with_sin:
                    value = value + (sin_rows[j] * f[2] + sin_swap[j] * f[3])
                out.append(value)
            for j in range(0, len(kinds), 2):
                row = 2 * k * P1_ALL + place * P1_ALL + OWNED * j
                save_pair(pl.multiple_of(row, 2 * OWNED), jnp.concatenate(out[j : j + 2], axis=0))

    group = 5

    def forward_dot(k, count):
        rows = 2 * P1_ALL
        base = k * rows if isinstance(k, int) else pl.multiple_of(k * rows, 2 * OWNED)
        both = dot(pair_ref[pl.ds(base, count * rows), :], table_ref[...])
        lines = both[:, :LANES] + both[:, LANES:]
        for i in range(count):
            first = k + i
            second = half if count == 1 else ROWS - first
            spec_ref[pl.ds(first * P1_ALL, P1_ALL), :] = lines[i * rows : i * rows + P1_ALL]
            spec_ref[pl.ds(second * P1_ALL, P1_ALL), :] = lines[i * rows + P1_ALL : (i + 1) * rows]

    twist(0, [0], False)
    cos_edge = blocks(sums_ref, half * P1_ALL, len(kinds))
    table = [factors(twiddle_ref, half, kind) for kind in range(2)]
    edge = [v * table[kind][0] + pltpu.roll(v, X_ROWS, 1) * table[kind][1] for v, kind in zip(cos_edge, kinds)]
    for j in range(0, len(kinds), 2):
        save_pair(P1_ALL + OWNED * j, jnp.concatenate(edge[j : j + 2], axis=0))
    forward_dot(0, 1)
    for k in range(1, 1 + group):
        twist(k, [k, ROWS - k], True)

    def twist_step(step, carry):
        first = 1 + group * step
        forward_dot(first - group, group)
        for i in range(group):
            twist(first + i, [first + i, ROWS - first - i], True)
        return carry

    lax.fori_loop(1, (half - 1) // group, twist_step, 0)
    forward_dot(half - group, group)
    fetch.wait()

    def mix(spectra, coefficient, edge=False):
        fields = []
        for target in range(LAYERS):
            total = [None, None, None]

            def add(comp, term):
                total[comp] = term if total[comp] is None else total[comp] + term

            for source in range(LAYERS):
                offset = target - source + LAYERS - 1
                mx, my, mz = spectra[source]
                if edge:
                    k = [coefficient(offset * EDGE_PARTS + j) for j in range(EDGE_PARTS)]
                    add(0, k[0] * mx + k[3] * mz)
                    add(1, k[1] * my)
                    add(2, k[3] * mx - k[2] * mz)
                    continue
                k = [coefficient(offset * PARTS + j) for j in range(PARTS)]
                add(0, k[0] * mx + k[3] * my + k[4] * mz)
                add(1, k[3] * mx + k[1] * my + k[5] * mz)
                add(2, k[4] * mx + k[5] * my - k[2] * mz)
            fields.append(total)
        return fields

    def fix_step(group, carry):
        base = group * OWNED
        spectra = [
            [
                spec_ref[pl.ds(base * P1_ALL + P1_ROWS + comp * LAYERS + source, OWNED, stride=P1_ALL), :]
                for comp in range(COMPS)
            ]
            for source in range(LAYERS)
        ]

        def coefficient(op):
            return delta_ref[pl.ds(pl.multiple_of(op * ROWS + base, OWNED), OWNED), :]

        fields = mix(spectra, coefficient, edge=True)
        for target in range(LAYERS):
            for comp in range(COMPS):
                row = base * P1_ROWS + (target * COMPS + comp) * OWNED
                fix_ref[pl.ds(row, OWNED, stride=P1_ROWS), :] = fields[target][comp]
        return carry

    lax.fori_loop(0, ROWS // OWNED, fix_step, 0)

    def mix_line(p1):
        lines = blocks(spec_ref, p1 * P1_ALL, LAYERS * COMPS)
        spectra = [lines[COMPS * s : COMPS * s + COMPS] for s in range(LAYERS)]
        kernel_base = p1 * (OPS * OWNED)

        def coefficient(op):
            return kernel_ref[pl.ds(kernel_base + op * OWNED, OWNED), :]

        fields = mix(spectra, coefficient)
        flat = [fields[j // COMPS][j % COMPS] for j in range(LAYERS * COMPS)]
        row = p1 * P1_ROWS
        fixes = blocks(fix_ref, row, LAYERS * COMPS)
        flat = [a + b for a, b in zip(flat, fixes)]
        for j in range(0, LAYERS * COMPS, 2):
            save_pair(row + OWNED * j, jnp.concatenate(flat[j : j + 2], axis=0))

    def backward_dot(p1, rows):
        both = dot(pair_ref[pl.ds(p1 * P1_ROWS, rows), :], back_table_ref[...])
        back_ref[pl.ds(p1 * P1_ROWS, rows), :] = both[:, :LANES] + both[:, LANES:]

    span = 8
    for p1 in range(span):
        mix_line(p1)

    def mix_step(step, carry):
        p1 = pl.multiple_of(span * step, span)
        backward_dot(p1 - span, span * P1_ROWS)
        for i in range(span):
            mix_line(p1 + i)
        return carry

    lax.fori_loop(1, ROWS // span, mix_step, 0)
    backward_dot(ROWS - span, span * P1_ROWS)

    count = LAYERS * COMPS

    def untwist_edge(p1, slot):
        table = [factors(back_twiddle_ref, p1, kind) for kind in range(2)]
        for j, value in enumerate(blocks(back_ref, p1 * P1_ROWS, count)):
            f = table[kinds[j]]
            sums_ref[pl.ds(slot * P1_ROWS + OWNED * j, OWNED), :] = value * f[0] + pltpu.roll(value, X_ROWS, 1) * f[1]

    untwist_edge(0, 0)
    untwist_edge(half, half)

    def untwist_step(k, carry):
        near = [factors(back_twiddle_ref, k, kind) for kind in range(2)]
        far = [factors(back_twiddle_ref, ROWS - k, kind) for kind in range(2)]
        near_rows = blocks(back_ref, pl.multiple_of(k * P1_ROWS, OWNED), count)
        far_rows = blocks(back_ref, pl.multiple_of((ROWS - k) * P1_ROWS, OWNED), count)
        cos_base = pl.multiple_of(k * P1_ROWS, OWNED)
        sin_base = pl.multiple_of((half + k) * P1_ROWS, OWNED)
        for j in range(count):
            n, f = near[kinds[j]], far[kinds[j]]
            a, b = near_rows[j], far_rows[j]
            a_swap, b_swap = pltpu.roll(a, X_ROWS, 1), pltpu.roll(b, X_ROWS, 1)
            sums_ref[pl.ds(cos_base + OWNED * j, OWNED), :] = (a * n[0] + a_swap * n[1]) + (b * f[0] + b_swap * f[1])
            sums_ref[pl.ds(sin_base + OWNED * j, OWNED), :] = (a * n[2] + a_swap * n[3]) + (b * f[2] + b_swap * f[3])
        return carry

    lax.fori_loop(1, half, untwist_step, 0)

    def back_rows(index, carry):
        place = pl.multiple_of(index * OWNED, OWNED)
        cos_in = [sums_ref[pl.ds(k * P1_ROWS + place, OWNED), :] for k in range(half + 1)]
        sin_in = [None] + [sums_ref[pl.ds((half + k) * P1_ROWS + place, OWNED), :] for k in range(1, half)] + [None]
        values = real_sum(cos_in, sin_in, ROWS)
        layer = index // COMPS
        comp = index % COMPS
        base = pl.multiple_of(layer * (ROWS * SLOT) + comp * OWNED, OWNED)
        for r in range(ROWS):
            out_ref[pl.ds(base + r * SLOT, OWNED), :] = values[r]
        return carry

    lax.fori_loop(0, LAYERS * COMPS, back_rows, 0)


def inverse_y_kernel(x_ref, table_ref, twiddle_ref, out_hbm, high_ref, low_ref, lines_ref, result_ref, sem):
    half = DEVICES // 2
    middle = COARSE // 2
    group = 8
    lane = lax.broadcasted_iota(jnp.int32, (X_ROWS, LANES), 1)
    alternate = 1.0 - 2.0 * (lax.broadcasted_iota(jnp.int32, (group, FINE), 1) % 2).astype(F32)
    copies = []
    for comp in range(COMPS):
        size = (middle + 1) * X_ROWS
        base = comp * size

        def put(k, real, imag):
            rows = slice(base + k * X_ROWS, base + (k + 1) * X_ROWS)
            high_ref[rows, :LANES], low_ref[rows, :LANES] = split_pair(real)
            high_ref[rows, LANES:], low_ref[rows, LANES:] = split_pair(imag)

        for k in range(middle):
            near, far = slot_rows(comp, k)
            if k == 0:
                far = slot_rows(comp, middle)[1]
            block = jnp.concatenate([x_ref[near, :], x_ref[far, :]], axis=0).T
            real, imag = block[:X_ROWS], block[X_ROWS:]
            if k == 0:
                nyquist = imag[:, :1]
                put(middle, jnp.where(lane < half, 0.0, real), jnp.where(lane < half, 0.0, imag))
                scale = jnp.where(lane < half, jnp.where(lane == 0, 0.5, 1.0), 0.0)
                real, imag = real * scale, imag * scale
            put(k, real, imag)
        lines_ref[base : base + size, :] = triple_dot(
            high_ref[base : base + size, :], low_ref[base : base + size, :], table_ref
        )
        for g in range(X_ROWS // group):
            cos_in = [None] * (middle + 1)
            sin_in = [None] * (middle + 1)
            for k in range(middle + 1):
                rows = slice(base + k * X_ROWS + g * group, base + k * X_ROWS + (g + 1) * group)
                real = lines_ref[rows, :LANES]
                if k == 0:
                    cos_in[0] = 2.0 * real + nyquist[g * group : (g + 1) * group] * alternate
                    continue
                imag = lines_ref[rows, LANES:]
                cosine = twiddle_ref[2 * k - 2 : 2 * k - 1, :]
                sine = twiddle_ref[2 * k - 1 : 2 * k, :]
                cos_in[k] = real * cosine - imag * sine
                if k < middle:
                    sin_in[k] = -(real * sine + imag * cosine)
            values = real_sum(cos_in, sin_in, COARSE)
            top = comp * X_ROWS + g * group
            for a in range(COARSE):
                result_ref[top : top + group, FINE * a : FINE * (a + 1)] = values[a]
        span = pl.ds(comp * X_ROWS, X_ROWS)
        copy = pltpu.make_async_copy(result_ref.at[span], out_hbm.at[span], sem.at[comp])
        copy.start()
        copies.append(copy)
    for copy in copies:
        copy.wait()


VMEM = pl.BlockSpec(memory_space=pltpu.VMEM)
HBM = pl.BlockSpec(memory_space=pltpu.HBM)
FINE_ROWS = COMPS * (COARSE // 2 + 1) * X_ROWS


def params(mebibytes):
    return pltpu.CompilerParams(vmem_limit_bytes=mebibytes * 1024 * 1024)


def edge_lines(kernel):
    return pl.pallas_call(
        edge_kernel,
        in_specs=[HBM],
        out_specs=VMEM,
        out_shape=jax.ShapeDtypeStruct((EDGES, CELLS), F32),
        scratch_shapes=[
            pltpu.VMEM((CELLS // LANES, OFFSETS, EDGE_PARTS, OWNED, LANES), F32),
            pltpu.SemaphoreType.DMA((CELLS // LANES, 2)),
        ],
        compiler_params=params(58),
        name="edge_lines",
    )(kernel)


def forward_y(field):
    table = stacked(fine_table())
    twiddle = y_twiddle(-1.0, 1.0)
    return pl.pallas_call(
        forward_y_kernel,
        in_specs=[VMEM] * 3,
        out_specs=HBM,
        out_shape=jax.ShapeDtypeStruct((DEVICES, SLOT, LANES), F32),
        scratch_shapes=[
            pltpu.VMEM((FINE_ROWS, 2 * LANES), BF16),
            pltpu.VMEM((FINE_ROWS, 2 * LANES), BF16),
            pltpu.VMEM((DEVICES * SLOT, LANES), F32),
            pltpu.SemaphoreType.DMA((COMPS,)),
        ],
        compiler_params=params(48),
        name="forward_y",
    )(field, jnp.asarray(table), jnp.asarray(twiddle))


def relayout(kernel, flag):
    groups = 3
    rows = OPS // groups * 16
    out_rows = OPS // groups * OWNED
    return pl.pallas_call(
        relayout_kernel,
        grid=(groups,),
        in_specs=[
            pl.BlockSpec(memory_space=pltpu.SMEM),
            pl.BlockSpec((rows, CELLS), lambda g: (g, 0)),
        ],
        out_specs=pl.BlockSpec((ROWS, out_rows, LANES), lambda g: (0, g, 0)),
        out_shape=jax.ShapeDtypeStruct((ROWS, OPS * OWNED, LANES), F32),
        scratch_shapes=[pltpu.VMEM((out_rows, CELLS), F32), pltpu.VMEM((CELLS, LANES), F32)],
        compiler_params=params(48),
        name="relayout",
    )(flag, kernel)


def spectral(lines, kernel, delta):
    twiddle = x_twiddle(-1.0, 1.0)
    back_twiddle = x_twiddle(1.0, -1.0 / (CELLS * CELLS))
    return pl.pallas_call(
        spectral_kernel,
        in_specs=[VMEM, HBM] + [VMEM] * 5,
        out_specs=VMEM,
        out_shape=jax.ShapeDtypeStruct((DEVICES * SLOT, LANES), F32),
        scratch_shapes=[
            pltpu.VMEM((ROWS * OPS * OWNED, LANES), F32),
            pltpu.VMEM((ROWS * EXTRA, LANES), F32),
            pltpu.VMEM((ROWS * P1_ALL, LANES), F32),
            pltpu.VMEM((ROWS * P1_ALL, 2 * LANES), BF16),
            pltpu.VMEM((ROWS * P1_ALL, LANES), F32),
            pltpu.VMEM((ROWS * P1_ROWS, LANES), F32),
            pltpu.VMEM((ROWS * P1_ROWS, LANES), F32),
            pltpu.SemaphoreType.DMA,
        ],
        compiler_params=params(48),
        name="spectral",
    )(
        lines,
        kernel,
        delta,
        jnp.asarray(twiddle),
        jnp.asarray(back_twiddle),
        jnp.asarray(x_table(-1.0)),
        jnp.asarray(x_table(1.0)),
    )


def inverse_y(spectra):
    rows = COMPS * X_ROWS
    return pl.pallas_call(
        inverse_y_kernel,
        in_specs=[VMEM] * 3,
        out_specs=HBM,
        out_shape=jax.ShapeDtypeStruct((rows, CELLS), F32),
        scratch_shapes=[
            pltpu.VMEM((FINE_ROWS, 2 * LANES), BF16),
            pltpu.VMEM((FINE_ROWS, 2 * LANES), BF16),
            pltpu.VMEM((FINE_ROWS, 2 * LANES), F32),
            pltpu.VMEM((rows, CELLS), F32),
            pltpu.SemaphoreType.DMA((COMPS,)),
        ],
        compiler_params=params(20),
        name="inverse_y",
    )(spectra, jnp.asarray(stacked(fine_table().T)), jnp.asarray(y_twiddle(1.0, 2.0)))


def exchange(lines):
    moved = lax.all_to_all(lines.reshape(DEVICES, SLOT, LANES), ("layer", "row"), 0, 0, tiled=True)
    return moved.reshape(DEVICES * SLOT, LANES)


def local(magnet, kernel):
    axes = ("layer", "row")
    device = lax.axis_index(axes)
    field = magnet.reshape(COMPS * X_ROWS, CELLS)
    flag = (device >= DEVICES // 2).astype(jnp.int32).reshape(1)
    edge = edge_lines(kernel)
    middle = lax.ppermute(edge, axes, [(DEVICES // 2, 0)])
    sent = forward_y(field)
    got = exchange(sent)
    coefficient = relayout(kernel.reshape(OPS * 16, CELLS), flag)
    delta = jnp.where(device == 0, middle - edge, 0.0)
    delta = jnp.swapaxes(delta.reshape(EDGES, X_ROWS, ROWS), 1, 2)
    delta = jnp.concatenate([delta, delta], axis=2).reshape(EDGES * ROWS, LANES)
    fields = spectral(got, coefficient.reshape(ROWS * OPS * OWNED, LANES), delta)
    result = inverse_y(exchange(fields))
    return result.reshape(COMPS, 1, X_ROWS, CELLS)


def solution(mesh):
    in_specs = (P(None, "layer", "row", None), P(None, None, ("layer", "row"), None))
    out_specs = P(None, "layer", "row", None)
    return jax.shard_map(local, mesh=mesh, in_specs=in_specs, out_specs=out_specs, check_vma=False)
```

```python
import math

import jax
import jax.numpy as jnp
import numpy as np
from jax import lax
from jax.experimental import pallas as pl
from jax.experimental.pallas import tpu as pltpu
from jax.sharding import PartitionSpec as P


CELLS = 2048
COMPS = 3
LAYERS = 4
ROWS = 32
X_ROWS = 64
DEVICES = 128
PARTS = 6
OFFSETS = 7
OPS = OFFSETS * PARTS
FINE = 128
COARSE = 16
OWNED = 8
SLOT = COMPS * OWNED
LANES = 128
EXTRA = 16
P1_ROWS = LAYERS * COMPS * OWNED
P1_ALL = P1_ROWS + EXTRA

F32 = jnp.float32
BF16 = jnp.bfloat16


def halves(table):
    high = np.asarray(table, np.float32).astype(jnp.bfloat16)
    low = (np.asarray(table, np.float64) - high.astype(np.float64)).astype(np.float32).astype(jnp.bfloat16)
    return high, low


def fine_table():
    index = np.arange(FINE)
    angle = 2.0 * np.pi * (np.outer(index, index) % FINE) / FINE
    return np.block([[np.cos(angle), -np.sin(angle)], [np.sin(angle), np.cos(angle)]])


def stacked(table):
    return np.concatenate(halves(table), axis=0)


def y_twiddle(sign, scale):
    k = np.arange(1, COARSE // 2 + 1)[:, None]
    b = np.arange(FINE)[None, :]
    angle = 2.0 * np.pi * k * b / CELLS
    table = scale * np.stack([np.cos(angle), sign * np.sin(angle)], axis=1)
    return table.reshape(COARSE, FINE).astype(np.float32)


def lane_pair(coefficient):
    real = np.concatenate([coefficient.real, coefficient.real], axis=-1)
    imag = np.concatenate([-coefficient.imag, coefficient.imag], axis=-1)
    return real, imag


def x_twiddle(sign, scale):
    p1 = np.arange(ROWS)[:, None]
    t = np.arange(X_ROWS)[None, :]
    base = scale * np.exp(sign * 2.0j * np.pi * (p1 * t) / CELLS)
    side = np.where(p1 <= ROWS // 2, 1.0, -1.0) * (sign * 1.0j)
    kinds = []
    for kind in (1.0, 1.0j):
        first = lane_pair(kind * base)
        second = lane_pair(kind * base * side)
        kinds.append(np.stack(first + second, axis=1))
    return np.stack(kinds).astype(np.float32).reshape(2 * ROWS * 4, LANES)


def x_table(sign):
    index = np.arange(X_ROWS)
    angle = 2.0 * np.pi * (np.outer(index, index) % X_ROWS) / X_ROWS
    real = np.cos(angle)
    imag = sign * np.sin(angle)
    whole = np.block([[real, imag], [-imag, real]])
    high, low = halves(whole)
    line = np.concatenate([high, low], axis=1)
    return np.concatenate([line, line], axis=0)


def real_dft(values):
    n = len(values)
    if n == 1:
        return [values[0]], [None]
    if n == 2:
        return [values[0] + values[1], values[0] - values[1]], [None, None]
    even_c, even_s = real_dft(values[0::2])
    odd_c, odd_s = real_dft(values[1::2])
    half = n // 2
    quarter = n // 4
    cos_out = [None] * (half + 1)
    sin_out = [None] * (half + 1)
    for k in range(quarter + 1):
        if k == 0:
            cos_out[0] = even_c[0] + odd_c[0]
            cos_out[half] = even_c[0] - odd_c[0]
        elif k == quarter:
            cos_out[k] = even_c[k]
            sin_out[k] = odd_c[k]
        else:
            theta = 2.0 * math.pi * k / n
            cosine, sine = math.cos(theta), math.sin(theta)
            if 8 * k == n:
                real = cosine * (odd_c[k] - odd_s[k])
                imag = cosine * (odd_s[k] + odd_c[k])
            else:
                real = cosine * odd_c[k] - sine * odd_s[k]
                imag = cosine * odd_s[k] + sine * odd_c[k]
            cos_out[k] = even_c[k] + real
            sin_out[k] = even_s[k] + imag
            cos_out[half - k] = even_c[k] - real
            sin_out[half - k] = imag - even_s[k]
    return cos_out, sin_out


def real_sum(cos_in, sin_in, n):
    if n == 1:
        return [cos_in[0]]
    half = n // 2
    if n == 2:
        return [cos_in[0] + cos_in[1], cos_in[0] - cos_in[1]]
    quarter = n // 4
    even_c = [None] * (quarter + 1)
    even_s = [None] * (quarter + 1)
    odd_c = [None] * (quarter + 1)
    odd_s = [None] * (quarter + 1)
    even_c[0] = cos_in[0] + cos_in[half]
    odd_c[0] = cos_in[0] - cos_in[half]
    even_c[quarter] = cos_in[quarter]
    odd_c[quarter] = sin_in[quarter]
    for k in range(1, quarter):
        theta = 2.0 * math.pi * k / n
        cosine, sine = math.cos(theta), math.sin(theta)
        even_c[k] = cos_in[k] + cos_in[half - k]
        even_s[k] = sin_in[k] - sin_in[half - k]
        gap = cos_in[k] - cos_in[half - k]
        both = sin_in[k] + sin_in[half - k]
        if 8 * k == n:
            odd_c[k] = cosine * (gap + both)
            odd_s[k] = cosine * (both - gap)
        else:
            odd_c[k] = cosine * gap + sine * both
            odd_s[k] = cosine * both - sine * gap
    evens = real_sum(even_c, even_s, half)
    odds = real_sum(odd_c, odd_s, half)
    out = [None] * n
    out[0::2] = evens
    out[1::2] = odds
    return out


def split_pair(value):
    high = value.astype(BF16)
    low = (value - high.astype(F32)).astype(BF16)
    return high, low


def dot(left, right):
    return jnp.dot(left, right, preferred_element_type=F32)


def triple_dot(high, low, table_ref):
    size = table_ref.shape[0] // 2
    table_high, table_low = table_ref[:size, :], table_ref[size:, :]
    left = jnp.concatenate([high, low, high], axis=1)
    return dot(left, jnp.concatenate([table_high, table_high, table_low], axis=0))


def slot_rows(comp, k1):
    half = DEVICES // 2
    near = pl.ds(comp * OWNED + k1, half, stride=SLOT)
    far = pl.ds(half * SLOT + comp * OWNED + k1 - 1, half, stride=SLOT)
    return near, far


EDGE_PARTS = 4
EDGES = OFFSETS * EDGE_PARTS


def edge_kernel(kernel_hbm, out_ref, tiles_ref, sem):
    n_tiles = CELLS // LANES
    copies = []
    for j in range(n_tiles):
        lanes = pl.ds(LANES * j, LANES)
        for i, (source, target) in enumerate([((0, 3), (0, 3)), ((4, 1), (3, 1))]):
            copy = pltpu.make_async_copy(
                kernel_hbm.at[:, pl.ds(*source), pl.ds(0, 1), lanes],
                tiles_ref.at[j, :, pl.ds(*target)],
                sem.at[j, i],
            )
            copy.start()
            copies.append(copy)
    flat = tiles_ref.reshape(n_tiles * EDGES, LANES)
    for j in range(n_tiles):
        copies[2 * j].wait()
        copies[2 * j + 1].wait()
        out_ref[:, LANES * j : LANES * (j + 1)] = flat[pl.ds(j * EDGES, EDGES), :]


def forward_y_kernel(x_ref, table_ref, twiddle_ref, out_hbm, high_ref, low_ref, out_ref, sem):
    slots = out_ref.reshape(DEVICES, SLOT, LANES)
    saves = []
    edges = []
    half = DEVICES // 2
    middle = COARSE // 2
    group = 16
    lane = lax.broadcasted_iota(jnp.int32, (X_ROWS, LANES), 1)
    alternate = 1.0 - 2.0 * (lax.broadcasted_iota(jnp.int32, (X_ROWS, FINE), 1) % 2).astype(F32)
    for comp in range(COMPS):
        base = comp * (middle + 1) * X_ROWS
        nyquist = []
        for g in range(X_ROWS // group):
            top = comp * X_ROWS + g * group
            parts = [x_ref[top : top + group, FINE * a : FINE * (a + 1)] for a in range(COARSE)]
            cos_out, sin_out = real_dft(parts)
            nyquist.append(jnp.sum(cos_out[0] * alternate[:group], axis=1, keepdims=True))
            for k in range(middle + 1):
                rows = slice(base + k * X_ROWS + g * group, base + k * X_ROWS + (g + 1) * group)
                real = cos_out[k]
                imag = None
                if k > 0:
                    cosine = twiddle_ref[2 * k - 2 : 2 * k - 1, :]
                    sine = twiddle_ref[2 * k - 1 : 2 * k, :]
                    if k == middle:
                        real, imag = real * cosine, real * sine
                    else:
                        real, imag = real * cosine + sin_out[k] * sine, real * sine - sin_out[k] * cosine
                high_ref[rows, :LANES], low_ref[rows, :LANES] = split_pair(real)
                if imag is None:
                    zero = jnp.zeros((group, LANES), BF16)
                    high_ref[rows, LANES:], low_ref[rows, LANES:] = zero, zero
                else:
                    high_ref[rows, LANES:], low_ref[rows, LANES:] = split_pair(imag)
        edges.append(jnp.concatenate(nyquist, axis=0))
    out = triple_dot(high_ref[...], low_ref[...], table_ref)
    for comp in range(COMPS):

        def pick(k):
            row = (comp * (middle + 1) + k) * X_ROWS
            rows = out[row : row + X_ROWS]
            return rows[:, :LANES], rows[:, LANES:]

        for k in range(middle):
            real, imag = pick(k)
            if k == 0:
                last_real, last_imag = pick(middle)
                imag = jnp.where(lane == 0, edges[comp], imag)
                real = jnp.where(lane < half, real, last_real)
                imag = jnp.where(lane < half, imag, last_imag)
            block = jnp.concatenate([real, imag], axis=0).T
            near, far = slot_rows(comp, k)
            if k == 0:
                far = slot_rows(comp, middle)[1]
            out_ref[near, :] = block[:half]
            out_ref[far, :] = block[half:]
        lines = (slice(None), pl.ds(comp * OWNED, OWNED))
        save = pltpu.make_async_copy(slots.at[lines], out_hbm.at[lines], sem.at[comp])
        save.start()
        saves.append(save)
    for save in saves:
        save.wait()


def relayout_kernel(flag_ref, kernel_ref, out_ref, rows_ref, columns_ref):
    shifted = flag_ref[0] > 0
    n_ops = kernel_ref.shape[0] // 16
    sub = lax.broadcasted_iota(jnp.int32, (OWNED, CELLS), 0)
    for op in range(n_ops):
        low = kernel_ref[16 * op : 16 * op + 8, :]
        high = kernel_ref[16 * op + 8 : 16 * op + 16, :]
        moved = jnp.where(sub < 7, pltpu.roll(low, 7, 0), pltpu.roll(high, 7, 0))
        rows_ref[8 * op : 8 * op + 8, :] = jnp.where(shifted, moved, low)
    for tile in range(CELLS // LANES):
        block = rows_ref[:, LANES * tile : LANES * (tile + 1)].T
        columns_ref[LANES * tile : LANES * (tile + 1), : 8 * n_ops] = block

    def step(p1, carry):
        column = columns_ref[pl.ds(p1, X_ROWS, stride=ROWS), :]
        both = jnp.concatenate([column, column], axis=0).T
        out_ref[p1] = both[: 8 * n_ops]
        return carry

    lax.fori_loop(0, ROWS, step, 0, unroll=4)


def spectral_kernel(
    x_ref,
    kernel_hbm,
    delta_ref,
    twiddle_ref,
    back_twiddle_ref,
    table_ref,
    back_table_ref,
    out_ref,
    kernel_ref,
    extra_ref,
    sums_ref,
    pair_ref,
    spec_ref,
    fix_ref,
    back_ref,
    kernel_sem,
):
    fetch = pltpu.make_async_copy(kernel_hbm, kernel_ref, kernel_sem)
    fetch.start()
    half = ROWS // 2
    lane = lax.broadcasted_iota(jnp.int32, (ROWS, LANES), 1)

    extra_ref[...] = jnp.zeros_like(extra_ref)
    for layer in range(LAYERS):
        for comp in range(COMPS):
            line = x_ref[pl.ds(layer * ROWS * SLOT + comp * OWNED, ROWS, stride=SLOT), :]
            extra_ref[pl.ds(comp * LAYERS + layer, ROWS, stride=EXTRA), :] = jnp.where(lane < X_ROWS, 0.0, line)
    fix_ref[...] = jnp.zeros_like(fix_ref)

    def store_sums(values, place):
        cos_out, sin_out = real_dft(values)
        for k in range(half + 1):
            sums_ref[pl.ds(k * P1_ALL + place, OWNED), :] = cos_out[k]
        for k in range(1, half):
            sums_ref[pl.ds((half + k) * P1_ALL + place, OWNED), :] = sin_out[k]

    def over_rows(index, carry):
        layer = index // COMPS
        comp = index % COMPS
        base = layer * (ROWS * SLOT) + comp * OWNED
        base = pl.multiple_of(base, OWNED)
        values = [x_ref[pl.ds(base + r * SLOT, OWNED), :] for r in range(ROWS)]
        store_sums(values, pl.multiple_of(index * OWNED, OWNED))
        return carry

    lax.fori_loop(0, LAYERS * COMPS, over_rows, 0)
    for group in range(2):
        values = [extra_ref[r * EXTRA + group * 8 : r * EXTRA + group * 8 + 8, :] for r in range(ROWS)]
        store_sums(values, P1_ROWS + group * 8)

    def factors(ref, p1, kind):
        base = kind * (ROWS * 4) + p1 * 4
        return [ref[pl.ds(base + j, 1), :] for j in range(4)]

    def save_pair(row, value):
        high, low = split_pair(value)
        pair_ref[pl.ds(row, value.shape[0]), :LANES] = high
        pair_ref[pl.ds(row, value.shape[0]), LANES:] = low

    kinds = [1 if j % COMPS == 2 else 0 for j in range(LAYERS * COMPS)] + [0, 1]

    def blocks(ref, row, count):
        return [ref[pl.ds(row + OWNED * j, OWNED), :] for j in range(count)]

    def twist(k, p1_list, with_sin):
        cos_rows = blocks(sums_ref, pl.multiple_of(k * P1_ALL, OWNED), len(kinds))
        cos_swap = [pltpu.roll(v, X_ROWS, 1) for v in cos_rows]
        if with_sin:
            sin_rows = blocks(sums_ref, pl.multiple_of((half + k) * P1_ALL, OWNED), len(kinds))
            sin_swap = [pltpu.roll(v, X_ROWS, 1) for v in sin_rows]
        for place, p1 in enumerate(p1_list):
            table = [factors(twiddle_ref, p1, kind) for kind in range(2)]
            out = []
            for j, kind in enumerate(kinds):
                f = table[kind]
                value = cos_rows[j] * f[0] + cos_swap[j] * f[1]
                if with_sin:
                    value = value + (sin_rows[j] * f[2] + sin_swap[j] * f[3])
                out.append(value)
            for j in range(0, len(kinds), 2):
                row = 2 * k * P1_ALL + place * P1_ALL + OWNED * j
                save_pair(pl.multiple_of(row, 2 * OWNED), jnp.concatenate(out[j : j + 2], axis=0))

    group = 5

    def forward_dot(k, count):
        rows = 2 * P1_ALL
        base = k * rows if isinstance(k, int) else pl.multiple_of(k * rows, 2 * OWNED)
        both = dot(pair_ref[pl.ds(base, count * rows), :], table_ref[...])
        lines = both[:, :LANES] + both[:, LANES:]
        for i in range(count):
            first = k + i
            second = half if count == 1 else ROWS - first
            spec_ref[pl.ds(first * P1_ALL, P1_ALL), :] = lines[i * rows : i * rows + P1_ALL]
            spec_ref[pl.ds(second * P1_ALL, P1_ALL), :] = lines[i * rows + P1_ALL : (i + 1) * rows]

    twist(0, [0], False)
    cos_edge = blocks(sums_ref, half * P1_ALL, len(kinds))
    table = [factors(twiddle_ref, half, kind) for kind in range(2)]
    edge = [v * table[kind][0] + pltpu.roll(v, X_ROWS, 1) * table[kind][1] for v, kind in zip(cos_edge, kinds)]
    for j in range(0, len(kinds), 2):
        save_pair(P1_ALL + OWNED * j, jnp.concatenate(edge[j : j + 2], axis=0))
    forward_dot(0, 1)
    for k in range(1, 1 + group):
        twist(k, [k, ROWS - k], True)

    def twist_step(step, carry):
        first = 1 + group * step
        forward_dot(first - group, group)
        for i in range(group):
            twist(first + i, [first + i, ROWS - first - i], True)
        return carry

    lax.fori_loop(1, (half - 1) // group, twist_step, 0)
    forward_dot(half - group, group)
    fetch.wait()

    def mix(spectra, coefficient, edge=False):
        fields = []
        for target in range(LAYERS):
            total = [None, None, None]

            def add(comp, term):
                total[comp] = term if total[comp] is None else total[comp] + term

            for source in range(LAYERS):
                offset = target - source + LAYERS - 1
                mx, my, mz = spectra[source]
                if edge:
                    k = [coefficient(offset * EDGE_PARTS + j) for j in range(EDGE_PARTS)]
                    add(0, k[0] * mx + k[3] * mz)
                    add(1, k[1] * my)
                    add(2, k[3] * mx - k[2] * mz)
                    continue
                k = [coefficient(offset * PARTS + j) for j in range(PARTS)]
                add(0, k[0] * mx + k[3] * my + k[4] * mz)
                add(1, k[3] * mx + k[1] * my + k[5] * mz)
                add(2, k[4] * mx + k[5] * my - k[2] * mz)
            fields.append(total)
        return fields

    def fix_step(group, carry):
        base = group * OWNED
        spectra = [
            [
                spec_ref[pl.ds(base * P1_ALL + P1_ROWS + comp * LAYERS + source, OWNED, stride=P1_ALL), :]
                for comp in range(COMPS)
            ]
            for source in range(LAYERS)
        ]

        def coefficient(op):
            return delta_ref[pl.ds(pl.multiple_of(op * ROWS + base, OWNED), OWNED), :]

        fields = mix(spectra, coefficient, edge=True)
        for target in range(LAYERS):
            for comp in range(COMPS):
                row = base * P1_ROWS + (target * COMPS + comp) * OWNED
                fix_ref[pl.ds(row, OWNED, stride=P1_ROWS), :] = fields[target][comp]
        return carry

    lax.fori_loop(0, ROWS // OWNED, fix_step, 0)

    def mix_line(p1):
        lines = blocks(spec_ref, p1 * P1_ALL, LAYERS * COMPS)
        spectra = [lines[COMPS * s : COMPS * s + COMPS] for s in range(LAYERS)]
        kernel_base = p1 * (OPS * OWNED)

        def coefficient(op):
            return kernel_ref[pl.ds(kernel_base + op * OWNED, OWNED), :]

        fields = mix(spectra, coefficient)
        flat = [fields[j // COMPS][j % COMPS] for j in range(LAYERS * COMPS)]
        row = p1 * P1_ROWS
        fixes = blocks(fix_ref, row, LAYERS * COMPS)
        flat = [a + b for a, b in zip(flat, fixes)]
        for j in range(0, LAYERS * COMPS, 2):
            save_pair(row + OWNED * j, jnp.concatenate(flat[j : j + 2], axis=0))

    def backward_dot(p1, rows):
        both = dot(pair_ref[pl.ds(p1 * P1_ROWS, rows), :], back_table_ref[...])
        back_ref[pl.ds(p1 * P1_ROWS, rows), :] = both[:, :LANES] + both[:, LANES:]

    span = 8
    for p1 in range(span):
        mix_line(p1)

    def mix_step(step, carry):
        p1 = pl.multiple_of(span * step, span)
        backward_dot(p1 - span, span * P1_ROWS)
        for i in range(span):
            mix_line(p1 + i)
        return carry

    lax.fori_loop(1, ROWS // span, mix_step, 0)
    backward_dot(ROWS - span, span * P1_ROWS)

    count = LAYERS * COMPS

    def untwist_edge(p1, slot):
        table = [factors(back_twiddle_ref, p1, kind) for kind in range(2)]
        for j, value in enumerate(blocks(back_ref, p1 * P1_ROWS, count)):
            f = table[kinds[j]]
            sums_ref[pl.ds(slot * P1_ROWS + OWNED * j, OWNED), :] = value * f[0] + pltpu.roll(value, X_ROWS, 1) * f[1]

    untwist_edge(0, 0)
    untwist_edge(half, half)

    def untwist_step(k, carry):
        near = [factors(back_twiddle_ref, k, kind) for kind in range(2)]
        far = [factors(back_twiddle_ref, ROWS - k, kind) for kind in range(2)]
        near_rows = blocks(back_ref, pl.multiple_of(k * P1_ROWS, OWNED), count)
        far_rows = blocks(back_ref, pl.multiple_of((ROWS - k) * P1_ROWS, OWNED), count)
        cos_base = pl.multiple_of(k * P1_ROWS, OWNED)
        sin_base = pl.multiple_of((half + k) * P1_ROWS, OWNED)
        for j in range(count):
            n, f = near[kinds[j]], far[kinds[j]]
            a, b = near_rows[j], far_rows[j]
            a_swap, b_swap = pltpu.roll(a, X_ROWS, 1), pltpu.roll(b, X_ROWS, 1)
            sums_ref[pl.ds(cos_base + OWNED * j, OWNED), :] = (a * n[0] + a_swap * n[1]) + (b * f[0] + b_swap * f[1])
            sums_ref[pl.ds(sin_base + OWNED * j, OWNED), :] = (a * n[2] + a_swap * n[3]) + (b * f[2] + b_swap * f[3])
        return carry

    lax.fori_loop(1, half, untwist_step, 0)

    def back_rows(index, carry):
        place = pl.multiple_of(index * OWNED, OWNED)
        cos_in = [sums_ref[pl.ds(k * P1_ROWS + place, OWNED), :] for k in range(half + 1)]
        sin_in = [None] + [sums_ref[pl.ds((half + k) * P1_ROWS + place, OWNED), :] for k in range(1, half)] + [None]
        values = real_sum(cos_in, sin_in, ROWS)
        layer = index // COMPS
        comp = index % COMPS
        base = pl.multiple_of(layer * (ROWS * SLOT) + comp * OWNED, OWNED)
        for r in range(ROWS):
            out_ref[pl.ds(base + r * SLOT, OWNED), :] = values[r]
        return carry

    lax.fori_loop(0, LAYERS * COMPS, back_rows, 0)


def inverse_y_kernel(x_ref, table_ref, twiddle_ref, out_hbm, high_ref, low_ref, lines_ref, result_ref, sem):
    half = DEVICES // 2
    middle = COARSE // 2
    group = 8
    lane = lax.broadcasted_iota(jnp.int32, (X_ROWS, LANES), 1)
    alternate = 1.0 - 2.0 * (lax.broadcasted_iota(jnp.int32, (group, FINE), 1) % 2).astype(F32)
    copies = []
    columns = []
    for comp in range(COMPS):
        size = (middle + 1) * X_ROWS
        base = comp * size

        def put(k, real, imag):
            rows = slice(base + k * X_ROWS, base + (k + 1) * X_ROWS)
            high_ref[rows, :LANES], low_ref[rows, :LANES] = split_pair(real)
            high_ref[rows, LANES:], low_ref[rows, LANES:] = split_pair(imag)

        for k in range(middle):
            near, far = slot_rows(comp, k)
            if k == 0:
                far = slot_rows(comp, middle)[1]
            block = jnp.concatenate([x_ref[near, :], x_ref[far, :]], axis=0).T
            real, imag = block[:X_ROWS], block[X_ROWS:]
            if k == 0:
                nyquist = imag[:, :1]
                put(middle, jnp.where(lane < half, 0.0, real), jnp.where(lane < half, 0.0, imag))
                scale = jnp.where(lane < half, jnp.where(lane == 0, 0.5, 1.0), 0.0)
                real, imag = real * scale, imag * scale
            put(k, real, imag)
        columns.append(nyquist)
    lines_ref[...] = triple_dot(high_ref[...], low_ref[...], table_ref)
    for comp in range(COMPS):
        base = comp * (middle + 1) * X_ROWS
        nyquist = columns[comp]
        for g in range(X_ROWS // group):
            cos_in = [None] * (middle + 1)
            sin_in = [None] * (middle + 1)
            for k in range(middle + 1):
                rows = slice(base + k * X_ROWS + g * group, base + k * X_ROWS + (g + 1) * group)
                real = lines_ref[rows, :LANES]
                if k == 0:
                    cos_in[0] = 2.0 * real + nyquist[g * group : (g + 1) * group] * alternate
                    continue
                imag = lines_ref[rows, LANES:]
                cosine = twiddle_ref[2 * k - 2 : 2 * k - 1, :]
                sine = twiddle_ref[2 * k - 1 : 2 * k, :]
                cos_in[k] = real * cosine - imag * sine
                if k < middle:
                    sin_in[k] = -(real * sine + imag * cosine)
            values = real_sum(cos_in, sin_in, COARSE)
            top = comp * X_ROWS + g * group
            for a in range(COARSE):
                result_ref[top : top + group, FINE * a : FINE * (a + 1)] = values[a]
        span = pl.ds(comp * X_ROWS, X_ROWS)
        copy = pltpu.make_async_copy(result_ref.at[span], out_hbm.at[span], sem.at[comp])
        copy.start()
        copies.append(copy)
    for copy in copies:
        copy.wait()


VMEM = pl.BlockSpec(memory_space=pltpu.VMEM)
HBM = pl.BlockSpec(memory_space=pltpu.HBM)
FINE_ROWS = COMPS * (COARSE // 2 + 1) * X_ROWS


def params(mebibytes):
    return pltpu.CompilerParams(vmem_limit_bytes=mebibytes * 1024 * 1024)


def edge_lines(kernel):
    return pl.pallas_call(
        edge_kernel,
        in_specs=[HBM],
        out_specs=VMEM,
        out_shape=jax.ShapeDtypeStruct((EDGES, CELLS), F32),
        scratch_shapes=[
            pltpu.VMEM((CELLS // LANES, OFFSETS, EDGE_PARTS, 1, LANES), F32),
            pltpu.SemaphoreType.DMA((CELLS // LANES, 2)),
        ],
        compiler_params=params(58),
        name="edge_lines",
    )(kernel)


def forward_y(field):
    table = stacked(fine_table())
    twiddle = y_twiddle(-1.0, 1.0)
    return pl.pallas_call(
        forward_y_kernel,
        in_specs=[VMEM] * 3,
        out_specs=HBM,
        out_shape=jax.ShapeDtypeStruct((DEVICES, SLOT, LANES), F32),
        scratch_shapes=[
            pltpu.VMEM((FINE_ROWS, 2 * LANES), BF16),
            pltpu.VMEM((FINE_ROWS, 2 * LANES), BF16),
            pltpu.VMEM((DEVICES * SLOT, LANES), F32),
            pltpu.SemaphoreType.DMA((COMPS,)),
        ],
        compiler_params=params(48),
        name="forward_y",
    )(field, jnp.asarray(table), jnp.asarray(twiddle))


def relayout(kernel, flag):
    groups = 3
    rows = OPS // groups * 16
    out_rows = OPS // groups * OWNED
    return pl.pallas_call(
        relayout_kernel,
        grid=(groups,),
        in_specs=[
            pl.BlockSpec(memory_space=pltpu.SMEM),
            pl.BlockSpec((rows, CELLS), lambda g: (g, 0)),
        ],
        out_specs=pl.BlockSpec((ROWS, out_rows, LANES), lambda g: (0, g, 0)),
        out_shape=jax.ShapeDtypeStruct((ROWS, OPS * OWNED, LANES), F32),
        scratch_shapes=[pltpu.VMEM((out_rows, CELLS), F32), pltpu.VMEM((CELLS, LANES), F32)],
        compiler_params=params(48),
        name="relayout",
    )(flag, kernel)


def spectral(lines, kernel, delta):
    twiddle = x_twiddle(-1.0, 1.0)
    back_twiddle = x_twiddle(1.0, -1.0 / (CELLS * CELLS))
    return pl.pallas_call(
        spectral_kernel,
        in_specs=[VMEM, HBM] + [VMEM] * 5,
        out_specs=VMEM,
        out_shape=jax.ShapeDtypeStruct((DEVICES * SLOT, LANES), F32),
        scratch_shapes=[
            pltpu.VMEM((ROWS * OPS * OWNED, LANES), F32),
            pltpu.VMEM((ROWS * EXTRA, LANES), F32),
            pltpu.VMEM((ROWS * P1_ALL, LANES), F32),
            pltpu.VMEM((ROWS * P1_ALL, 2 * LANES), BF16),
            pltpu.VMEM((ROWS * P1_ALL, LANES), F32),
            pltpu.VMEM((ROWS * P1_ROWS, LANES), F32),
            pltpu.VMEM((ROWS * P1_ROWS, LANES), F32),
            pltpu.SemaphoreType.DMA,
        ],
        compiler_params=params(48),
        name="spectral",
    )(
        lines,
        kernel,
        delta,
        jnp.asarray(twiddle),
        jnp.asarray(back_twiddle),
        jnp.asarray(x_table(-1.0)),
        jnp.asarray(x_table(1.0)),
    )


def inverse_y(spectra):
    rows = COMPS * X_ROWS
    return pl.pallas_call(
        inverse_y_kernel,
        in_specs=[VMEM] * 3,
        out_specs=HBM,
        out_shape=jax.ShapeDtypeStruct((rows, CELLS), F32),
        scratch_shapes=[
            pltpu.VMEM((FINE_ROWS, 2 * LANES), BF16),
            pltpu.VMEM((FINE_ROWS, 2 * LANES), BF16),
            pltpu.VMEM((FINE_ROWS, 2 * LANES), F32),
            pltpu.VMEM((rows, CELLS), F32),
            pltpu.SemaphoreType.DMA((COMPS,)),
        ],
        compiler_params=params(20),
        name="inverse_y",
    )(spectra, jnp.asarray(stacked(fine_table().T)), jnp.asarray(y_twiddle(1.0, 2.0)))


def exchange(lines):
    moved = lax.all_to_all(lines.reshape(DEVICES, SLOT, LANES), ("layer", "row"), 0, 0, tiled=True)
    return moved.reshape(DEVICES * SLOT, LANES)


def local(magnet, kernel):
    axes = ("layer", "row")
    device = lax.axis_index(axes)
    field = magnet.reshape(COMPS * X_ROWS, CELLS)
    flag = (device >= DEVICES // 2).astype(jnp.int32).reshape(1)
    edge = edge_lines(kernel)
    middle = lax.ppermute(edge, axes, [(DEVICES // 2, 0)])
    sent = forward_y(field)
    got = exchange(sent)
    coefficient = relayout(kernel.reshape(OPS * 16, CELLS), flag)
    delta = jnp.where(device == 0, middle - edge, 0.0)
    delta = jnp.swapaxes(delta.reshape(EDGES, X_ROWS, ROWS), 1, 2)
    delta = jnp.concatenate([delta, delta], axis=2).reshape(EDGES * ROWS, LANES)
    fields = spectral(got, coefficient.reshape(ROWS * OPS * OWNED, LANES), delta)
    result = inverse_y(exchange(fields))
    return result.reshape(COMPS, 1, X_ROWS, CELLS)


def solution(mesh):
    in_specs = (P(None, "layer", "row", None), P(None, None, ("layer", "row"), None))
    out_specs = P(None, "layer", "row", None)
    return jax.shard_map(local, mesh=mesh, in_specs=in_specs, out_specs=out_specs, check_vma=False)
```

```python
import math

import jax
import jax.numpy as jnp
import numpy as np
from jax import lax
from jax.experimental import pallas as pl
from jax.experimental.pallas import tpu as pltpu
from jax.sharding import PartitionSpec as P


CELLS = 2048
COMPS = 3
LAYERS = 4
ROWS = 32
X_ROWS = 64
DEVICES = 128
PARTS = 6
OFFSETS = 7
OPS = OFFSETS * PARTS
FINE = 128
COARSE = 16
OWNED = 8
SLOT = COMPS * OWNED
LANES = 128
EXTRA = 16
P1_ROWS = LAYERS * COMPS * OWNED
P1_ALL = P1_ROWS + EXTRA

F32 = jnp.float32
BF16 = jnp.bfloat16


def halves(table):
    high = np.asarray(table, np.float32).astype(jnp.bfloat16)
    low = (np.asarray(table, np.float64) - high.astype(np.float64)).astype(np.float32).astype(jnp.bfloat16)
    return high, low


def fine_table():
    index = np.arange(FINE)
    angle = 2.0 * np.pi * (np.outer(index, index) % FINE) / FINE
    return np.block([[np.cos(angle), -np.sin(angle)], [np.sin(angle), np.cos(angle)]])


def stacked(table):
    return np.concatenate(halves(table), axis=0)


def y_twiddle(sign, scale):
    k = np.arange(1, COARSE // 2 + 1)[:, None]
    b = np.arange(FINE)[None, :]
    angle = 2.0 * np.pi * k * b / CELLS
    table = scale * np.stack([np.cos(angle), sign * np.sin(angle)], axis=1)
    return table.reshape(COARSE, FINE).astype(np.float32)


def x_twiddle(sign, scale, inner):
    k = np.arange(ROWS // 2 + 1)[:, None]
    t = np.arange(X_ROWS)[None, :]
    angle = 2.0 * np.pi * k * t / CELLS
    cosine = scale * np.cos(angle)
    sine = scale * sign * np.sin(angle)
    lines = [
        np.concatenate([cosine, cosine], axis=1),
        np.concatenate([sine, sine], axis=1),
        np.concatenate([inner * sine, -inner * sine], axis=1),
        np.concatenate([inner * cosine, -inner * cosine], axis=1),
    ]
    return np.stack(lines, axis=1).astype(np.float32).reshape(-1, LANES)


def x_table(sign, shift):
    index = np.arange(X_ROWS)
    place = np.outer(index, index + shift) if sign < 0 else np.outer(index + shift, index)
    angle = 2.0 * np.pi * (place % X_ROWS) / X_ROWS
    real = np.cos(angle)
    imag = sign * np.sin(angle)
    whole = np.block([[real, imag], [-imag, real]])
    high, low = halves(whole)
    line = np.concatenate([high, low], axis=1)
    return np.concatenate([line, line], axis=0)


def x_tables(sign):
    return np.concatenate([x_table(sign, 0), x_table(sign, 1)], axis=0)


def real_dft(values):
    n = len(values)
    if n == 1:
        return [values[0]], [None]
    if n == 2:
        return [values[0] + values[1], values[0] - values[1]], [None, None]
    even_c, even_s = real_dft(values[0::2])
    odd_c, odd_s = real_dft(values[1::2])
    half = n // 2
    quarter = n // 4
    cos_out = [None] * (half + 1)
    sin_out = [None] * (half + 1)
    for k in range(quarter + 1):
        if k == 0:
            cos_out[0] = even_c[0] + odd_c[0]
            cos_out[half] = even_c[0] - odd_c[0]
        elif k == quarter:
            cos_out[k] = even_c[k]
            sin_out[k] = odd_c[k]
        else:
            theta = 2.0 * math.pi * k / n
            cosine, sine = math.cos(theta), math.sin(theta)
            if 8 * k == n:
                real = cosine * (odd_c[k] - odd_s[k])
                imag = cosine * (odd_s[k] + odd_c[k])
            else:
                real = cosine * odd_c[k] - sine * odd_s[k]
                imag = cosine * odd_s[k] + sine * odd_c[k]
            cos_out[k] = even_c[k] + real
            sin_out[k] = even_s[k] + imag
            cos_out[half - k] = even_c[k] - real
            sin_out[half - k] = imag - even_s[k]
    return cos_out, sin_out


def real_sum(cos_in, sin_in, n):
    if n == 1:
        return [cos_in[0]]
    half = n // 2
    if n == 2:
        return [cos_in[0] + cos_in[1], cos_in[0] - cos_in[1]]
    quarter = n // 4
    even_c = [None] * (quarter + 1)
    even_s = [None] * (quarter + 1)
    odd_c = [None] * (quarter + 1)
    odd_s = [None] * (quarter + 1)
    even_c[0] = cos_in[0] + cos_in[half]
    odd_c[0] = cos_in[0] - cos_in[half]
    even_c[quarter] = cos_in[quarter]
    odd_c[quarter] = sin_in[quarter]
    for k in range(1, quarter):
        theta = 2.0 * math.pi * k / n
        cosine, sine = math.cos(theta), math.sin(theta)
        even_c[k] = cos_in[k] + cos_in[half - k]
        even_s[k] = sin_in[k] - sin_in[half - k]
        gap = cos_in[k] - cos_in[half - k]
        both = sin_in[k] + sin_in[half - k]
        if 8 * k == n:
            odd_c[k] = cosine * (gap + both)
            odd_s[k] = cosine * (both - gap)
        else:
            odd_c[k] = cosine * gap + sine * both
            odd_s[k] = cosine * both - sine * gap
    evens = real_sum(even_c, even_s, half)
    odds = real_sum(odd_c, odd_s, half)
    out = [None] * n
    out[0::2] = evens
    out[1::2] = odds
    return out


def split_pair(value):
    high = value.astype(BF16)
    low = (value - high.astype(F32)).astype(BF16)
    return high, low


def dot(left, right):
    return jnp.dot(left, right, preferred_element_type=F32)


def triple_dot(high, low, table_ref):
    size = table_ref.shape[0] // 2
    table_high, table_low = table_ref[:size, :], table_ref[size:, :]
    left = jnp.concatenate([high, low, high], axis=1)
    return dot(left, jnp.concatenate([table_high, table_high, table_low], axis=0))


def slot_rows(comp, k1):
    half = DEVICES // 2
    near = pl.ds(comp * OWNED + k1, half, stride=SLOT)
    far = pl.ds(half * SLOT + comp * OWNED + k1 - 1, half, stride=SLOT)
    return near, far


EDGE_PARTS = 4
EDGES = OFFSETS * EDGE_PARTS


def edge_kernel(kernel_hbm, out_ref, tiles_ref, sem):
    n_tiles = CELLS // LANES
    copies = []
    for j in range(n_tiles):
        lanes = pl.ds(LANES * j, LANES)
        for i, (source, target) in enumerate([((0, 3), (0, 3)), ((4, 1), (3, 1))]):
            copy = pltpu.make_async_copy(
                kernel_hbm.at[:, pl.ds(*source), pl.ds(0, 1), lanes],
                tiles_ref.at[j, :, pl.ds(*target)],
                sem.at[j, i],
            )
            copy.start()
            copies.append(copy)
    flat = tiles_ref.reshape(n_tiles * EDGES, LANES)
    for j in range(n_tiles):
        copies[2 * j].wait()
        copies[2 * j + 1].wait()
        out_ref[:, LANES * j : LANES * (j + 1)] = flat[pl.ds(j * EDGES, EDGES), :]


def forward_y_kernel(x_ref, table_ref, twiddle_ref, out_hbm, high_ref, low_ref, out_ref, sem):
    slots = out_ref.reshape(DEVICES, SLOT, LANES)
    saves = []
    edges = []
    half = DEVICES // 2
    middle = COARSE // 2
    group = 16
    lane = lax.broadcasted_iota(jnp.int32, (X_ROWS, LANES), 1)
    alternate = 1.0 - 2.0 * (lax.broadcasted_iota(jnp.int32, (X_ROWS, FINE), 1) % 2).astype(F32)
    for comp in range(COMPS):
        base = comp * (middle + 1) * X_ROWS
        nyquist = []
        for g in range(X_ROWS // group):
            top = comp * X_ROWS + g * group
            parts = [x_ref[top : top + group, FINE * a : FINE * (a + 1)] for a in range(COARSE)]
            cos_out, sin_out = real_dft(parts)
            nyquist.append(jnp.sum(cos_out[0] * alternate[:group], axis=1, keepdims=True))
            for k in range(middle + 1):
                rows = slice(base + k * X_ROWS + g * group, base + k * X_ROWS + (g + 1) * group)
                real = cos_out[k]
                imag = None
                if k > 0:
                    cosine = twiddle_ref[2 * k - 2 : 2 * k - 1, :]
                    sine = twiddle_ref[2 * k - 1 : 2 * k, :]
                    if k == middle:
                        real, imag = real * cosine, real * sine
                    else:
                        real, imag = real * cosine + sin_out[k] * sine, real * sine - sin_out[k] * cosine
                high_ref[rows, :LANES], low_ref[rows, :LANES] = split_pair(real)
                if imag is None:
                    zero = jnp.zeros((group, LANES), BF16)
                    high_ref[rows, LANES:], low_ref[rows, LANES:] = zero, zero
                else:
                    high_ref[rows, LANES:], low_ref[rows, LANES:] = split_pair(imag)
        edges.append(jnp.concatenate(nyquist, axis=0))
    out = triple_dot(high_ref[...], low_ref[...], table_ref)
    for comp in range(COMPS):

        def pick(k):
            row = (comp * (middle + 1) + k) * X_ROWS
            rows = out[row : row + X_ROWS]
            return rows[:, :LANES], rows[:, LANES:]

        for k in range(middle):
            real, imag = pick(k)
            if k == 0:
                last_real, last_imag = pick(middle)
                imag = jnp.where(lane == 0, edges[comp], imag)
                real = jnp.where(lane < half, real, last_real)
                imag = jnp.where(lane < half, imag, last_imag)
            if comp == COMPS - 1:
                real, imag = -imag, real
            block = jnp.concatenate([real, imag], axis=0).T
            near, far = slot_rows(comp, k)
            if k == 0:
                far = slot_rows(comp, middle)[1]
            out_ref[near, :] = block[:half]
            out_ref[far, :] = block[half:]
        lines = (slice(None), pl.ds(comp * OWNED, OWNED))
        save = pltpu.make_async_copy(slots.at[lines], out_hbm.at[lines], sem.at[comp])
        save.start()
        saves.append(save)
    for save in saves:
        save.wait()


def relayout_kernel(flag_ref, kernel_ref, out_ref, rows_ref, columns_ref):
    shifted = flag_ref[0] > 0
    n_ops = kernel_ref.shape[0] // 16
    sub = lax.broadcasted_iota(jnp.int32, (OWNED, CELLS), 0)
    for op in range(n_ops):
        low = kernel_ref[16 * op : 16 * op + 8, :]
        high = kernel_ref[16 * op + 8 : 16 * op + 16, :]
        moved = jnp.where(sub < 7, pltpu.roll(low, 7, 0), pltpu.roll(high, 7, 0))
        rows_ref[8 * op : 8 * op + 8, :] = jnp.where(shifted, moved, low)
    for tile in range(CELLS // LANES):
        block = rows_ref[:, LANES * tile : LANES * (tile + 1)].T
        columns_ref[LANES * tile : LANES * (tile + 1), : 8 * n_ops] = block

    def step(p1, carry):
        column = columns_ref[pl.ds(p1, X_ROWS, stride=ROWS), :]
        both = jnp.concatenate([column, column], axis=0).T
        out_ref[p1] = both[: 8 * n_ops]
        return carry

    lax.fori_loop(0, ROWS, step, 0, unroll=4)


def spectral_kernel(
    x_ref,
    kernel_hbm,
    delta_ref,
    twiddle_ref,
    back_twiddle_ref,
    table_ref,
    back_table_ref,
    out_ref,
    kernel_ref,
    extra_ref,
    sums_ref,
    pair_ref,
    spec_ref,
    fix_ref,
    back_ref,
    kernel_sem,
):
    fetch = pltpu.make_async_copy(kernel_hbm, kernel_ref, kernel_sem)
    fetch.start()
    half = ROWS // 2
    lane = lax.broadcasted_iota(jnp.int32, (ROWS, LANES), 1)

    extra_ref[...] = jnp.zeros_like(extra_ref)
    for layer in range(LAYERS):
        for comp in range(COMPS):
            line = x_ref[pl.ds(layer * ROWS * SLOT + comp * OWNED, ROWS, stride=SLOT), :]
            extra_ref[pl.ds(comp * LAYERS + layer, ROWS, stride=EXTRA), :] = jnp.where((lane < X_ROWS) == (comp == COMPS - 1), line, 0.0)
    fix_ref[...] = jnp.zeros_like(fix_ref)

    def store_sums(values, place):
        cos_out, sin_out = real_dft(values)
        for k in range(half + 1):
            sums_ref[pl.ds(k * P1_ALL + place, OWNED), :] = cos_out[k]
        for k in range(1, half):
            sums_ref[pl.ds((half + k) * P1_ALL + place, OWNED), :] = sin_out[k]

    def over_rows(index, carry):
        layer = index // COMPS
        comp = index % COMPS
        base = layer * (ROWS * SLOT) + comp * OWNED
        base = pl.multiple_of(base, OWNED)
        values = [x_ref[pl.ds(base + r * SLOT, OWNED), :] for r in range(ROWS)]
        store_sums(values, pl.multiple_of(index * OWNED, OWNED))
        return carry

    lax.fori_loop(0, LAYERS * COMPS, over_rows, 0)
    for group in range(2):
        values = [extra_ref[r * EXTRA + group * 8 : r * EXTRA + group * 8 + 8, :] for r in range(ROWS)]
        store_sums(values, P1_ROWS + group * 8)

    def factors(ref, k):
        return [ref[pl.ds(4 * k + j, 1), :] for j in range(4)]

    def save_pair(row, value):
        high, low = split_pair(value)
        pair_ref[pl.ds(row, value.shape[0]), :LANES] = high
        pair_ref[pl.ds(row, value.shape[0]), LANES:] = low

    n_blocks = P1_ALL // OWNED

    def blocks(ref, row, count):
        return [ref[pl.ds(row + OWNED * j, OWNED), :] for j in range(count)]

    def save_line(p1, values):
        for j in range(0, n_blocks, 2):
            save_pair(p1 * P1_ALL + OWNED * j, jnp.concatenate(values[j : j + 2], axis=0))

    def twist(k):
        f = factors(twiddle_ref, k)
        cos_rows = blocks(sums_ref, k * P1_ALL, n_blocks)
        if k in (0, half):
            even = [c * f[0] for c in cos_rows]
            odd = [c * f[2] for c in cos_rows]
        else:
            sin_rows = blocks(sums_ref, (half + k) * P1_ALL, n_blocks)
            even = [c * f[0] + v * f[1] for c, v in zip(cos_rows, sin_rows)]
            odd = [c * f[2] - v * f[3] for c, v in zip(cos_rows, sin_rows)]
        if k == 0:
            save_line(0, even)
            return
        odd = [pltpu.roll(v, X_ROWS, 1) for v in odd]
        if k != half:
            save_line(k, [a + b for a, b in zip(even, odd)])
        save_line(ROWS - k, [a - b for a, b in zip(even, odd)])

    size = 2 * LANES

    def forward_dot(first, count, which):
        rows = pl.ds(first * P1_ALL, count * P1_ALL)
        both = dot(pair_ref[rows, :], table_ref[which * size : (which + 1) * size, :])
        spec_ref[rows, :] = both[:, :LANES] + both[:, LANES:]

    for k in range(6):
        twist(k)
    forward_dot(0, 6, 0)
    forward_dot(27, 5, 1)
    for k in range(6, 11):
        twist(k)
    forward_dot(6, 5, 0)
    forward_dot(22, 5, 1)
    for k in range(11, half + 1):
        twist(k)
    forward_dot(11, 5, 0)
    forward_dot(half, 6, 1)
    fetch.wait()

    def mix(spectra, coefficient, edge=False):
        fields = []
        for target in range(LAYERS):
            total = [None, None, None]

            def add(comp, term):
                total[comp] = term if total[comp] is None else total[comp] + term

            for source in range(LAYERS):
                offset = target - source + LAYERS - 1
                mx, my, mz = spectra[source]
                if edge:
                    k = [coefficient(offset * EDGE_PARTS + j) for j in range(EDGE_PARTS)]
                    add(0, k[0] * mx + k[3] * mz)
                    add(1, k[1] * my)
                    add(2, k[3] * mx - k[2] * mz)
                    continue
                k = [coefficient(offset * PARTS + j) for j in range(PARTS)]
                add(0, k[0] * mx + k[3] * my + k[4] * mz)
                add(1, k[3] * mx + k[1] * my + k[5] * mz)
                add(2, k[4] * mx + k[5] * my - k[2] * mz)
            fields.append(total)
        return fields

    def fix_step(group, carry):
        base = group * OWNED
        spectra = [
            [
                spec_ref[pl.ds(base * P1_ALL + P1_ROWS + comp * LAYERS + source, OWNED, stride=P1_ALL), :]
                for comp in range(COMPS)
            ]
            for source in range(LAYERS)
        ]

        def coefficient(op):
            return delta_ref[pl.ds(pl.multiple_of(op * ROWS + base, OWNED), OWNED), :]

        fields = mix(spectra, coefficient, edge=True)
        for target in range(LAYERS):
            for comp in range(COMPS):
                row = base * P1_ROWS + (target * COMPS + comp) * OWNED
                fix_ref[pl.ds(row, OWNED, stride=P1_ROWS), :] = fields[target][comp]
        return carry

    lax.fori_loop(0, ROWS // OWNED, fix_step, 0)

    def mix_line(p1):
        lines = blocks(spec_ref, p1 * P1_ALL, LAYERS * COMPS)
        spectra = [lines[COMPS * s : COMPS * s + COMPS] for s in range(LAYERS)]
        kernel_base = p1 * (OPS * OWNED)

        def coefficient(op):
            return kernel_ref[pl.ds(kernel_base + op * OWNED, OWNED), :]

        fields = mix(spectra, coefficient)
        flat = [fields[j // COMPS][j % COMPS] for j in range(LAYERS * COMPS)]
        row = p1 * P1_ROWS
        fixes = blocks(fix_ref, row, LAYERS * COMPS)
        flat = [a + b for a, b in zip(flat, fixes)]
        for j in range(0, LAYERS * COMPS, 2):
            save_pair(row + OWNED * j, jnp.concatenate(flat[j : j + 2], axis=0))

    def backward_dot(p1, rows):
        which = p1 // half
        base = which * size if isinstance(p1, int) else pl.multiple_of(which * size, size)
        both = dot(pair_ref[pl.ds(p1 * P1_ROWS, rows), :], back_table_ref[pl.ds(base, size), :])
        back_ref[pl.ds(p1 * P1_ROWS, rows), :] = both[:, :LANES] + both[:, LANES:]

    span = 8
    for p1 in range(span):
        mix_line(p1)

    def mix_step(step, carry):
        p1 = pl.multiple_of(span * step, span)
        backward_dot(p1 - span, span * P1_ROWS)
        for i in range(span):
            mix_line(p1 + i)
        return carry

    lax.fori_loop(1, ROWS // span, mix_step, 0)
    backward_dot(ROWS - span, span * P1_ROWS)

    count = LAYERS * COMPS
    f = factors(back_twiddle_ref, 0)
    for j, value in enumerate(blocks(back_ref, 0, count)):
        sums_ref[pl.ds(OWNED * j, OWNED), :] = value * f[0]
    f = factors(back_twiddle_ref, half)
    for j, value in enumerate(blocks(back_ref, half * P1_ROWS, count)):
        swap = pltpu.roll(value, X_ROWS, 1)
        sums_ref[pl.ds(half * P1_ROWS + OWNED * j, OWNED), :] = value * f[0] - swap * f[2]

    def untwist_step(k, carry):
        f = factors(back_twiddle_ref, k)
        near = blocks(back_ref, pl.multiple_of(k * P1_ROWS, OWNED), count)
        far = blocks(back_ref, pl.multiple_of((ROWS - k) * P1_ROWS, OWNED), count)
        cos_base = pl.multiple_of(k * P1_ROWS, OWNED)
        sin_base = pl.multiple_of((half + k) * P1_ROWS, OWNED)
        for j in range(count):
            plus = near[j] + far[j]
            swap = pltpu.roll(near[j] - far[j], X_ROWS, 1)
            sums_ref[pl.ds(cos_base + OWNED * j, OWNED), :] = plus * f[0] + swap * f[2]
            sums_ref[pl.ds(sin_base + OWNED * j, OWNED), :] = swap * f[3] - plus * f[1]
        return carry

    lax.fori_loop(1, half, untwist_step, 0)

    def back_rows(index, carry):
        place = pl.multiple_of(index * OWNED, OWNED)
        cos_in = [sums_ref[pl.ds(k * P1_ROWS + place, OWNED), :] for k in range(half + 1)]
        sin_in = [None] + [sums_ref[pl.ds((half + k) * P1_ROWS + place, OWNED), :] for k in range(1, half)] + [None]
        values = real_sum(cos_in, sin_in, ROWS)
        layer = index // COMPS
        comp = index % COMPS
        base = pl.multiple_of(layer * (ROWS * SLOT) + comp * OWNED, OWNED)
        for r in range(ROWS):
            out_ref[pl.ds(base + r * SLOT, OWNED), :] = values[r]
        return carry

    lax.fori_loop(0, LAYERS * COMPS, back_rows, 0)


def inverse_y_kernel(x_ref, table_ref, twiddle_ref, out_hbm, high_ref, low_ref, lines_ref, result_ref, sem):
    half = DEVICES // 2
    middle = COARSE // 2
    group = 8
    lane = lax.broadcasted_iota(jnp.int32, (X_ROWS, LANES), 1)
    alternate = 1.0 - 2.0 * (lax.broadcasted_iota(jnp.int32, (group, FINE), 1) % 2).astype(F32)
    copies = []
    columns = []
    for comp in range(COMPS):
        size = (middle + 1) * X_ROWS
        base = comp * size

        def put(k, real, imag):
            rows = slice(base + k * X_ROWS, base + (k + 1) * X_ROWS)
            high_ref[rows, :LANES], low_ref[rows, :LANES] = split_pair(real)
            high_ref[rows, LANES:], low_ref[rows, LANES:] = split_pair(imag)

        for k in range(middle):
            near, far = slot_rows(comp, k)
            if k == 0:
                far = slot_rows(comp, middle)[1]
            block = jnp.concatenate([x_ref[near, :], x_ref[far, :]], axis=0).T
            real, imag = block[:X_ROWS], block[X_ROWS:]
            if comp == COMPS - 1:
                real, imag = -imag, real
            if k == 0:
                nyquist = imag[:, :1]
                put(middle, jnp.where(lane < half, 0.0, real), jnp.where(lane < half, 0.0, imag))
                scale = jnp.where(lane < half, jnp.where(lane == 0, 0.5, 1.0), 0.0)
                real, imag = real * scale, imag * scale
            put(k, real, imag)
        columns.append(nyquist)
    lines_ref[...] = triple_dot(high_ref[...], low_ref[...], table_ref)
    for comp in range(COMPS):
        base = comp * (middle + 1) * X_ROWS
        nyquist = columns[comp]
        for g in range(X_ROWS // group):
            cos_in = [None] * (middle + 1)
            sin_in = [None] * (middle + 1)
            for k in range(middle + 1):
                rows = slice(base + k * X_ROWS + g * group, base + k * X_ROWS + (g + 1) * group)
                real = lines_ref[rows, :LANES]
                if k == 0:
                    cos_in[0] = 2.0 * real + nyquist[g * group : (g + 1) * group] * alternate
                    continue
                imag = lines_ref[rows, LANES:]
                cosine = twiddle_ref[2 * k - 2 : 2 * k - 1, :]
                sine = twiddle_ref[2 * k - 1 : 2 * k, :]
                cos_in[k] = real * cosine - imag * sine
                if k < middle:
                    sin_in[k] = -(real * sine + imag * cosine)
            values = real_sum(cos_in, sin_in, COARSE)
            top = comp * X_ROWS + g * group
            for a in range(COARSE):
                result_ref[top : top + group, FINE * a : FINE * (a + 1)] = values[a]
        span = pl.ds(comp * X_ROWS, X_ROWS)
        copy = pltpu.make_async_copy(result_ref.at[span], out_hbm.at[span], sem.at[comp])
        copy.start()
        copies.append(copy)
    for copy in copies:
        copy.wait()


VMEM = pl.BlockSpec(memory_space=pltpu.VMEM)
HBM = pl.BlockSpec(memory_space=pltpu.HBM)
FINE_ROWS = COMPS * (COARSE // 2 + 1) * X_ROWS


def params(mebibytes):
    return pltpu.CompilerParams(vmem_limit_bytes=mebibytes * 1024 * 1024)


def edge_lines(kernel):
    return pl.pallas_call(
        edge_kernel,
        in_specs=[HBM],
        out_specs=VMEM,
        out_shape=jax.ShapeDtypeStruct((EDGES, CELLS), F32),
        scratch_shapes=[
            pltpu.VMEM((CELLS // LANES, OFFSETS, EDGE_PARTS, 1, LANES), F32),
            pltpu.SemaphoreType.DMA((CELLS // LANES, 2)),
        ],
        compiler_params=params(58),
        name="edge_lines",
    )(kernel)


def forward_y(field):
    table = stacked(fine_table())
    twiddle = y_twiddle(-1.0, 1.0)
    return pl.pallas_call(
        forward_y_kernel,
        in_specs=[VMEM] * 3,
        out_specs=HBM,
        out_shape=jax.ShapeDtypeStruct((DEVICES, SLOT, LANES), F32),
        scratch_shapes=[
            pltpu.VMEM((FINE_ROWS, 2 * LANES), BF16),
            pltpu.VMEM((FINE_ROWS, 2 * LANES), BF16),
            pltpu.VMEM((DEVICES * SLOT, LANES), F32),
            pltpu.SemaphoreType.DMA((COMPS,)),
        ],
        compiler_params=params(48),
        name="forward_y",
    )(field, jnp.asarray(table), jnp.asarray(twiddle))


def relayout(kernel, flag):
    groups = 3
    rows = OPS // groups * 16
    out_rows = OPS // groups * OWNED
    return pl.pallas_call(
        relayout_kernel,
        grid=(groups,),
        in_specs=[
            pl.BlockSpec(memory_space=pltpu.SMEM),
            pl.BlockSpec((rows, CELLS), lambda g: (g, 0)),
        ],
        out_specs=pl.BlockSpec((ROWS, out_rows, LANES), lambda g: (0, g, 0)),
        out_shape=jax.ShapeDtypeStruct((ROWS, OPS * OWNED, LANES), F32),
        scratch_shapes=[pltpu.VMEM((out_rows, CELLS), F32), pltpu.VMEM((CELLS, LANES), F32)],
        compiler_params=params(48),
        name="relayout",
    )(flag, kernel)


def spectral(lines, kernel, delta):
    twiddle = x_twiddle(-1.0, 1.0, 1.0)
    back_twiddle = x_twiddle(1.0, -1.0 / (CELLS * CELLS), -1.0)
    return pl.pallas_call(
        spectral_kernel,
        in_specs=[VMEM, HBM] + [VMEM] * 5,
        out_specs=VMEM,
        out_shape=jax.ShapeDtypeStruct((DEVICES * SLOT, LANES), F32),
        scratch_shapes=[
            pltpu.VMEM((ROWS * OPS * OWNED, LANES), F32),
            pltpu.VMEM((ROWS * EXTRA, LANES), F32),
            pltpu.VMEM((ROWS * P1_ALL, LANES), F32),
            pltpu.VMEM((ROWS * P1_ALL, 2 * LANES), BF16),
            pltpu.VMEM((ROWS * P1_ALL, LANES), F32),
            pltpu.VMEM((ROWS * P1_ROWS, LANES), F32),
            pltpu.VMEM((ROWS * P1_ROWS, LANES), F32),
            pltpu.SemaphoreType.DMA,
        ],
        compiler_params=params(48),
        name="spectral",
    )(
        lines,
        kernel,
        delta,
        jnp.asarray(twiddle),
        jnp.asarray(back_twiddle),
        jnp.asarray(x_tables(-1.0)),
        jnp.asarray(x_tables(1.0)),
    )


def inverse_y(spectra):
    rows = COMPS * X_ROWS
    return pl.pallas_call(
        inverse_y_kernel,
        in_specs=[VMEM] * 3,
        out_specs=HBM,
        out_shape=jax.ShapeDtypeStruct((rows, CELLS), F32),
        scratch_shapes=[
            pltpu.VMEM((FINE_ROWS, 2 * LANES), BF16),
            pltpu.VMEM((FINE_ROWS, 2 * LANES), BF16),
            pltpu.VMEM((FINE_ROWS, 2 * LANES), F32),
            pltpu.VMEM((rows, CELLS), F32),
            pltpu.SemaphoreType.DMA((COMPS,)),
        ],
        compiler_params=params(20),
        name="inverse_y",
    )(spectra, jnp.asarray(stacked(fine_table().T)), jnp.asarray(y_twiddle(1.0, 2.0)))


def exchange(lines):
    moved = lax.all_to_all(lines.reshape(DEVICES, SLOT, LANES), ("layer", "row"), 0, 0, tiled=True)
    return moved.reshape(DEVICES * SLOT, LANES)


def local(magnet, kernel):
    axes = ("layer", "row")
    device = lax.axis_index(axes)
    field = magnet.reshape(COMPS * X_ROWS, CELLS)
    flag = (device >= DEVICES // 2).astype(jnp.int32).reshape(1)
    edge = edge_lines(kernel)
    middle = lax.ppermute(edge, axes, [(DEVICES // 2, 0)])
    sent = forward_y(field)
    got = exchange(sent)
    coefficient = relayout(kernel.reshape(OPS * 16, CELLS), flag)
    delta = jnp.where(device == 0, middle - edge, 0.0)
    delta = jnp.swapaxes(delta.reshape(EDGES, X_ROWS, ROWS), 1, 2)
    delta = jnp.concatenate([delta, delta], axis=2).reshape(EDGES * ROWS, LANES)
    fields = spectral(got, coefficient.reshape(ROWS * OPS * OWNED, LANES), delta)
    result = inverse_y(exchange(fields))
    return result.reshape(COMPS, 1, X_ROWS, CELLS)


def solution(mesh):
    in_specs = (P(None, "layer", "row", None), P(None, None, ("layer", "row"), None))
    out_specs = P(None, "layer", "row", None)
    return jax.shard_map(local, mesh=mesh, in_specs=in_specs, out_specs=out_specs, check_vma=False)
```

```python
import math

import jax
import jax.numpy as jnp
import numpy as np
from jax import lax
from jax.experimental import pallas as pl
from jax.experimental.pallas import tpu as pltpu
from jax.sharding import PartitionSpec as P


CELLS = 2048
COMPS = 3
LAYERS = 4
ROWS = 32
X_ROWS = 64
DEVICES = 128
PARTS = 6
OFFSETS = 7
OPS = OFFSETS * PARTS
FINE = 128
COARSE = 16
OWNED = 8
SLOT = COMPS * OWNED
LANES = 128
EXTRA = 16
P1_ROWS = LAYERS * COMPS * OWNED
P1_ALL = P1_ROWS + EXTRA

F32 = jnp.float32
BF16 = jnp.bfloat16


def halves(table):
    high = np.asarray(table, np.float32).astype(jnp.bfloat16)
    low = (np.asarray(table, np.float64) - high.astype(np.float64)).astype(np.float32).astype(jnp.bfloat16)
    return high, low


def fine_table():
    index = np.arange(FINE)
    angle = 2.0 * np.pi * (np.outer(index, index) % FINE) / FINE
    return np.block([[np.cos(angle), -np.sin(angle)], [np.sin(angle), np.cos(angle)]])


def stacked(table):
    return np.concatenate(halves(table), axis=0)


def y_twiddle(sign, scale):
    k = np.arange(1, COARSE // 2 + 1)[:, None]
    b = np.arange(FINE)[None, :]
    angle = 2.0 * np.pi * k * b / CELLS
    table = scale * np.stack([np.cos(angle), sign * np.sin(angle)], axis=1)
    return table.reshape(COARSE, FINE).astype(np.float32)


def x_twiddle(sign, scale, inner):
    k = np.arange(ROWS // 2 + 1)[:, None]
    t = np.arange(X_ROWS)[None, :]
    angle = 2.0 * np.pi * k * t / CELLS
    cosine = scale * np.cos(angle)
    sine = scale * sign * np.sin(angle)
    lines = [
        np.concatenate([cosine, cosine], axis=1),
        np.concatenate([sine, sine], axis=1),
        np.concatenate([inner * sine, -inner * sine], axis=1),
        np.concatenate([inner * cosine, -inner * cosine], axis=1),
    ]
    return np.stack(lines, axis=1).astype(np.float32).reshape(-1, LANES)


def x_table(sign, shift):
    index = np.arange(X_ROWS)
    place = np.outer(index, index + shift) if sign < 0 else np.outer(index + shift, index)
    angle = 2.0 * np.pi * (place % X_ROWS) / X_ROWS
    real = np.cos(angle)
    imag = sign * np.sin(angle)
    whole = np.block([[real, imag], [-imag, real]])
    high, low = halves(whole)
    line = np.concatenate([high, low], axis=1)
    return np.concatenate([line, line], axis=0)


def x_tables(sign):
    return np.concatenate([x_table(sign, 0), x_table(sign, 1)], axis=0)


def real_dft(values):
    n = len(values)
    if n == 1:
        return [values[0]], [None]
    if n == 2:
        return [values[0] + values[1], values[0] - values[1]], [None, None]
    even_c, even_s = real_dft(values[0::2])
    odd_c, odd_s = real_dft(values[1::2])
    half = n // 2
    quarter = n // 4
    cos_out = [None] * (half + 1)
    sin_out = [None] * (half + 1)
    for k in range(quarter + 1):
        if k == 0:
            cos_out[0] = even_c[0] + odd_c[0]
            cos_out[half] = even_c[0] - odd_c[0]
        elif k == quarter:
            cos_out[k] = even_c[k]
            sin_out[k] = odd_c[k]
        else:
            theta = 2.0 * math.pi * k / n
            cosine, sine = math.cos(theta), math.sin(theta)
            if 8 * k == n:
                real = cosine * (odd_c[k] - odd_s[k])
                imag = cosine * (odd_s[k] + odd_c[k])
            else:
                real = cosine * odd_c[k] - sine * odd_s[k]
                imag = cosine * odd_s[k] + sine * odd_c[k]
            cos_out[k] = even_c[k] + real
            sin_out[k] = even_s[k] + imag
            cos_out[half - k] = even_c[k] - real
            sin_out[half - k] = imag - even_s[k]
    return cos_out, sin_out


def real_sum(cos_in, sin_in, n):
    if n == 1:
        return [cos_in[0]]
    half = n // 2
    if n == 2:
        return [cos_in[0] + cos_in[1], cos_in[0] - cos_in[1]]
    quarter = n // 4
    even_c = [None] * (quarter + 1)
    even_s = [None] * (quarter + 1)
    odd_c = [None] * (quarter + 1)
    odd_s = [None] * (quarter + 1)
    even_c[0] = cos_in[0] + cos_in[half]
    odd_c[0] = cos_in[0] - cos_in[half]
    even_c[quarter] = cos_in[quarter]
    odd_c[quarter] = sin_in[quarter]
    for k in range(1, quarter):
        theta = 2.0 * math.pi * k / n
        cosine, sine = math.cos(theta), math.sin(theta)
        even_c[k] = cos_in[k] + cos_in[half - k]
        even_s[k] = sin_in[k] - sin_in[half - k]
        gap = cos_in[k] - cos_in[half - k]
        both = sin_in[k] + sin_in[half - k]
        if 8 * k == n:
            odd_c[k] = cosine * (gap + both)
            odd_s[k] = cosine * (both - gap)
        else:
            odd_c[k] = cosine * gap + sine * both
            odd_s[k] = cosine * both - sine * gap
    evens = real_sum(even_c, even_s, half)
    odds = real_sum(odd_c, odd_s, half)
    out = [None] * n
    out[0::2] = evens
    out[1::2] = odds
    return out


def split_pair(value):
    high = value.astype(BF16)
    low = (value - high.astype(F32)).astype(BF16)
    return high, low


def dot(left, right):
    return jnp.dot(left, right, preferred_element_type=F32)


def triple_dot(high, low, table_ref):
    size = table_ref.shape[0] // 2
    table_high, table_low = table_ref[:size, :], table_ref[size:, :]
    left = jnp.concatenate([high, low, high], axis=1)
    return dot(left, jnp.concatenate([table_high, table_high, table_low], axis=0))


def slot_rows(comp, k1):
    half = DEVICES // 2
    near = pl.ds(comp * OWNED + k1, half, stride=SLOT)
    far = pl.ds(half * SLOT + comp * OWNED + k1 - 1, half, stride=SLOT)
    return near, far


EDGE_PARTS = 4
EDGES = OFFSETS * EDGE_PARTS


def edge_kernel(kernel_hbm, out_ref, tiles_ref, sem):
    n_tiles = CELLS // LANES
    copies = []
    for j in range(n_tiles):
        lanes = pl.ds(LANES * j, LANES)
        for i, (source, target) in enumerate([((0, 3), (0, 3)), ((4, 1), (3, 1))]):
            copy = pltpu.make_async_copy(
                kernel_hbm.at[:, pl.ds(*source), pl.ds(0, 1), lanes],
                tiles_ref.at[j, :, pl.ds(*target)],
                sem.at[j, i],
            )
            copy.start()
            copies.append(copy)
    flat = tiles_ref.reshape(n_tiles * EDGES, LANES)
    for j in range(n_tiles):
        copies[2 * j].wait()
        copies[2 * j + 1].wait()
        out_ref[:, LANES * j : LANES * (j + 1)] = flat[pl.ds(j * EDGES, EDGES), :]


def forward_y_kernel(x_ref, table_ref, twiddle_ref, out_hbm, high_ref, low_ref, out_ref, sem):
    slots = out_ref.reshape(DEVICES, SLOT, LANES)
    saves = []
    edges = []
    half = DEVICES // 2
    middle = COARSE // 2
    group = 16
    lane = lax.broadcasted_iota(jnp.int32, (X_ROWS, LANES), 1)
    alternate = 1.0 - 2.0 * (lax.broadcasted_iota(jnp.int32, (X_ROWS, FINE), 1) % 2).astype(F32)
    for comp in range(COMPS):
        base = comp * (middle + 1) * X_ROWS
        nyquist = []
        for g in range(X_ROWS // group):
            top = comp * X_ROWS + g * group
            parts = [x_ref[top : top + group, FINE * a : FINE * (a + 1)] for a in range(COARSE)]
            cos_out, sin_out = real_dft(parts)
            nyquist.append(jnp.sum(cos_out[0] * alternate[:group], axis=1, keepdims=True))
            for k in range(middle + 1):
                rows = slice(base + k * X_ROWS + g * group, base + k * X_ROWS + (g + 1) * group)
                real = cos_out[k]
                imag = None
                if k > 0:
                    cosine = twiddle_ref[2 * k - 2 : 2 * k - 1, :]
                    sine = twiddle_ref[2 * k - 1 : 2 * k, :]
                    if k == middle:
                        real, imag = real * cosine, real * sine
                    else:
                        real, imag = real * cosine + sin_out[k] * sine, real * sine - sin_out[k] * cosine
                high_ref[rows, :LANES], low_ref[rows, :LANES] = split_pair(real)
                if imag is None:
                    zero = jnp.zeros((group, LANES), BF16)
                    high_ref[rows, LANES:], low_ref[rows, LANES:] = zero, zero
                else:
                    high_ref[rows, LANES:], low_ref[rows, LANES:] = split_pair(imag)
        edges.append(jnp.concatenate(nyquist, axis=0))
    out = triple_dot(high_ref[...], low_ref[...], table_ref)
    for comp in range(COMPS):

        def pick(k):
            row = (comp * (middle + 1) + k) * X_ROWS
            rows = out[row : row + X_ROWS]
            return rows[:, :LANES], rows[:, LANES:]

        for k in range(middle):
            real, imag = pick(k)
            if k == 0:
                last_real, last_imag = pick(middle)
                imag = jnp.where(lane == 0, edges[comp], imag)
                real = jnp.where(lane < half, real, last_real)
                imag = jnp.where(lane < half, imag, last_imag)
            if comp == COMPS - 1:
                real, imag = -imag, real
            block = jnp.concatenate([real, imag], axis=0).T
            near, far = slot_rows(comp, k)
            if k == 0:
                far = slot_rows(comp, middle)[1]
            out_ref[near, :] = block[:half]
            out_ref[far, :] = block[half:]
        lines = (slice(None), pl.ds(comp * OWNED, OWNED))
        save = pltpu.make_async_copy(slots.at[lines], out_hbm.at[lines], sem.at[comp])
        save.start()
        saves.append(save)
    for save in saves:
        save.wait()


def relayout_kernel(flag_ref, kernel_ref, out_ref, rows_ref, columns_ref):
    shifted = flag_ref[0] > 0
    n_ops = kernel_ref.shape[0] // 16
    sub = lax.broadcasted_iota(jnp.int32, (OWNED, CELLS), 0)
    for op in range(n_ops):
        low = kernel_ref[16 * op : 16 * op + 8, :]
        high = kernel_ref[16 * op + 8 : 16 * op + 16, :]
        moved = jnp.where(sub < 7, pltpu.roll(low, 7, 0), pltpu.roll(high, 7, 0))
        rows_ref[8 * op : 8 * op + 8, :] = jnp.where(shifted, moved, low)
    for tile in range(CELLS // LANES):
        block = rows_ref[:, LANES * tile : LANES * (tile + 1)].T
        columns_ref[LANES * tile : LANES * (tile + 1), : 8 * n_ops] = block

    def step(p1, carry):
        column = columns_ref[pl.ds(p1, X_ROWS, stride=ROWS), :]
        both = jnp.concatenate([column, column], axis=0).T
        out_ref[p1] = both[: 8 * n_ops]
        return carry

    lax.fori_loop(0, ROWS, step, 0, unroll=4)


def spectral_kernel(
    x_ref,
    kernel_hbm,
    delta_ref,
    twiddle_ref,
    back_twiddle_ref,
    table_ref,
    back_table_ref,
    out_ref,
    kernel_ref,
    extra_ref,
    sums_ref,
    pair_ref,
    spec_ref,
    fix_ref,
    back_ref,
    kernel_sem,
):
    fetch = pltpu.make_async_copy(kernel_hbm, kernel_ref, kernel_sem)
    fetch.start()
    half = ROWS // 2
    lane = lax.broadcasted_iota(jnp.int32, (ROWS, LANES), 1)

    extra_ref[...] = jnp.zeros_like(extra_ref)
    for layer in range(LAYERS):
        for comp in range(COMPS):
            line = x_ref[pl.ds(layer * ROWS * SLOT + comp * OWNED, ROWS, stride=SLOT), :]
            extra_ref[pl.ds(comp * LAYERS + layer, ROWS, stride=EXTRA), :] = jnp.where((lane < X_ROWS) == (comp == COMPS - 1), line, 0.0)
    fix_ref[...] = jnp.zeros_like(fix_ref)

    def store_sums(values, place):
        cos_out, sin_out = real_dft(values)
        for k in range(half + 1):
            sums_ref[pl.ds(k * P1_ALL + place, OWNED), :] = cos_out[k]
        for k in range(1, half):
            sums_ref[pl.ds((half + k) * P1_ALL + place, OWNED), :] = sin_out[k]

    def over_rows(index, carry):
        layer = index // COMPS
        comp = index % COMPS
        base = layer * (ROWS * SLOT) + comp * OWNED
        base = pl.multiple_of(base, OWNED)
        values = [x_ref[pl.ds(base + r * SLOT, OWNED), :] for r in range(ROWS)]
        store_sums(values, pl.multiple_of(index * OWNED, OWNED))
        return carry

    lax.fori_loop(0, LAYERS * COMPS, over_rows, 0)
    for group in range(2):
        values = [extra_ref[r * EXTRA + group * 8 : r * EXTRA + group * 8 + 8, :] for r in range(ROWS)]
        store_sums(values, P1_ROWS + group * 8)

    def factors(ref, k):
        return [ref[pl.ds(4 * k + j, 1), :] for j in range(4)]

    def save_pair(row, value):
        high, low = split_pair(value)
        pair_ref[pl.ds(row, value.shape[0]), :LANES] = high
        pair_ref[pl.ds(row, value.shape[0]), LANES:] = low

    n_blocks = P1_ALL // OWNED

    def blocks(ref, row, count):
        return [ref[pl.ds(row + OWNED * j, OWNED), :] for j in range(count)]

    def save_line(p1, values):
        for j in range(0, n_blocks, 2):
            save_pair(p1 * P1_ALL + OWNED * j, jnp.concatenate(values[j : j + 2], axis=0))

    def twist(k):
        f = factors(twiddle_ref, k)
        cos_rows = blocks(sums_ref, k * P1_ALL, n_blocks)
        if k in (0, half):
            even = [c * f[0] for c in cos_rows]
            odd = [c * f[2] for c in cos_rows]
        else:
            sin_rows = blocks(sums_ref, (half + k) * P1_ALL, n_blocks)
            even = [c * f[0] + v * f[1] for c, v in zip(cos_rows, sin_rows)]
            odd = [c * f[2] - v * f[3] for c, v in zip(cos_rows, sin_rows)]
        if k == 0:
            save_line(0, even)
            return
        odd = [pltpu.roll(v, X_ROWS, 1) for v in odd]
        if k != half:
            save_line(k, [a + b for a, b in zip(even, odd)])
        save_line(ROWS - k, [a - b for a, b in zip(even, odd)])

    size = 2 * LANES

    def forward_dot(first, count, which):
        rows = pl.ds(first * P1_ALL, count * P1_ALL)
        both = dot(pair_ref[rows, :], table_ref[which * size : (which + 1) * size, :])
        spec_ref[rows, :] = both[:, :LANES] + both[:, LANES:]

    for k in range(6):
        twist(k)
    forward_dot(0, 6, 0)
    forward_dot(27, 5, 1)
    for k in range(6, 11):
        twist(k)
    forward_dot(6, 5, 0)
    forward_dot(22, 5, 1)
    for k in range(11, half + 1):
        twist(k)
    forward_dot(11, 5, 0)
    forward_dot(half, 6, 1)
    fetch.wait()

    def mix(spectra, coefficient, edge=False):
        fields = []
        for target in range(LAYERS):
            total = [None, None, None]

            def add(comp, term):
                total[comp] = term if total[comp] is None else total[comp] + term

            for source in range(LAYERS):
                offset = target - source + LAYERS - 1
                mx, my, mz = spectra[source]
                if edge:
                    k = [coefficient(offset * EDGE_PARTS + j) for j in range(EDGE_PARTS)]
                    add(0, k[0] * mx + k[3] * mz)
                    add(1, k[1] * my)
                    add(2, k[3] * mx - k[2] * mz)
                    continue
                k = [coefficient(offset * PARTS + j) for j in range(PARTS)]
                add(0, k[0] * mx + k[3] * my + k[4] * mz)
                add(1, k[3] * mx + k[1] * my + k[5] * mz)
                add(2, k[4] * mx + k[5] * my - k[2] * mz)
            fields.append(total)
        return fields

    def fix_step(group, carry):
        base = group * OWNED
        spectra = [
            [
                spec_ref[pl.ds(base * P1_ALL + P1_ROWS + comp * LAYERS + source, OWNED, stride=P1_ALL), :]
                for comp in range(COMPS)
            ]
            for source in range(LAYERS)
        ]

        def coefficient(op):
            return delta_ref[pl.ds(pl.multiple_of(op * ROWS + base, OWNED), OWNED), :]

        fields = mix(spectra, coefficient, edge=True)
        for target in range(LAYERS):
            for comp in range(COMPS):
                row = base * P1_ROWS + (target * COMPS + comp) * OWNED
                fix_ref[pl.ds(row, OWNED, stride=P1_ROWS), :] = fields[target][comp]
        return carry

    lax.fori_loop(0, ROWS // OWNED, fix_step, 0)

    def mix_line(p1):
        lines = blocks(spec_ref, p1 * P1_ALL, LAYERS * COMPS)
        spectra = [lines[COMPS * s : COMPS * s + COMPS] for s in range(LAYERS)]
        kernel_base = p1 * (OPS * OWNED)

        def coefficient(op):
            return kernel_ref[pl.ds(kernel_base + op * OWNED, OWNED), :]

        fields = mix(spectra, coefficient)
        flat = [fields[j // COMPS][j % COMPS] for j in range(LAYERS * COMPS)]
        row = p1 * P1_ROWS
        fixes = blocks(fix_ref, row, LAYERS * COMPS)
        flat = [a + b for a, b in zip(flat, fixes)]
        for j in range(0, LAYERS * COMPS, 2):
            save_pair(row + OWNED * j, jnp.concatenate(flat[j : j + 2], axis=0))

    def backward_dot(p1, rows):
        which = p1 // half
        base = which * size if isinstance(p1, int) else pl.multiple_of(which * size, size)
        both = dot(pair_ref[pl.ds(p1 * P1_ROWS, rows), :], back_table_ref[pl.ds(base, size), :])
        back_ref[pl.ds(p1 * P1_ROWS, rows), :] = both[:, :LANES] + both[:, LANES:]

    span = 8
    for p1 in range(span):
        mix_line(p1)

    def mix_step(step, carry):
        p1 = pl.multiple_of(span * step, span)
        backward_dot(p1 - span, span * P1_ROWS)
        for i in range(span):
            mix_line(p1 + i)
        return carry

    lax.fori_loop(1, ROWS // span, mix_step, 0)
    backward_dot(ROWS - span, span * P1_ROWS)

    count = LAYERS * COMPS
    f = factors(back_twiddle_ref, 0)
    for j, value in enumerate(blocks(back_ref, 0, count)):
        sums_ref[pl.ds(OWNED * j, OWNED), :] = value * f[0]
    f = factors(back_twiddle_ref, half)
    for j, value in enumerate(blocks(back_ref, half * P1_ROWS, count)):
        swap = pltpu.roll(value, X_ROWS, 1)
        sums_ref[pl.ds(half * P1_ROWS + OWNED * j, OWNED), :] = value * f[0] - swap * f[2]

    def untwist(k):
        f = factors(back_twiddle_ref, k)
        near = blocks(back_ref, k * P1_ROWS, count)
        far = blocks(back_ref, (ROWS - k) * P1_ROWS, count)
        swaps = [pltpu.roll(a - b, X_ROWS, 1) for a, b in zip(near, far)]
        for j in range(count):
            plus = near[j] + far[j]
            sums_ref[pl.ds(k * P1_ROWS + OWNED * j, OWNED), :] = plus * f[0] + swaps[j] * f[2]
            sums_ref[pl.ds((half + k) * P1_ROWS + OWNED * j, OWNED), :] = swaps[j] * f[3] - plus * f[1]

    for k in range(1, half):
        untwist(k)

    def back_rows(index, carry):
        place = pl.multiple_of(index * OWNED, OWNED)
        cos_in = [sums_ref[pl.ds(k * P1_ROWS + place, OWNED), :] for k in range(half + 1)]
        sin_in = [None] + [sums_ref[pl.ds((half + k) * P1_ROWS + place, OWNED), :] for k in range(1, half)] + [None]
        values = real_sum(cos_in, sin_in, ROWS)
        layer = index // COMPS
        comp = index % COMPS
        base = pl.multiple_of(layer * (ROWS * SLOT) + comp * OWNED, OWNED)
        for r in range(ROWS):
            out_ref[pl.ds(base + r * SLOT, OWNED), :] = values[r]
        return carry

    lax.fori_loop(0, LAYERS * COMPS, back_rows, 0)


def inverse_y_kernel(x_ref, table_ref, twiddle_ref, out_hbm, high_ref, low_ref, lines_ref, result_ref, sem):
    half = DEVICES // 2
    middle = COARSE // 2
    group = 8
    lane = lax.broadcasted_iota(jnp.int32, (X_ROWS, LANES), 1)
    alternate = 1.0 - 2.0 * (lax.broadcasted_iota(jnp.int32, (group, FINE), 1) % 2).astype(F32)
    copies = []
    columns = []
    for comp in range(COMPS):
        size = (middle + 1) * X_ROWS
        base = comp * size

        def put(k, real, imag):
            rows = slice(base + k * X_ROWS, base + (k + 1) * X_ROWS)
            high_ref[rows, :LANES], low_ref[rows, :LANES] = split_pair(real)
            high_ref[rows, LANES:], low_ref[rows, LANES:] = split_pair(imag)

        for k in range(middle):
            near, far = slot_rows(comp, k)
            if k == 0:
                far = slot_rows(comp, middle)[1]
            block = jnp.concatenate([x_ref[near, :], x_ref[far, :]], axis=0).T
            real, imag = block[:X_ROWS], block[X_ROWS:]
            if comp == COMPS - 1:
                real, imag = -imag, real
            if k == 0:
                nyquist = imag[:, :1]
                put(middle, jnp.where(lane < half, 0.0, real), jnp.where(lane < half, 0.0, imag))
                scale = jnp.where(lane < half, jnp.where(lane == 0, 0.5, 1.0), 0.0)
                real, imag = real * scale, imag * scale
            put(k, real, imag)
        columns.append(nyquist)
    lines_ref[...] = triple_dot(high_ref[...], low_ref[...], table_ref)
    for comp in range(COMPS):
        base = comp * (middle + 1) * X_ROWS
        nyquist = columns[comp]
        for g in range(X_ROWS // group):
            cos_in = [None] * (middle + 1)
            sin_in = [None] * (middle + 1)
            for k in range(middle + 1):
                rows = slice(base + k * X_ROWS + g * group, base + k * X_ROWS + (g + 1) * group)
                real = lines_ref[rows, :LANES]
                if k == 0:
                    cos_in[0] = 2.0 * real + nyquist[g * group : (g + 1) * group] * alternate
                    continue
                imag = lines_ref[rows, LANES:]
                cosine = twiddle_ref[2 * k - 2 : 2 * k - 1, :]
                sine = twiddle_ref[2 * k - 1 : 2 * k, :]
                cos_in[k] = real * cosine - imag * sine
                if k < middle:
                    sin_in[k] = -(real * sine + imag * cosine)
            values = real_sum(cos_in, sin_in, COARSE)
            top = comp * X_ROWS + g * group
            for a in range(COARSE):
                result_ref[top : top + group, FINE * a : FINE * (a + 1)] = values[a]
        span = pl.ds(comp * X_ROWS, X_ROWS)
        copy = pltpu.make_async_copy(result_ref.at[span], out_hbm.at[span], sem.at[comp])
        copy.start()
        copies.append(copy)
    for copy in copies:
        copy.wait()


VMEM = pl.BlockSpec(memory_space=pltpu.VMEM)
HBM = pl.BlockSpec(memory_space=pltpu.HBM)
FINE_ROWS = COMPS * (COARSE // 2 + 1) * X_ROWS


def params(mebibytes):
    return pltpu.CompilerParams(vmem_limit_bytes=mebibytes * 1024 * 1024)


def edge_lines(kernel):
    return pl.pallas_call(
        edge_kernel,
        in_specs=[HBM],
        out_specs=VMEM,
        out_shape=jax.ShapeDtypeStruct((EDGES, CELLS), F32),
        scratch_shapes=[
            pltpu.VMEM((CELLS // LANES, OFFSETS, EDGE_PARTS, 1, LANES), F32),
            pltpu.SemaphoreType.DMA((CELLS // LANES, 2)),
        ],
        compiler_params=params(58),
        name="edge_lines",
    )(kernel)


def forward_y(field):
    table = stacked(fine_table())
    twiddle = y_twiddle(-1.0, 1.0)
    return pl.pallas_call(
        forward_y_kernel,
        in_specs=[VMEM] * 3,
        out_specs=HBM,
        out_shape=jax.ShapeDtypeStruct((DEVICES, SLOT, LANES), F32),
        scratch_shapes=[
            pltpu.VMEM((FINE_ROWS, 2 * LANES), BF16),
            pltpu.VMEM((FINE_ROWS, 2 * LANES), BF16),
            pltpu.VMEM((DEVICES * SLOT, LANES), F32),
            pltpu.SemaphoreType.DMA((COMPS,)),
        ],
        compiler_params=params(48),
        name="forward_y",
    )(field, jnp.asarray(table), jnp.asarray(twiddle))


def relayout(kernel, flag):
    groups = 3
    rows = OPS // groups * 16
    out_rows = OPS // groups * OWNED
    return pl.pallas_call(
        relayout_kernel,
        grid=(groups,),
        in_specs=[
            pl.BlockSpec(memory_space=pltpu.SMEM),
            pl.BlockSpec((rows, CELLS), lambda g: (g, 0)),
        ],
        out_specs=pl.BlockSpec((ROWS, out_rows, LANES), lambda g: (0, g, 0)),
        out_shape=jax.ShapeDtypeStruct((ROWS, OPS * OWNED, LANES), F32),
        scratch_shapes=[pltpu.VMEM((out_rows, CELLS), F32), pltpu.VMEM((CELLS, LANES), F32)],
        compiler_params=params(48),
        name="relayout",
    )(flag, kernel)


def spectral(lines, kernel, delta):
    twiddle = x_twiddle(-1.0, 1.0, 1.0)
    back_twiddle = x_twiddle(1.0, -1.0 / (CELLS * CELLS), -1.0)
    return pl.pallas_call(
        spectral_kernel,
        in_specs=[VMEM, HBM] + [VMEM] * 5,
        out_specs=VMEM,
        out_shape=jax.ShapeDtypeStruct((DEVICES * SLOT, LANES), F32),
        scratch_shapes=[
            pltpu.VMEM((ROWS * OPS * OWNED, LANES), F32),
            pltpu.VMEM((ROWS * EXTRA, LANES), F32),
            pltpu.VMEM((ROWS * P1_ALL, LANES), F32),
            pltpu.VMEM((ROWS * P1_ALL, 2 * LANES), BF16),
            pltpu.VMEM((ROWS * P1_ALL, LANES), F32),
            pltpu.VMEM((ROWS * P1_ROWS, LANES), F32),
            pltpu.VMEM((ROWS * P1_ROWS, LANES), F32),
            pltpu.SemaphoreType.DMA,
        ],
        compiler_params=params(48),
        name="spectral",
    )(
        lines,
        kernel,
        delta,
        jnp.asarray(twiddle),
        jnp.asarray(back_twiddle),
        jnp.asarray(x_tables(-1.0)),
        jnp.asarray(x_tables(1.0)),
    )


def inverse_y(spectra):
    rows = COMPS * X_ROWS
    return pl.pallas_call(
        inverse_y_kernel,
        in_specs=[VMEM] * 3,
        out_specs=HBM,
        out_shape=jax.ShapeDtypeStruct((rows, CELLS), F32),
        scratch_shapes=[
            pltpu.VMEM((FINE_ROWS, 2 * LANES), BF16),
            pltpu.VMEM((FINE_ROWS, 2 * LANES), BF16),
            pltpu.VMEM((FINE_ROWS, 2 * LANES), F32),
            pltpu.VMEM((rows, CELLS), F32),
            pltpu.SemaphoreType.DMA((COMPS,)),
        ],
        compiler_params=params(20),
        name="inverse_y",
    )(spectra, jnp.asarray(stacked(fine_table().T)), jnp.asarray(y_twiddle(1.0, 2.0)))


def exchange(lines):
    moved = lax.all_to_all(lines.reshape(DEVICES, SLOT, LANES), ("layer", "row"), 0, 0, tiled=True)
    return moved.reshape(DEVICES * SLOT, LANES)


def local(magnet, kernel):
    axes = ("layer", "row")
    device = lax.axis_index(axes)
    field = magnet.reshape(COMPS * X_ROWS, CELLS)
    flag = (device >= DEVICES // 2).astype(jnp.int32).reshape(1)
    edge = edge_lines(kernel)
    middle = lax.ppermute(edge, axes, [(DEVICES // 2, 0)])
    sent = forward_y(field)
    got = exchange(sent)
    coefficient = relayout(kernel.reshape(OPS * 16, CELLS), flag)
    delta = jnp.where(device == 0, middle - edge, 0.0)
    delta = jnp.swapaxes(delta.reshape(EDGES, X_ROWS, ROWS), 1, 2)
    delta = jnp.concatenate([delta, delta], axis=2).reshape(EDGES * ROWS, LANES)
    fields = spectral(got, coefficient.reshape(ROWS * OPS * OWNED, LANES), delta)
    result = inverse_y(exchange(fields))
    return result.reshape(COMPS, 1, X_ROWS, CELLS)


def solution(mesh):
    in_specs = (P(None, "layer", "row", None), P(None, None, ("layer", "row"), None))
    out_specs = P(None, "layer", "row", None)
    return jax.shard_map(local, mesh=mesh, in_specs=in_specs, out_specs=out_specs, check_vma=False)
```

```python
import math

import jax
import jax.numpy as jnp
import numpy as np
from jax import lax
from jax.experimental import pallas as pl
from jax.experimental.pallas import tpu as pltpu
from jax.sharding import PartitionSpec as P


CELLS = 2048
COMPS = 3
LAYERS = 4
ROWS = 32
X_ROWS = 64
DEVICES = 128
PARTS = 6
OFFSETS = 7
OPS = OFFSETS * PARTS
FINE = 128
COARSE = 16
OWNED = 8
SLOT = COMPS * OWNED
LANES = 128
EXTRA = 16
P1_ROWS = LAYERS * COMPS * OWNED
P1_ALL = P1_ROWS + EXTRA

F32 = jnp.float32
BF16 = jnp.bfloat16


def halves(table):
    high = np.asarray(table, np.float32).astype(jnp.bfloat16)
    low = (np.asarray(table, np.float64) - high.astype(np.float64)).astype(np.float32).astype(jnp.bfloat16)
    return high, low


def fine_table():
    index = np.arange(FINE)
    angle = 2.0 * np.pi * (np.outer(index, index) % FINE) / FINE
    return np.block([[np.cos(angle), -np.sin(angle)], [np.sin(angle), np.cos(angle)]])


def stacked(table):
    return np.concatenate(halves(table), axis=0)


def y_twiddle(sign, scale):
    k = np.arange(1, COARSE // 2 + 1)[:, None]
    b = np.arange(FINE)[None, :]
    angle = 2.0 * np.pi * k * b / CELLS
    table = scale * np.stack([np.cos(angle), sign * np.sin(angle)], axis=1)
    return table.reshape(COARSE, FINE).astype(np.float32)


def x_twiddle(sign, scale, inner):
    k = np.arange(ROWS // 2 + 1)[:, None]
    t = np.arange(X_ROWS)[None, :]
    angle = 2.0 * np.pi * k * t / CELLS
    cosine = scale * np.cos(angle)
    sine = scale * sign * np.sin(angle)
    lines = [
        np.concatenate([cosine, cosine], axis=1),
        np.concatenate([sine, sine], axis=1),
        np.concatenate([inner * sine, -inner * sine], axis=1),
        np.concatenate([inner * cosine, -inner * cosine], axis=1),
    ]
    return np.stack(lines, axis=1).astype(np.float32).reshape(-1, LANES)


def x_table(sign, shift):
    index = np.arange(X_ROWS)
    place = np.outer(index, index + shift) if sign < 0 else np.outer(index + shift, index)
    angle = 2.0 * np.pi * (place % X_ROWS) / X_ROWS
    real = np.cos(angle)
    imag = sign * np.sin(angle)
    whole = np.block([[real, imag], [-imag, real]])
    high, low = halves(whole)
    line = np.concatenate([high, low], axis=1)
    return np.concatenate([line, line], axis=0)


def x_tables(sign):
    return np.concatenate([x_table(sign, 0), x_table(sign, 1)], axis=0)


def real_dft(values):
    n = len(values)
    if n == 1:
        return [values[0]], [None]
    if n == 2:
        return [values[0] + values[1], values[0] - values[1]], [None, None]
    even_c, even_s = real_dft(values[0::2])
    odd_c, odd_s = real_dft(values[1::2])
    half = n // 2
    quarter = n // 4
    cos_out = [None] * (half + 1)
    sin_out = [None] * (half + 1)
    for k in range(quarter + 1):
        if k == 0:
            cos_out[0] = even_c[0] + odd_c[0]
            cos_out[half] = even_c[0] - odd_c[0]
        elif k == quarter:
            cos_out[k] = even_c[k]
            sin_out[k] = odd_c[k]
        else:
            theta = 2.0 * math.pi * k / n
            cosine, sine = math.cos(theta), math.sin(theta)
            if 8 * k == n:
                real = cosine * (odd_c[k] - odd_s[k])
                imag = cosine * (odd_s[k] + odd_c[k])
            else:
                real = cosine * odd_c[k] - sine * odd_s[k]
                imag = cosine * odd_s[k] + sine * odd_c[k]
            cos_out[k] = even_c[k] + real
            sin_out[k] = even_s[k] + imag
            cos_out[half - k] = even_c[k] - real
            sin_out[half - k] = imag - even_s[k]
    return cos_out, sin_out


def real_sum(cos_in, sin_in, n):
    if n == 1:
        return [cos_in[0]]
    half = n // 2
    if n == 2:
        return [cos_in[0] + cos_in[1], cos_in[0] - cos_in[1]]
    quarter = n // 4
    even_c = [None] * (quarter + 1)
    even_s = [None] * (quarter + 1)
    odd_c = [None] * (quarter + 1)
    odd_s = [None] * (quarter + 1)
    even_c[0] = cos_in[0] + cos_in[half]
    odd_c[0] = cos_in[0] - cos_in[half]
    even_c[quarter] = cos_in[quarter]
    odd_c[quarter] = sin_in[quarter]
    for k in range(1, quarter):
        theta = 2.0 * math.pi * k / n
        cosine, sine = math.cos(theta), math.sin(theta)
        even_c[k] = cos_in[k] + cos_in[half - k]
        even_s[k] = sin_in[k] - sin_in[half - k]
        gap = cos_in[k] - cos_in[half - k]
        both = sin_in[k] + sin_in[half - k]
        if 8 * k == n:
            odd_c[k] = cosine * (gap + both)
            odd_s[k] = cosine * (both - gap)
        else:
            odd_c[k] = cosine * gap + sine * both
            odd_s[k] = cosine * both - sine * gap
    evens = real_sum(even_c, even_s, half)
    odds = real_sum(odd_c, odd_s, half)
    out = [None] * n
    out[0::2] = evens
    out[1::2] = odds
    return out


def split_pair(value):
    high = value.astype(BF16)
    low = (value - high.astype(F32)).astype(BF16)
    return high, low


def dot(left, right):
    return jnp.dot(left, right, preferred_element_type=F32)


def triple_dot(high, low, table_ref):
    size = table_ref.shape[0] // 2
    table_high, table_low = table_ref[:size, :], table_ref[size:, :]
    left = jnp.concatenate([high, low, high], axis=1)
    return dot(left, jnp.concatenate([table_high, table_high, table_low], axis=0))


def slot_rows(comp, k1):
    half = DEVICES // 2
    near = pl.ds(comp * OWNED + k1, half, stride=SLOT)
    far = pl.ds(half * SLOT + comp * OWNED + k1 - 1, half, stride=SLOT)
    return near, far


EDGE_PARTS = 4
EDGES = OFFSETS * EDGE_PARTS


def edge_kernel(kernel_hbm, out_ref, tiles_ref, sem):
    n_tiles = CELLS // LANES
    copies = []
    for j in range(n_tiles):
        lanes = pl.ds(LANES * j, LANES)
        for i, (source, target) in enumerate([((0, 3), (0, 3)), ((4, 1), (3, 1))]):
            copy = pltpu.make_async_copy(
                kernel_hbm.at[:, pl.ds(*source), pl.ds(0, 1), lanes],
                tiles_ref.at[j, :, pl.ds(*target)],
                sem.at[j, i],
            )
            copy.start()
            copies.append(copy)
    flat = tiles_ref.reshape(n_tiles * EDGES, LANES)
    for j in range(n_tiles):
        copies[2 * j].wait()
        copies[2 * j + 1].wait()
        out_ref[:, LANES * j : LANES * (j + 1)] = flat[pl.ds(j * EDGES, EDGES), :]


def forward_y_kernel(x_ref, table_ref, twiddle_ref, out_hbm, high_ref, low_ref, out_ref, sem):
    slots = out_ref.reshape(DEVICES, SLOT, LANES)
    saves = []
    edges = []
    half = DEVICES // 2
    middle = COARSE // 2
    group = 16
    lane = lax.broadcasted_iota(jnp.int32, (X_ROWS, LANES), 1)
    alternate = 1.0 - 2.0 * (lax.broadcasted_iota(jnp.int32, (X_ROWS, FINE), 1) % 2).astype(F32)
    for comp in range(COMPS):
        base = comp * (middle + 1) * X_ROWS
        nyquist = []
        for g in range(X_ROWS // group):
            top = comp * X_ROWS + g * group
            parts = [x_ref[top : top + group, FINE * a : FINE * (a + 1)] for a in range(COARSE)]
            cos_out, sin_out = real_dft(parts)
            nyquist.append(jnp.sum(cos_out[0] * alternate[:group], axis=1, keepdims=True))
            for k in range(middle + 1):
                rows = slice(base + k * X_ROWS + g * group, base + k * X_ROWS + (g + 1) * group)
                real = cos_out[k]
                imag = None
                if k > 0:
                    cosine = twiddle_ref[2 * k - 2 : 2 * k - 1, :]
                    sine = twiddle_ref[2 * k - 1 : 2 * k, :]
                    if k == middle:
                        real, imag = real * cosine, real * sine
                    else:
                        real, imag = real * cosine + sin_out[k] * sine, real * sine - sin_out[k] * cosine
                high_ref[rows, :LANES], low_ref[rows, :LANES] = split_pair(real)
                if imag is None:
                    zero = jnp.zeros((group, LANES), BF16)
                    high_ref[rows, LANES:], low_ref[rows, LANES:] = zero, zero
                else:
                    high_ref[rows, LANES:], low_ref[rows, LANES:] = split_pair(imag)
        edges.append(jnp.concatenate(nyquist, axis=0))
    out = triple_dot(high_ref[...], low_ref[...], table_ref)
    for comp in range(COMPS):

        def pick(k):
            row = (comp * (middle + 1) + k) * X_ROWS
            rows = out[row : row + X_ROWS]
            return rows[:, :LANES], rows[:, LANES:]

        for k in range(middle):
            real, imag = pick(k)
            if k == 0:
                last_real, last_imag = pick(middle)
                imag = jnp.where(lane == 0, edges[comp], imag)
                real = jnp.where(lane < half, real, last_real)
                imag = jnp.where(lane < half, imag, last_imag)
            if comp == COMPS - 1:
                real, imag = -imag, real
            block = jnp.concatenate([real, imag], axis=0).T
            near, far = slot_rows(comp, k)
            if k == 0:
                far = slot_rows(comp, middle)[1]
            out_ref[near, :] = block[:half]
            out_ref[far, :] = block[half:]
        lines = (slice(None), pl.ds(comp * OWNED, OWNED))
        save = pltpu.make_async_copy(slots.at[lines], out_hbm.at[lines], sem.at[comp])
        save.start()
        saves.append(save)
    for save in saves:
        save.wait()


def relayout_kernel(flag_ref, kernel_ref, out_ref, rows_ref, columns_ref):
    shifted = flag_ref[0] > 0
    n_ops = kernel_ref.shape[0] // 16
    sub = lax.broadcasted_iota(jnp.int32, (OWNED, CELLS), 0)
    for op in range(n_ops):
        low = kernel_ref[16 * op : 16 * op + 8, :]
        high = kernel_ref[16 * op + 8 : 16 * op + 16, :]
        moved = jnp.where(sub < 7, pltpu.roll(low, 7, 0), pltpu.roll(high, 7, 0))
        rows_ref[8 * op : 8 * op + 8, :] = jnp.where(shifted, moved, low)
    for tile in range(CELLS // LANES):
        block = rows_ref[:, LANES * tile : LANES * (tile + 1)].T
        columns_ref[LANES * tile : LANES * (tile + 1), : 8 * n_ops] = block

    def step(p1, carry):
        column = columns_ref[pl.ds(p1, X_ROWS, stride=ROWS), :]
        both = jnp.concatenate([column, column], axis=0).T
        out_ref[p1] = both[: 8 * n_ops]
        return carry

    lax.fori_loop(0, ROWS, step, 0, unroll=4)


def spectral_kernel(
    x_ref,
    kernel_hbm,
    delta_ref,
    twiddle_ref,
    back_twiddle_ref,
    table_ref,
    back_table_ref,
    out_ref,
    kernel_ref,
    extra_ref,
    sums_ref,
    pair_ref,
    spec_ref,
    fix_ref,
    back_ref,
    kernel_sem,
):
    span = 8
    piece = span * OPS * OWNED

    def fetch(step):
        start = step * piece if isinstance(step, int) else pl.multiple_of(step * piece, OWNED)
        rows = pl.ds(start, piece)
        return pltpu.make_async_copy(kernel_hbm.at[rows], kernel_ref.at[rows], kernel_sem.at[step])

    for step in range(ROWS // span):
        fetch(step).start()
    half = ROWS // 2
    lane = lax.broadcasted_iota(jnp.int32, (ROWS, LANES), 1)

    extra_ref[...] = jnp.zeros_like(extra_ref)
    for layer in range(LAYERS):
        for comp in range(COMPS):
            line = x_ref[pl.ds(layer * ROWS * SLOT + comp * OWNED, ROWS, stride=SLOT), :]
            extra_ref[pl.ds(comp * LAYERS + layer, ROWS, stride=EXTRA), :] = jnp.where((lane < X_ROWS) == (comp == COMPS - 1), line, 0.0)
    fix_ref[...] = jnp.zeros_like(fix_ref)

    def store_sums(values, place):
        cos_out, sin_out = real_dft(values)
        for k in range(half + 1):
            sums_ref[pl.ds(k * P1_ALL + place, OWNED), :] = cos_out[k]
        for k in range(1, half):
            sums_ref[pl.ds((half + k) * P1_ALL + place, OWNED), :] = sin_out[k]

    def over_rows(index, carry):
        layer = index // COMPS
        comp = index % COMPS
        base = layer * (ROWS * SLOT) + comp * OWNED
        base = pl.multiple_of(base, OWNED)
        values = [x_ref[pl.ds(base + r * SLOT, OWNED), :] for r in range(ROWS)]
        store_sums(values, pl.multiple_of(index * OWNED, OWNED))
        return carry

    lax.fori_loop(0, LAYERS * COMPS, over_rows, 0)
    for group in range(2):
        values = [extra_ref[r * EXTRA + group * 8 : r * EXTRA + group * 8 + 8, :] for r in range(ROWS)]
        store_sums(values, P1_ROWS + group * 8)

    def factors(ref, k):
        return [ref[pl.ds(4 * k + j, 1), :] for j in range(4)]

    def save_pair(row, value):
        high, low = split_pair(value)
        pair_ref[pl.ds(row, value.shape[0]), :LANES] = high
        pair_ref[pl.ds(row, value.shape[0]), LANES:] = low

    n_blocks = P1_ALL // OWNED

    def blocks(ref, row, count):
        return [ref[pl.ds(row + OWNED * j, OWNED), :] for j in range(count)]

    def save_line(p1, values):
        for j in range(0, n_blocks, 2):
            save_pair(p1 * P1_ALL + OWNED * j, jnp.concatenate(values[j : j + 2], axis=0))

    def twist(k):
        f = factors(twiddle_ref, k)
        cos_rows = blocks(sums_ref, k * P1_ALL, n_blocks)
        if k in (0, half):
            even = [c * f[0] for c in cos_rows]
            odd = [c * f[2] for c in cos_rows]
        else:
            sin_rows = blocks(sums_ref, (half + k) * P1_ALL, n_blocks)
            even = [c * f[0] + v * f[1] for c, v in zip(cos_rows, sin_rows)]
            odd = [c * f[2] - v * f[3] for c, v in zip(cos_rows, sin_rows)]
        if k == 0:
            save_line(0, even)
            return
        odd = [pltpu.roll(v, X_ROWS, 1) for v in odd]
        if k != half:
            save_line(k, [a + b for a, b in zip(even, odd)])
        save_line(ROWS - k, [a - b for a, b in zip(even, odd)])

    size = 2 * LANES

    def forward_dot(first, count, which):
        rows = pl.ds(first * P1_ALL, count * P1_ALL)
        both = dot(pair_ref[rows, :], table_ref[which * size : (which + 1) * size, :])
        spec_ref[rows, :] = both[:, :LANES] + both[:, LANES:]

    for k in range(6):
        twist(k)
    forward_dot(0, 6, 0)
    forward_dot(27, 5, 1)
    for k in range(6, 11):
        twist(k)
    forward_dot(6, 5, 0)
    forward_dot(22, 5, 1)
    for k in range(11, half + 1):
        twist(k)
    forward_dot(11, 5, 0)
    forward_dot(half, 6, 1)

    def mix(spectra, coefficient, edge=False):
        fields = []
        for target in range(LAYERS):
            total = [None, None, None]

            def add(comp, term):
                total[comp] = term if total[comp] is None else total[comp] + term

            for source in range(LAYERS):
                offset = target - source + LAYERS - 1
                mx, my, mz = spectra[source]
                if edge:
                    k = [coefficient(offset * EDGE_PARTS + j) for j in range(EDGE_PARTS)]
                    add(0, k[0] * mx + k[3] * mz)
                    add(1, k[1] * my)
                    add(2, k[3] * mx - k[2] * mz)
                    continue
                k = [coefficient(offset * PARTS + j) for j in range(PARTS)]
                add(0, k[0] * mx + k[3] * my + k[4] * mz)
                add(1, k[3] * mx + k[1] * my + k[5] * mz)
                add(2, k[4] * mx + k[5] * my - k[2] * mz)
            fields.append(total)
        return fields

    def fix_step(group, carry):
        base = group * OWNED
        spectra = [
            [
                spec_ref[pl.ds(base * P1_ALL + P1_ROWS + comp * LAYERS + source, OWNED, stride=P1_ALL), :]
                for comp in range(COMPS)
            ]
            for source in range(LAYERS)
        ]

        def coefficient(op):
            return delta_ref[pl.ds(pl.multiple_of(op * ROWS + base, OWNED), OWNED), :]

        fields = mix(spectra, coefficient, edge=True)
        for target in range(LAYERS):
            for comp in range(COMPS):
                row = base * P1_ROWS + (target * COMPS + comp) * OWNED
                fix_ref[pl.ds(row, OWNED, stride=P1_ROWS), :] = fields[target][comp]
        return carry

    lax.fori_loop(0, ROWS // OWNED, fix_step, 0)

    def mix_line(p1):
        lines = blocks(spec_ref, p1 * P1_ALL, LAYERS * COMPS)
        spectra = [lines[COMPS * s : COMPS * s + COMPS] for s in range(LAYERS)]
        kernel_base = p1 * (OPS * OWNED)

        def coefficient(op):
            return kernel_ref[pl.ds(kernel_base + op * OWNED, OWNED), :]

        fields = mix(spectra, coefficient)
        flat = [fields[j // COMPS][j % COMPS] for j in range(LAYERS * COMPS)]
        row = p1 * P1_ROWS
        fixes = blocks(fix_ref, row, LAYERS * COMPS)
        flat = [a + b for a, b in zip(flat, fixes)]
        for j in range(0, LAYERS * COMPS, 2):
            save_pair(row + OWNED * j, jnp.concatenate(flat[j : j + 2], axis=0))

    def backward_dot(p1, rows):
        which = p1 // half
        base = which * size if isinstance(p1, int) else pl.multiple_of(which * size, size)
        both = dot(pair_ref[pl.ds(p1 * P1_ROWS, rows), :], back_table_ref[pl.ds(base, size), :])
        back_ref[pl.ds(p1 * P1_ROWS, rows), :] = both[:, :LANES] + both[:, LANES:]

    fetch(0).wait()
    for p1 in range(span):
        mix_line(p1)

    def mix_step(step, carry):
        fetch(step).wait()
        p1 = pl.multiple_of(span * step, span)
        backward_dot(p1 - span, span * P1_ROWS)
        for i in range(span):
            mix_line(p1 + i)
        return carry

    lax.fori_loop(1, ROWS // span, mix_step, 0)
    backward_dot(ROWS - span, span * P1_ROWS)

    count = LAYERS * COMPS
    f = factors(back_twiddle_ref, 0)
    for j, value in enumerate(blocks(back_ref, 0, count)):
        sums_ref[pl.ds(OWNED * j, OWNED), :] = value * f[0]
    f = factors(back_twiddle_ref, half)
    for j, value in enumerate(blocks(back_ref, half * P1_ROWS, count)):
        swap = pltpu.roll(value, X_ROWS, 1)
        sums_ref[pl.ds(half * P1_ROWS + OWNED * j, OWNED), :] = value * f[0] - swap * f[2]

    def untwist(k):
        f = factors(back_twiddle_ref, k)
        near = blocks(back_ref, k * P1_ROWS, count)
        far = blocks(back_ref, (ROWS - k) * P1_ROWS, count)
        swaps = [pltpu.roll(a - b, X_ROWS, 1) for a, b in zip(near, far)]
        for j in range(count):
            plus = near[j] + far[j]
            sums_ref[pl.ds(k * P1_ROWS + OWNED * j, OWNED), :] = plus * f[0] + swaps[j] * f[2]
            sums_ref[pl.ds((half + k) * P1_ROWS + OWNED * j, OWNED), :] = swaps[j] * f[3] - plus * f[1]

    for k in range(1, half):
        untwist(k)

    def back_rows(index, carry):
        place = pl.multiple_of(index * OWNED, OWNED)
        cos_in = [sums_ref[pl.ds(k * P1_ROWS + place, OWNED), :] for k in range(half + 1)]
        sin_in = [None] + [sums_ref[pl.ds((half + k) * P1_ROWS + place, OWNED), :] for k in range(1, half)] + [None]
        values = real_sum(cos_in, sin_in, ROWS)
        layer = index // COMPS
        comp = index % COMPS
        base = pl.multiple_of(layer * (ROWS * SLOT) + comp * OWNED, OWNED)
        for r in range(ROWS):
            out_ref[pl.ds(base + r * SLOT, OWNED), :] = values[r]
        return carry

    lax.fori_loop(0, LAYERS * COMPS, back_rows, 0)


def inverse_y_kernel(x_ref, table_ref, twiddle_ref, out_hbm, high_ref, low_ref, lines_ref, result_ref, sem):
    half = DEVICES // 2
    middle = COARSE // 2
    group = 8
    lane = lax.broadcasted_iota(jnp.int32, (X_ROWS, LANES), 1)
    alternate = 1.0 - 2.0 * (lax.broadcasted_iota(jnp.int32, (group, FINE), 1) % 2).astype(F32)
    copies = []
    columns = []
    for comp in range(COMPS):
        size = (middle + 1) * X_ROWS
        base = comp * size

        def put(k, real, imag):
            rows = slice(base + k * X_ROWS, base + (k + 1) * X_ROWS)
            high_ref[rows, :LANES], low_ref[rows, :LANES] = split_pair(real)
            high_ref[rows, LANES:], low_ref[rows, LANES:] = split_pair(imag)

        for k in range(middle):
            near, far = slot_rows(comp, k)
            if k == 0:
                far = slot_rows(comp, middle)[1]
            block = jnp.concatenate([x_ref[near, :], x_ref[far, :]], axis=0).T
            real, imag = block[:X_ROWS], block[X_ROWS:]
            if comp == COMPS - 1:
                real, imag = -imag, real
            if k == 0:
                nyquist = imag[:, :1]
                put(middle, jnp.where(lane < half, 0.0, real), jnp.where(lane < half, 0.0, imag))
                scale = jnp.where(lane < half, jnp.where(lane == 0, 0.5, 1.0), 0.0)
                real, imag = real * scale, imag * scale
            put(k, real, imag)
        columns.append(nyquist)
    lines_ref[...] = triple_dot(high_ref[...], low_ref[...], table_ref)
    for comp in range(COMPS):
        base = comp * (middle + 1) * X_ROWS
        nyquist = columns[comp]
        for g in range(X_ROWS // group):
            cos_in = [None] * (middle + 1)
            sin_in = [None] * (middle + 1)
            for k in range(middle + 1):
                rows = slice(base + k * X_ROWS + g * group, base + k * X_ROWS + (g + 1) * group)
                real = lines_ref[rows, :LANES]
                if k == 0:
                    cos_in[0] = 2.0 * real + nyquist[g * group : (g + 1) * group] * alternate
                    continue
                imag = lines_ref[rows, LANES:]
                cosine = twiddle_ref[2 * k - 2 : 2 * k - 1, :]
                sine = twiddle_ref[2 * k - 1 : 2 * k, :]
                cos_in[k] = real * cosine - imag * sine
                if k < middle:
                    sin_in[k] = -(real * sine + imag * cosine)
            values = real_sum(cos_in, sin_in, COARSE)
            top = comp * X_ROWS + g * group
            for a in range(COARSE):
                result_ref[top : top + group, FINE * a : FINE * (a + 1)] = values[a]
        span = pl.ds(comp * X_ROWS, X_ROWS)
        copy = pltpu.make_async_copy(result_ref.at[span], out_hbm.at[span], sem.at[comp])
        copy.start()
        copies.append(copy)
    for copy in copies:
        copy.wait()


VMEM = pl.BlockSpec(memory_space=pltpu.VMEM)
HBM = pl.BlockSpec(memory_space=pltpu.HBM)
FINE_ROWS = COMPS * (COARSE // 2 + 1) * X_ROWS


def params(mebibytes):
    return pltpu.CompilerParams(vmem_limit_bytes=mebibytes * 1024 * 1024)


def edge_lines(kernel):
    return pl.pallas_call(
        edge_kernel,
        in_specs=[HBM],
        out_specs=VMEM,
        out_shape=jax.ShapeDtypeStruct((EDGES, CELLS), F32),
        scratch_shapes=[
            pltpu.VMEM((CELLS // LANES, OFFSETS, EDGE_PARTS, 1, LANES), F32),
            pltpu.SemaphoreType.DMA((CELLS // LANES, 2)),
        ],
        compiler_params=params(58),
        name="edge_lines",
    )(kernel)


def forward_y(field):
    table = stacked(fine_table())
    twiddle = y_twiddle(-1.0, 1.0)
    return pl.pallas_call(
        forward_y_kernel,
        in_specs=[VMEM] * 3,
        out_specs=HBM,
        out_shape=jax.ShapeDtypeStruct((DEVICES, SLOT, LANES), F32),
        scratch_shapes=[
            pltpu.VMEM((FINE_ROWS, 2 * LANES), BF16),
            pltpu.VMEM((FINE_ROWS, 2 * LANES), BF16),
            pltpu.VMEM((DEVICES * SLOT, LANES), F32),
            pltpu.SemaphoreType.DMA((COMPS,)),
        ],
        compiler_params=params(48),
        name="forward_y",
    )(field, jnp.asarray(table), jnp.asarray(twiddle))


def relayout(kernel, flag):
    groups = 3
    rows = OPS // groups * 16
    out_rows = OPS // groups * OWNED
    return pl.pallas_call(
        relayout_kernel,
        grid=(groups,),
        in_specs=[
            pl.BlockSpec(memory_space=pltpu.SMEM),
            pl.BlockSpec((rows, CELLS), lambda g: (g, 0)),
        ],
        out_specs=pl.BlockSpec((ROWS, out_rows, LANES), lambda g: (0, g, 0)),
        out_shape=jax.ShapeDtypeStruct((ROWS, OPS * OWNED, LANES), F32),
        scratch_shapes=[pltpu.VMEM((out_rows, CELLS), F32), pltpu.VMEM((CELLS, LANES), F32)],
        compiler_params=params(48),
        name="relayout",
    )(flag, kernel)


def spectral(lines, kernel, delta):
    twiddle = x_twiddle(-1.0, 1.0, 1.0)
    back_twiddle = x_twiddle(1.0, -1.0 / (CELLS * CELLS), -1.0)
    return pl.pallas_call(
        spectral_kernel,
        in_specs=[VMEM, HBM] + [VMEM] * 5,
        out_specs=VMEM,
        out_shape=jax.ShapeDtypeStruct((DEVICES * SLOT, LANES), F32),
        scratch_shapes=[
            pltpu.VMEM((ROWS * OPS * OWNED, LANES), F32),
            pltpu.VMEM((ROWS * EXTRA, LANES), F32),
            pltpu.VMEM((ROWS * P1_ALL, LANES), F32),
            pltpu.VMEM((ROWS * P1_ALL, 2 * LANES), BF16),
            pltpu.VMEM((ROWS * P1_ALL, LANES), F32),
            pltpu.VMEM((ROWS * P1_ROWS, LANES), F32),
            pltpu.VMEM((ROWS * P1_ROWS, LANES), F32),
            pltpu.SemaphoreType.DMA((4,)),
        ],
        compiler_params=params(48),
        name="spectral",
    )(
        lines,
        kernel,
        delta,
        jnp.asarray(twiddle),
        jnp.asarray(back_twiddle),
        jnp.asarray(x_tables(-1.0)),
        jnp.asarray(x_tables(1.0)),
    )


def inverse_y(spectra):
    rows = COMPS * X_ROWS
    return pl.pallas_call(
        inverse_y_kernel,
        in_specs=[VMEM] * 3,
        out_specs=HBM,
        out_shape=jax.ShapeDtypeStruct((rows, CELLS), F32),
        scratch_shapes=[
            pltpu.VMEM((FINE_ROWS, 2 * LANES), BF16),
            pltpu.VMEM((FINE_ROWS, 2 * LANES), BF16),
            pltpu.VMEM((FINE_ROWS, 2 * LANES), F32),
            pltpu.VMEM((rows, CELLS), F32),
            pltpu.SemaphoreType.DMA((COMPS,)),
        ],
        compiler_params=params(20),
        name="inverse_y",
    )(spectra, jnp.asarray(stacked(fine_table().T)), jnp.asarray(y_twiddle(1.0, 2.0)))


def exchange(lines):
    moved = lax.all_to_all(lines.reshape(DEVICES, SLOT, LANES), ("layer", "row"), 0, 0, tiled=True)
    return moved.reshape(DEVICES * SLOT, LANES)


def local(magnet, kernel):
    axes = ("layer", "row")
    device = lax.axis_index(axes)
    field = magnet.reshape(COMPS * X_ROWS, CELLS)
    flag = (device >= DEVICES // 2).astype(jnp.int32).reshape(1)
    edge = edge_lines(kernel)
    middle = lax.ppermute(edge, axes, [(DEVICES // 2, 0)])
    sent = forward_y(field)
    got = exchange(sent)
    coefficient = relayout(kernel.reshape(OPS * 16, CELLS), flag)
    delta = jnp.where(device == 0, middle - edge, 0.0)
    delta = jnp.swapaxes(delta.reshape(EDGES, X_ROWS, ROWS), 1, 2)
    delta = jnp.concatenate([delta, delta], axis=2).reshape(EDGES * ROWS, LANES)
    fields = spectral(got, coefficient.reshape(ROWS * OPS * OWNED, LANES), delta)
    result = inverse_y(exchange(fields))
    return result.reshape(COMPS, 1, X_ROWS, CELLS)


def solution(mesh):
    in_specs = (P(None, "layer", "row", None), P(None, None, ("layer", "row"), None))
    out_specs = P(None, "layer", "row", None)
    return jax.shard_map(local, mesh=mesh, in_specs=in_specs, out_specs=out_specs, check_vma=False)
```

```python
import math

import jax
import jax.numpy as jnp
import numpy as np
from jax import lax
from jax.experimental import pallas as pl
from jax.experimental.pallas import tpu as pltpu
from jax.sharding import PartitionSpec as P


CELLS = 2048
COMPS = 3
LAYERS = 4
ROWS = 32
X_ROWS = 64
DEVICES = 128
PARTS = 6
OFFSETS = 7
OPS = OFFSETS * PARTS
FINE = 128
COARSE = 16
OWNED = 8
SLOT = COMPS * OWNED
LANES = 128
EXTRA = 16
P1_ROWS = LAYERS * COMPS * OWNED
P1_ALL = P1_ROWS + EXTRA

F32 = jnp.float32
BF16 = jnp.bfloat16


def halves(table):
    high = np.asarray(table, np.float32).astype(jnp.bfloat16)
    low = (np.asarray(table, np.float64) - high.astype(np.float64)).astype(np.float32).astype(jnp.bfloat16)
    return high, low


def fine_table():
    index = np.arange(FINE)
    angle = 2.0 * np.pi * (np.outer(index, index) % FINE) / FINE
    return np.block([[np.cos(angle), -np.sin(angle)], [np.sin(angle), np.cos(angle)]])


def stacked(table):
    return np.concatenate(halves(table), axis=0)


def y_twiddle(sign, scale):
    k = np.arange(1, COARSE // 2 + 1)[:, None]
    b = np.arange(FINE)[None, :]
    angle = 2.0 * np.pi * k * b / CELLS
    table = scale * np.stack([np.cos(angle), sign * np.sin(angle)], axis=1)
    return table.reshape(COARSE, FINE).astype(np.float32)


def x_twiddle(sign, scale, inner):
    k = np.arange(ROWS // 2 + 1)[:, None]
    t = np.arange(X_ROWS)[None, :]
    angle = 2.0 * np.pi * k * t / CELLS
    cosine = scale * np.cos(angle)
    sine = scale * sign * np.sin(angle)
    lines = [
        np.concatenate([cosine, cosine], axis=1),
        np.concatenate([sine, sine], axis=1),
        np.concatenate([inner * sine, -inner * sine], axis=1),
        np.concatenate([inner * cosine, -inner * cosine], axis=1),
    ]
    return np.stack(lines, axis=1).astype(np.float32).reshape(-1, LANES)


def x_table(sign, shift):
    index = np.arange(X_ROWS)
    place = np.outer(index, index + shift) if sign < 0 else np.outer(index + shift, index)
    angle = 2.0 * np.pi * (place % X_ROWS) / X_ROWS
    real = np.cos(angle)
    imag = sign * np.sin(angle)
    whole = np.block([[real, imag], [-imag, real]])
    high, low = halves(whole)
    line = np.concatenate([high, low], axis=1)
    return np.concatenate([line, line], axis=0)


def x_tables(sign):
    return np.concatenate([x_table(sign, 0), x_table(sign, 1)], axis=0)


def real_dft(values):
    n = len(values)
    if n == 1:
        return [values[0]], [None]
    if n == 2:
        return [values[0] + values[1], values[0] - values[1]], [None, None]
    even_c, even_s = real_dft(values[0::2])
    odd_c, odd_s = real_dft(values[1::2])
    half = n // 2
    quarter = n // 4
    cos_out = [None] * (half + 1)
    sin_out = [None] * (half + 1)
    for k in range(quarter + 1):
        if k == 0:
            cos_out[0] = even_c[0] + odd_c[0]
            cos_out[half] = even_c[0] - odd_c[0]
        elif k == quarter:
            cos_out[k] = even_c[k]
            sin_out[k] = odd_c[k]
        else:
            theta = 2.0 * math.pi * k / n
            cosine, sine = math.cos(theta), math.sin(theta)
            if 8 * k == n:
                real = cosine * (odd_c[k] - odd_s[k])
                imag = cosine * (odd_s[k] + odd_c[k])
            else:
                real = cosine * odd_c[k] - sine * odd_s[k]
                imag = cosine * odd_s[k] + sine * odd_c[k]
            cos_out[k] = even_c[k] + real
            sin_out[k] = even_s[k] + imag
            cos_out[half - k] = even_c[k] - real
            sin_out[half - k] = imag - even_s[k]
    return cos_out, sin_out


def real_sum(cos_in, sin_in, n):
    if n == 1:
        return [cos_in[0]]
    half = n // 2
    if n == 2:
        return [cos_in[0] + cos_in[1], cos_in[0] - cos_in[1]]
    quarter = n // 4
    even_c = [None] * (quarter + 1)
    even_s = [None] * (quarter + 1)
    odd_c = [None] * (quarter + 1)
    odd_s = [None] * (quarter + 1)
    even_c[0] = cos_in[0] + cos_in[half]
    odd_c[0] = cos_in[0] - cos_in[half]
    even_c[quarter] = cos_in[quarter]
    odd_c[quarter] = sin_in[quarter]
    for k in range(1, quarter):
        theta = 2.0 * math.pi * k / n
        cosine, sine = math.cos(theta), math.sin(theta)
        even_c[k] = cos_in[k] + cos_in[half - k]
        even_s[k] = sin_in[k] - sin_in[half - k]
        gap = cos_in[k] - cos_in[half - k]
        both = sin_in[k] + sin_in[half - k]
        if 8 * k == n:
            odd_c[k] = cosine * (gap + both)
            odd_s[k] = cosine * (both - gap)
        else:
            odd_c[k] = cosine * gap + sine * both
            odd_s[k] = cosine * both - sine * gap
    evens = real_sum(even_c, even_s, half)
    odds = real_sum(odd_c, odd_s, half)
    out = [None] * n
    out[0::2] = evens
    out[1::2] = odds
    return out


def split_pair(value):
    high = value.astype(BF16)
    low = (value - high.astype(F32)).astype(BF16)
    return high, low


def dot(left, right):
    return jnp.dot(left, right, preferred_element_type=F32)


def triple_dot(high, low, table_ref):
    size = table_ref.shape[0] // 2
    table_high, table_low = table_ref[:size, :], table_ref[size:, :]
    left = jnp.concatenate([high, low, high], axis=1)
    return dot(left, jnp.concatenate([table_high, table_high, table_low], axis=0))


def slot_rows(comp, k1):
    half = DEVICES // 2
    near = pl.ds(comp * OWNED + k1, half, stride=SLOT)
    far = pl.ds(half * SLOT + comp * OWNED + k1 - 1, half, stride=SLOT)
    return near, far


EDGE_PARTS = 4
EDGES = OFFSETS * EDGE_PARTS


def forward_y_kernel(
    x_hbm, table_hbm, twiddle_hbm, kernel_hbm, out_hbm, edge_hbm,
    high_ref, low_ref, out_ref, x_ref, table_ref, twiddle_ref, edge_ref, sem, load_sem, edge_sem,
):
    spans = [pl.ds(comp * X_ROWS, X_ROWS) for comp in range(COMPS)]
    loads = [pltpu.make_async_copy(x_hbm.at[b], x_ref.at[b], load_sem.at[c]) for c, b in enumerate(spans)]
    tables = [
        pltpu.make_async_copy(twiddle_hbm, twiddle_ref, load_sem.at[COMPS]),
        pltpu.make_async_copy(table_hbm, table_ref, load_sem.at[COMPS + 1]),
    ]
    lines = [
        pltpu.make_async_copy(
            kernel_hbm.at[:, pl.ds(*source), pl.ds(0, 1)], edge_ref.at[:, pl.ds(*target)], edge_sem.at[i]
        )
        for i, (source, target) in enumerate([((0, 3), (0, 3)), ((4, 1), (3, 1))])
    ]
    for copy in [loads[0]] + tables + loads[1:] + lines:
        copy.start()
    tables[0].wait()
    slots = out_ref.reshape(DEVICES, SLOT, LANES)
    saves = []
    edges = []
    half = DEVICES // 2
    middle = COARSE // 2
    group = 16
    lane = lax.broadcasted_iota(jnp.int32, (X_ROWS, LANES), 1)
    alternate = 1.0 - 2.0 * (lax.broadcasted_iota(jnp.int32, (X_ROWS, FINE), 1) % 2).astype(F32)
    for comp in range(COMPS):
        base = comp * (middle + 1) * X_ROWS
        nyquist = []
        loads[comp].wait()
        for g in range(X_ROWS // group):
            top = comp * X_ROWS + g * group
            parts = [x_ref[top : top + group, FINE * a : FINE * (a + 1)] for a in range(COARSE)]
            cos_out, sin_out = real_dft(parts)
            nyquist.append(jnp.sum(cos_out[0] * alternate[:group], axis=1, keepdims=True))
            for k in range(middle + 1):
                rows = slice(base + k * X_ROWS + g * group, base + k * X_ROWS + (g + 1) * group)
                real = cos_out[k]
                imag = None
                if k > 0:
                    cosine = twiddle_ref[2 * k - 2 : 2 * k - 1, :]
                    sine = twiddle_ref[2 * k - 1 : 2 * k, :]
                    if k == middle:
                        real, imag = real * cosine, real * sine
                    else:
                        real, imag = real * cosine + sin_out[k] * sine, real * sine - sin_out[k] * cosine
                high_ref[rows, :LANES], low_ref[rows, :LANES] = split_pair(real)
                if imag is None:
                    zero = jnp.zeros((group, LANES), BF16)
                    high_ref[rows, LANES:], low_ref[rows, LANES:] = zero, zero
                else:
                    high_ref[rows, LANES:], low_ref[rows, LANES:] = split_pair(imag)
        edges.append(jnp.concatenate(nyquist, axis=0))
    for copy in lines:
        copy.wait()
    save = pltpu.make_async_copy(edge_ref, edge_hbm, edge_sem.at[2])
    save.start()
    saves.append(save)
    tables[1].wait()
    out = triple_dot(high_ref[...], low_ref[...], table_ref)
    for comp in range(COMPS):

        def pick(k):
            row = (comp * (middle + 1) + k) * X_ROWS
            rows = out[row : row + X_ROWS]
            return rows[:, :LANES], rows[:, LANES:]

        for k in range(middle):
            real, imag = pick(k)
            if k == 0:
                last_real, last_imag = pick(middle)
                imag = jnp.where(lane == 0, edges[comp], imag)
                real = jnp.where(lane < half, real, last_real)
                imag = jnp.where(lane < half, imag, last_imag)
            if comp == COMPS - 1:
                real, imag = -imag, real
            block = jnp.concatenate([real, imag], axis=0).T
            near, far = slot_rows(comp, k)
            if k == 0:
                far = slot_rows(comp, middle)[1]
            out_ref[near, :] = block[:half]
            out_ref[far, :] = block[half:]
        part = (slice(None), pl.ds(comp * OWNED, OWNED))
        save = pltpu.make_async_copy(slots.at[part], out_hbm.at[part], sem.at[comp])
        save.start()
        saves.append(save)
    for save in saves:
        save.wait()


def relayout_kernel(flag_ref, kernel_ref, out_ref, rows_ref, columns_ref):
    shifted = flag_ref[0] > 0
    n_ops = kernel_ref.shape[0] // 16
    sub = lax.broadcasted_iota(jnp.int32, (OWNED, CELLS), 0)
    for op in range(n_ops):
        low = kernel_ref[16 * op : 16 * op + 8, :]
        high = kernel_ref[16 * op + 8 : 16 * op + 16, :]
        moved = jnp.where(sub < 7, pltpu.roll(low, 7, 0), pltpu.roll(high, 7, 0))
        rows_ref[8 * op : 8 * op + 8, :] = jnp.where(shifted, moved, low)
    for tile in range(CELLS // LANES):
        block = rows_ref[:, LANES * tile : LANES * (tile + 1)].T
        columns_ref[LANES * tile : LANES * (tile + 1), : 8 * n_ops] = block

    def step(p1, carry):
        column = columns_ref[pl.ds(p1, X_ROWS, stride=ROWS), :]
        both = jnp.concatenate([column, column], axis=0).T
        out_ref[p1] = both[: 8 * n_ops]
        return carry

    lax.fori_loop(0, ROWS, step, 0, unroll=4)


def spectral_kernel(
    x_ref,
    kernel_hbm,
    delta_ref,
    twiddle_ref,
    back_twiddle_ref,
    table_ref,
    back_table_ref,
    out_ref,
    kernel_ref,
    extra_ref,
    sums_ref,
    pair_ref,
    spec_ref,
    fix_ref,
    back_ref,
    kernel_sem,
):
    span = 8
    piece = span * OPS * OWNED

    def fetch(step):
        start = step * piece if isinstance(step, int) else pl.multiple_of(step * piece, OWNED)
        rows = pl.ds(start, piece)
        return pltpu.make_async_copy(kernel_hbm.at[rows], kernel_ref.at[rows], kernel_sem.at[step])

    for step in range(ROWS // span):
        fetch(step).start()
    half = ROWS // 2
    lane = lax.broadcasted_iota(jnp.int32, (ROWS, LANES), 1)

    extra_ref[...] = jnp.zeros_like(extra_ref)
    for layer in range(LAYERS):
        for comp in range(COMPS):
            line = x_ref[pl.ds(layer * ROWS * SLOT + comp * OWNED, ROWS, stride=SLOT), :]
            extra_ref[pl.ds(comp * LAYERS + layer, ROWS, stride=EXTRA), :] = jnp.where((lane < X_ROWS) == (comp == COMPS - 1), line, 0.0)
    fix_ref[...] = jnp.zeros_like(fix_ref)

    def store_sums(values, place):
        cos_out, sin_out = real_dft(values)
        for k in range(half + 1):
            sums_ref[pl.ds(k * P1_ALL + place, OWNED), :] = cos_out[k]
        for k in range(1, half):
            sums_ref[pl.ds((half + k) * P1_ALL + place, OWNED), :] = sin_out[k]

    def over_rows(index, carry):
        layer = index // COMPS
        comp = index % COMPS
        base = layer * (ROWS * SLOT) + comp * OWNED
        base = pl.multiple_of(base, OWNED)
        values = [x_ref[pl.ds(base + r * SLOT, OWNED), :] for r in range(ROWS)]
        store_sums(values, pl.multiple_of(index * OWNED, OWNED))
        return carry

    lax.fori_loop(0, LAYERS * COMPS, over_rows, 0)
    for group in range(2):
        values = [extra_ref[r * EXTRA + group * 8 : r * EXTRA + group * 8 + 8, :] for r in range(ROWS)]
        store_sums(values, P1_ROWS + group * 8)

    def factors(ref, k):
        return [ref[pl.ds(4 * k + j, 1), :] for j in range(4)]

    def save_pair(row, value):
        high, low = split_pair(value)
        pair_ref[pl.ds(row, value.shape[0]), :LANES] = high
        pair_ref[pl.ds(row, value.shape[0]), LANES:] = low

    n_blocks = P1_ALL // OWNED

    def blocks(ref, row, count):
        return [ref[pl.ds(row + OWNED * j, OWNED), :] for j in range(count)]

    def save_line(p1, values):
        for j in range(0, n_blocks, 2):
            save_pair(p1 * P1_ALL + OWNED * j, jnp.concatenate(values[j : j + 2], axis=0))

    def twist(k):
        f = factors(twiddle_ref, k)
        cos_rows = blocks(sums_ref, k * P1_ALL, n_blocks)
        if k in (0, half):
            even = [c * f[0] for c in cos_rows]
            odd = [c * f[2] for c in cos_rows]
        else:
            sin_rows = blocks(sums_ref, (half + k) * P1_ALL, n_blocks)
            even = [c * f[0] + v * f[1] for c, v in zip(cos_rows, sin_rows)]
            odd = [c * f[2] - v * f[3] for c, v in zip(cos_rows, sin_rows)]
        if k == 0:
            save_line(0, even)
            return
        odd = [pltpu.roll(v, X_ROWS, 1) for v in odd]
        if k != half:
            save_line(k, [a + b for a, b in zip(even, odd)])
        save_line(ROWS - k, [a - b for a, b in zip(even, odd)])

    size = 2 * LANES

    def forward_dot(first, count, which):
        rows = pl.ds(first * P1_ALL, count * P1_ALL)
        both = dot(pair_ref[rows, :], table_ref[which * size : (which + 1) * size, :])
        spec_ref[rows, :] = both[:, :LANES] + both[:, LANES:]

    for k in range(6):
        twist(k)
    forward_dot(0, 6, 0)
    forward_dot(27, 5, 1)
    for k in range(6, 11):
        twist(k)
    forward_dot(6, 5, 0)
    forward_dot(22, 5, 1)
    for k in range(11, half + 1):
        twist(k)
    forward_dot(11, 5, 0)
    forward_dot(half, 6, 1)

    def mix(spectra, coefficient, edge=False):
        fields = []
        for target in range(LAYERS):
            total = [None, None, None]

            def add(comp, term):
                total[comp] = term if total[comp] is None else total[comp] + term

            for source in range(LAYERS):
                offset = target - source + LAYERS - 1
                mx, my, mz = spectra[source]
                if edge:
                    k = [coefficient(offset * EDGE_PARTS + j) for j in range(EDGE_PARTS)]
                    add(0, k[0] * mx + k[3] * mz)
                    add(1, k[1] * my)
                    add(2, k[3] * mx - k[2] * mz)
                    continue
                k = [coefficient(offset * PARTS + j) for j in range(PARTS)]
                add(0, k[0] * mx + k[3] * my + k[4] * mz)
                add(1, k[3] * mx + k[1] * my + k[5] * mz)
                add(2, k[4] * mx + k[5] * my - k[2] * mz)
            fields.append(total)
        return fields

    def fix_step(group, carry):
        base = group * OWNED
        spectra = [
            [
                spec_ref[pl.ds(base * P1_ALL + P1_ROWS + comp * LAYERS + source, OWNED, stride=P1_ALL), :]
                for comp in range(COMPS)
            ]
            for source in range(LAYERS)
        ]

        def coefficient(op):
            return delta_ref[pl.ds(pl.multiple_of(op * ROWS + base, OWNED), OWNED), :]

        fields = mix(spectra, coefficient, edge=True)
        for target in range(LAYERS):
            for comp in range(COMPS):
                row = base * P1_ROWS + (target * COMPS + comp) * OWNED
                fix_ref[pl.ds(row, OWNED, stride=P1_ROWS), :] = fields[target][comp]
        return carry

    lax.fori_loop(0, ROWS // OWNED, fix_step, 0)

    def mix_line(p1):
        lines = blocks(spec_ref, p1 * P1_ALL, LAYERS * COMPS)
        spectra = [lines[COMPS * s : COMPS * s + COMPS] for s in range(LAYERS)]
        kernel_base = p1 * (OPS * OWNED)

        def coefficient(op):
            return kernel_ref[pl.ds(kernel_base + op * OWNED, OWNED), :]

        fields = mix(spectra, coefficient)
        flat = [fields[j // COMPS][j % COMPS] for j in range(LAYERS * COMPS)]
        row = p1 * P1_ROWS
        fixes = blocks(fix_ref, row, LAYERS * COMPS)
        flat = [a + b for a, b in zip(flat, fixes)]
        for j in range(0, LAYERS * COMPS, 2):
            save_pair(row + OWNED * j, jnp.concatenate(flat[j : j + 2], axis=0))

    def backward_dot(p1, rows):
        which = p1 // half
        base = which * size if isinstance(p1, int) else pl.multiple_of(which * size, size)
        both = dot(pair_ref[pl.ds(p1 * P1_ROWS, rows), :], back_table_ref[pl.ds(base, size), :])
        back_ref[pl.ds(p1 * P1_ROWS, rows), :] = both[:, :LANES] + both[:, LANES:]

    fetch(0).wait()
    for p1 in range(span):
        mix_line(p1)

    def mix_step(step, carry):
        fetch(step).wait()
        p1 = pl.multiple_of(span * step, span)
        backward_dot(p1 - span, span * P1_ROWS)
        for i in range(span):
            mix_line(p1 + i)
        return carry

    lax.fori_loop(1, ROWS // span, mix_step, 0)
    backward_dot(ROWS - span, span * P1_ROWS)

    count = LAYERS * COMPS
    f = factors(back_twiddle_ref, 0)
    for j, value in enumerate(blocks(back_ref, 0, count)):
        sums_ref[pl.ds(OWNED * j, OWNED), :] = value * f[0]
    f = factors(back_twiddle_ref, half)
    for j, value in enumerate(blocks(back_ref, half * P1_ROWS, count)):
        swap = pltpu.roll(value, X_ROWS, 1)
        sums_ref[pl.ds(half * P1_ROWS + OWNED * j, OWNED), :] = value * f[0] - swap * f[2]

    def untwist(k):
        f = factors(back_twiddle_ref, k)
        near = blocks(back_ref, k * P1_ROWS, count)
        far = blocks(back_ref, (ROWS - k) * P1_ROWS, count)
        swaps = [pltpu.roll(a - b, X_ROWS, 1) for a, b in zip(near, far)]
        for j in range(count):
            plus = near[j] + far[j]
            sums_ref[pl.ds(k * P1_ROWS + OWNED * j, OWNED), :] = plus * f[0] + swaps[j] * f[2]
            sums_ref[pl.ds((half + k) * P1_ROWS + OWNED * j, OWNED), :] = swaps[j] * f[3] - plus * f[1]

    for k in range(1, half):
        untwist(k)

    def back_rows(index, carry):
        place = pl.multiple_of(index * OWNED, OWNED)
        cos_in = [sums_ref[pl.ds(k * P1_ROWS + place, OWNED), :] for k in range(half + 1)]
        sin_in = [None] + [sums_ref[pl.ds((half + k) * P1_ROWS + place, OWNED), :] for k in range(1, half)] + [None]
        values = real_sum(cos_in, sin_in, ROWS)
        layer = index // COMPS
        comp = index % COMPS
        base = pl.multiple_of(layer * (ROWS * SLOT) + comp * OWNED, OWNED)
        for r in range(ROWS):
            out_ref[pl.ds(base + r * SLOT, OWNED), :] = values[r]
        return carry

    lax.fori_loop(0, LAYERS * COMPS, back_rows, 0)


def inverse_y_kernel(x_ref, table_ref, twiddle_ref, out_hbm, high_ref, low_ref, lines_ref, result_ref, sem):
    half = DEVICES // 2
    middle = COARSE // 2
    group = 8
    lane = lax.broadcasted_iota(jnp.int32, (X_ROWS, LANES), 1)
    alternate = 1.0 - 2.0 * (lax.broadcasted_iota(jnp.int32, (group, FINE), 1) % 2).astype(F32)
    copies = []
    columns = []
    for comp in range(COMPS):
        size = (middle + 1) * X_ROWS
        base = comp * size

        def put(k, real, imag):
            rows = slice(base + k * X_ROWS, base + (k + 1) * X_ROWS)
            high_ref[rows, :LANES], low_ref[rows, :LANES] = split_pair(real)
            high_ref[rows, LANES:], low_ref[rows, LANES:] = split_pair(imag)

        for k in range(middle):
            near, far = slot_rows(comp, k)
            if k == 0:
                far = slot_rows(comp, middle)[1]
            block = jnp.concatenate([x_ref[near, :], x_ref[far, :]], axis=0).T
            real, imag = block[:X_ROWS], block[X_ROWS:]
            if comp == COMPS - 1:
                real, imag = -imag, real
            if k == 0:
                nyquist = imag[:, :1]
                put(middle, jnp.where(lane < half, 0.0, real), jnp.where(lane < half, 0.0, imag))
                scale = jnp.where(lane < half, jnp.where(lane == 0, 0.5, 1.0), 0.0)
                real, imag = real * scale, imag * scale
            put(k, real, imag)
        columns.append(nyquist)
    lines_ref[...] = triple_dot(high_ref[...], low_ref[...], table_ref)
    for comp in range(COMPS):
        base = comp * (middle + 1) * X_ROWS
        nyquist = columns[comp]
        for g in range(X_ROWS // group):
            cos_in = [None] * (middle + 1)
            sin_in = [None] * (middle + 1)
            for k in range(middle + 1):
                rows = slice(base + k * X_ROWS + g * group, base + k * X_ROWS + (g + 1) * group)
                real = lines_ref[rows, :LANES]
                if k == 0:
                    cos_in[0] = 2.0 * real + nyquist[g * group : (g + 1) * group] * alternate
                    continue
                imag = lines_ref[rows, LANES:]
                cosine = twiddle_ref[2 * k - 2 : 2 * k - 1, :]
                sine = twiddle_ref[2 * k - 1 : 2 * k, :]
                cos_in[k] = real * cosine - imag * sine
                if k < middle:
                    sin_in[k] = -(real * sine + imag * cosine)
            values = real_sum(cos_in, sin_in, COARSE)
            top = comp * X_ROWS + g * group
            for a in range(COARSE):
                result_ref[top : top + group, FINE * a : FINE * (a + 1)] = values[a]
        span = pl.ds(comp * X_ROWS, X_ROWS)
        copy = pltpu.make_async_copy(result_ref.at[span], out_hbm.at[span], sem.at[comp])
        copy.start()
        copies.append(copy)
    for copy in copies:
        copy.wait()


VMEM = pl.BlockSpec(memory_space=pltpu.VMEM)
HBM = pl.BlockSpec(memory_space=pltpu.HBM)
FINE_ROWS = COMPS * (COARSE // 2 + 1) * X_ROWS


def params(mebibytes):
    return pltpu.CompilerParams(vmem_limit_bytes=mebibytes * 1024 * 1024)


def forward_y(field, kernel):
    table = stacked(fine_table())
    twiddle = y_twiddle(-1.0, 1.0)
    edge = (OFFSETS, EDGE_PARTS, 1, CELLS)
    return pl.pallas_call(
        forward_y_kernel,
        in_specs=[HBM] * 4,
        out_specs=[HBM, HBM],
        out_shape=[jax.ShapeDtypeStruct((DEVICES, SLOT, LANES), F32), jax.ShapeDtypeStruct(edge, F32)],
        scratch_shapes=[
            pltpu.VMEM((FINE_ROWS, 2 * LANES), BF16),
            pltpu.VMEM((FINE_ROWS, 2 * LANES), BF16),
            pltpu.VMEM((DEVICES * SLOT, LANES), F32),
            pltpu.VMEM((COMPS * X_ROWS, CELLS), F32),
            pltpu.VMEM(table.shape, BF16),
            pltpu.VMEM(twiddle.shape, F32),
            pltpu.VMEM(edge, F32),
            pltpu.SemaphoreType.DMA((COMPS,)),
            pltpu.SemaphoreType.DMA((COMPS + 2,)),
            pltpu.SemaphoreType.DMA((3,)),
        ],
        compiler_params=params(63),
        name="forward_y",
    )(field, jnp.asarray(table), jnp.asarray(twiddle), kernel)


def relayout(kernel, flag):
    groups = 3
    rows = OPS // groups * 16
    out_rows = OPS // groups * OWNED
    return pl.pallas_call(
        relayout_kernel,
        grid=(groups,),
        in_specs=[
            pl.BlockSpec(memory_space=pltpu.SMEM),
            pl.BlockSpec((rows, CELLS), lambda g: (g, 0)),
        ],
        out_specs=pl.BlockSpec((ROWS, out_rows, LANES), lambda g: (0, g, 0)),
        out_shape=jax.ShapeDtypeStruct((ROWS, OPS * OWNED, LANES), F32),
        scratch_shapes=[pltpu.VMEM((out_rows, CELLS), F32), pltpu.VMEM((CELLS, LANES), F32)],
        compiler_params=params(48),
        name="relayout",
    )(flag, kernel)


def spectral(lines, kernel, delta):
    twiddle = x_twiddle(-1.0, 1.0, 1.0)
    back_twiddle = x_twiddle(1.0, -1.0 / (CELLS * CELLS), -1.0)
    return pl.pallas_call(
        spectral_kernel,
        in_specs=[VMEM, HBM] + [VMEM] * 5,
        out_specs=VMEM,
        out_shape=jax.ShapeDtypeStruct((DEVICES * SLOT, LANES), F32),
        scratch_shapes=[
            pltpu.VMEM((ROWS * OPS * OWNED, LANES), F32),
            pltpu.VMEM((ROWS * EXTRA, LANES), F32),
            pltpu.VMEM((ROWS * P1_ALL, LANES), F32),
            pltpu.VMEM((ROWS * P1_ALL, 2 * LANES), BF16),
            pltpu.VMEM((ROWS * P1_ALL, LANES), F32),
            pltpu.VMEM((ROWS * P1_ROWS, LANES), F32),
            pltpu.VMEM((ROWS * P1_ROWS, LANES), F32),
            pltpu.SemaphoreType.DMA((4,)),
        ],
        compiler_params=params(48),
        name="spectral",
    )(
        lines,
        kernel,
        delta,
        jnp.asarray(twiddle),
        jnp.asarray(back_twiddle),
        jnp.asarray(x_tables(-1.0)),
        jnp.asarray(x_tables(1.0)),
    )


def inverse_y(spectra):
    rows = COMPS * X_ROWS
    return pl.pallas_call(
        inverse_y_kernel,
        in_specs=[VMEM] * 3,
        out_specs=HBM,
        out_shape=jax.ShapeDtypeStruct((rows, CELLS), F32),
        scratch_shapes=[
            pltpu.VMEM((FINE_ROWS, 2 * LANES), BF16),
            pltpu.VMEM((FINE_ROWS, 2 * LANES), BF16),
            pltpu.VMEM((FINE_ROWS, 2 * LANES), F32),
            pltpu.VMEM((rows, CELLS), F32),
            pltpu.SemaphoreType.DMA((COMPS,)),
        ],
        compiler_params=params(20),
        name="inverse_y",
    )(spectra, jnp.asarray(stacked(fine_table().T)), jnp.asarray(y_twiddle(1.0, 2.0)))


def exchange(lines):
    moved = lax.all_to_all(lines.reshape(DEVICES, SLOT, LANES), ("layer", "row"), 0, 0, tiled=True)
    return moved.reshape(DEVICES * SLOT, LANES)


def local(magnet, kernel):
    axes = ("layer", "row")
    device = lax.axis_index(axes)
    field = magnet.reshape(COMPS * X_ROWS, CELLS)
    flag = (device >= DEVICES // 2).astype(jnp.int32).reshape(1)
    sent, edge = forward_y(field, kernel)
    middle = lax.ppermute(edge, axes, [(DEVICES // 2, 0)])
    got = exchange(sent)
    coefficient = relayout(kernel.reshape(OPS * 16, CELLS), flag)
    delta = jnp.where(device == 0, middle - edge, 0.0)
    delta = jnp.swapaxes(delta.reshape(EDGES, X_ROWS, ROWS), 1, 2)
    delta = jnp.concatenate([delta, delta], axis=2).reshape(EDGES * ROWS, LANES)
    fields = spectral(got, coefficient.reshape(ROWS * OPS * OWNED, LANES), delta)
    result = inverse_y(exchange(fields))
    return result.reshape(COMPS, 1, X_ROWS, CELLS)


def solution(mesh):
    in_specs = (P(None, "layer", "row", None), P(None, None, ("layer", "row"), None))
    out_specs = P(None, "layer", "row", None)
    return jax.shard_map(local, mesh=mesh, in_specs=in_specs, out_specs=out_specs, check_vma=False)
```
